256 devices in a mesh: wide: 64 (over x, y_hi, z), narrow: 4 (over y_lo, core).
Axes of the slice: x: 4, y: 4 (y_hi: 2, y_lo: 2; y = y_hi * 2 + y_lo), z: 8, core: 2. Of those that a mesh axis runs over, the one named last changes fastest.
Arguments:
- tokens: bfloat16 [8192, 2048], P('wide'), may hold values from -6 to 6
- expert_ids: int32 [8192, 6], P('wide'), may hold values from 0 to 63, all different within a row; in each aligned block of 128 rows (0 to 127, 128 to 255, ...) at most 16 rows name the same one
- gate_weights: float32 [8192, 6], P('wide'), may hold values from 0.05 to 0.6
- shared_gate: bfloat16 [2048, 2816], P('wide', 'narrow'), may hold values from -0.125 to 0.125
- shared_up: bfloat16 [2048, 2816], P('wide', 'narrow'), may hold values from -0.125 to 0.125
- shared_down: bfloat16 [2816, 2048], P('narrow', 'wide'), may hold values from -0.109375 to 0.109375
- expert_gate: bfloat16 [64, 2048, 1408], P('wide', None, 'narrow'), may hold values from -0.125 to 0.125
- expert_up: bfloat16 [64, 2048, 1408], P('wide', None, 'narrow'), may hold values from -0.125 to 0.125
- expert_down: bfloat16 [64, 1408, 2048], P('wide', 'narrow'), may hold values from -0.15625 to 0.15625
Outputs:
- moe_out: bfloat16 [8192, 2048], P('wide', 'narrow')
The draws below stay inside these ranges and needn't reach their ends.
Inputs may be any that keep to these rules, and one draw needn't show every extreme that they name: `expert_ids`: the 6 ids of a row differ. Among the 128 rows of one index of wide, no expert is named by more than 16 rows.
All inputs are finite; a program needn't handle non-finite values.
Results may differ from the reference program's by a relative error of at most 0.0075.
Values may be sent and summed in bfloat16 or wider, within the bound.
No kernel may reach another device: no remote copies, remote signals or barrier semaphores. Data moves between devices by JAX's collectives and lax.ppermute only.
A program may use at most 128 MiB of HBM per device.

```python
import math
import jax
import jax.numpy as jnp
import numpy as np
from jax import lax

D = 2048
MF = 1408
FS = 2816
TOP = 6
TOK_DEV = 128
EXPERTS = 64
TOKENS = 8192
CAP = 16
N_WIDE = 64
N_NARROW = 4


def block_scale(stream_key, dims, split, low, high):
    def one(axis_at, blocks):
        steps = jax.random.uniform(jax.random.fold_in(jax.random.fold_in(stream_key, 6), axis_at), (blocks,), jnp.float32, low / len(split), high / len(split))
        return jnp.repeat(jnp.exp(steps), dims[axis_at] // blocks).reshape((-1,) + (1,) * (len(dims) - axis_at - 1))

    factor_of = one(*split[0])
    for cut in split[1:]:
        factor_of = factor_of * one(*cut)
    return factor_of


def shared_out(rng, own, number, rows, number_of, top, most, slope):
    ranking = jax.random.permutation(rng, number_of)
    packed, usual = load_shares(number_of, rows * top, most, slope, True), load_shares(number_of, rows * top, most, slope, False)
    places = jnp.arange(number_of)

    def named(lengths, offset_by):
        used = int((lengths > 0).sum())
        fixed = max(1, used // 4)
        passed = fixed + (places - fixed + offset_by * (used - fixed)) % max(1, number_of - fixed)
        return jnp.zeros((number_of,), jnp.int32).at[ranking[jnp.where(places < fixed, places, passed)]].set(jnp.asarray(lengths, jnp.int32))

    lengths = jnp.where(number % 4 == 0, named(packed, number // 4), named(usual, number - number // 4 - 1))
    mixed = jax.random.permutation(jax.random.fold_in(own, 3), number_of)
    donor, receiver = mixed[0:number_of // 2 * 2:2], mixed[1:number_of // 2 * 2:2]
    margin = jnp.minimum(lengths[donor] - 1, most - lengths[receiver]) // 2
    margin = jnp.where((donor == ranking[0]) | (receiver == ranking[0]) | (lengths[receiver] == 0), 0, jnp.maximum(margin, 0))
    passed = jax.random.randint(jax.random.fold_in(own, 4), (number_of // 2,), 0, 1 << 20) % (margin + 1)
    lengths = lengths.at[donor].add(-passed).at[receiver].add(passed)
    labels = jnp.searchsorted(jnp.cumsum(lengths), jnp.arange(rows * top), side="right").astype(jnp.int32)
    listing = labels.reshape(top, rows).T
    listing = listing[jax.random.permutation(jax.random.fold_in(own, 1), rows)]
    offset_by = jax.random.randint(jax.random.fold_in(own, 2), (rows, 1), 0, top)
    return jnp.take_along_axis(listing, (jnp.arange(top)[None, :] + offset_by) % top, axis=1)


def load_shares(amount, total, limit, lean, full):
    portions = [(1 << 20) // math.isqrt(grade ** lean) + 1 for grade in range(1, amount + 1)]
    largest = limit if full else min(limit, max(-(-total // amount), total * portions[0] // sum(portions)))
    least = 1 if total - largest >= amount - 1 else 0
    counts, surplus = [largest] + [least] * (amount - 1), total - largest - least * (amount - 1)
    while surplus > 0:
        candidates = [i for i in range(1, amount) if counts[i] < largest] or [i for i in range(1, amount) if counts[i] < limit]
        whole, budget = sum([portions[i] for i in candidates]), surplus
        for i in candidates:
            more = min(limit - counts[i], max(1, budget * portions[i] // whole), surplus)
            counts[i] = counts[i] + more
            surplus = surplus - more
    return np.array(counts)


def normal_values(stream_key, extent, spread, reach, cuts=(), held_as=jnp.bfloat16):
    array = jax.random.normal(stream_key, extent, jnp.float32) * spread
    if len(cuts) > 0:
        array = block_scale(stream_key, extent, cuts, -0.22, 0.18) * array
    return jnp.clip(array, min=-reach, max=reach).astype(held_as)


def setup_inputs(seed: int = 0) -> dict:
    keys = jax.random.split(jax.random.key(seed), 10)
    tokens = normal_values(keys[0], (TOKENS, D), 1.0, 6.0, ((0, 64),))
    expert_ids_keys = jax.random.split(jax.random.fold_in(keys[1], 1), TOKENS // TOK_DEV)
    expert_ids_turns = jax.random.permutation(jax.random.fold_in(keys[1], 3), TOKENS // TOK_DEV)
    expert_ids = jax.vmap(lambda own, number: shared_out(jax.random.fold_in(keys[1], 2), own, number, TOK_DEV, EXPERTS, TOP, CAP, 2))(expert_ids_keys, expert_ids_turns).reshape((TOKENS, TOP))
    gate_weights = jnp.clip(jnp.exp(math.log(0.6) - 2.4849067 * jax.random.uniform(keys[2], (TOKENS, TOP), jnp.float32) ** block_scale(keys[2], (TOKENS, TOP), ((0, 64),), -0.2, 0.2)), 0.05, 0.6)
    shared_gate = normal_values(keys[3], (D, FS), D ** -0.5, 0.125, ((0, 64), (1, 4)))
    shared_up = normal_values(keys[4], (D, FS), D ** -0.5, 0.125, ((0, 64), (1, 4)))
    shared_down = normal_values(keys[5], (FS, D), FS ** -0.5, 0.109375, ((0, 4), (1, 64)))
    expert_gate = normal_values(keys[6], (EXPERTS, D, MF), D ** -0.5, 0.125, ((0, 64), (2, 4)))
    expert_up = normal_values(keys[7], (EXPERTS, D, MF), D ** -0.5, 0.125, ((0, 64), (2, 4)))
    expert_down = normal_values(keys[8], (EXPERTS, MF, D), MF ** -0.5, 0.15625, ((0, 64), (1, 4)))
    return {"tokens": tokens, "expert_ids": expert_ids, "gate_weights": gate_weights, "shared_gate": shared_gate, "shared_up": shared_up, "shared_down": shared_down, "expert_gate": expert_gate, "expert_up": expert_up, "expert_down": expert_down}


def expert_rows(rows_in, w_gate, w_up, w_down):
    gate_part = jnp.dot(rows_in, w_gate, preferred_element_type=jnp.float32)
    up_part = jnp.dot(rows_in, w_up, preferred_element_type=jnp.float32)
    hidden = (jax.nn.silu(gate_part) * up_part).astype(jnp.bfloat16)
    quarter = MF // N_NARROW
    summed = jnp.zeros((rows_in.shape[0], w_down.shape[1]), jnp.float32)
    for slice_idx in range(N_NARROW):
        lower = slice_idx * quarter
        partial_value = jnp.dot(hidden[:, lower:lower + quarter], w_down[lower:lower + quarter], preferred_element_type=jnp.float32)
        summed = summed + partial_value.astype(jnp.bfloat16).astype(jnp.float32)
    return summed.astype(jnp.bfloat16)


def reference(tokens, expert_ids, gate_weights, shared_gate, shared_up, shared_down, expert_gate, expert_up, expert_down):
    shared_g = jnp.dot(tokens, shared_gate, preferred_element_type=jnp.float32)
    shared_u = jnp.dot(tokens, shared_up, preferred_element_type=jnp.float32)
    shared_hidden = (jax.nn.silu(shared_g) * shared_u).astype(jnp.bfloat16)
    shared = jnp.dot(shared_hidden, shared_down, preferred_element_type=jnp.float32)
    slot_count = N_WIDE * CAP
    positions = jnp.arange(TOKENS, dtype=jnp.int32)

    def one_expert(routed, inputs):
        expert_index, w_gate, w_up, w_down = inputs
        matches = expert_ids == expert_index
        chosen = jnp.any(matches, axis=1)
        weight = jnp.sum(jnp.where(matches, gate_weights, jnp.float32(0.0)), axis=1)
        rank_pos = (jnp.cumsum(chosen.astype(jnp.int32)) - 1).astype(jnp.int32)
        target = jnp.where(chosen, rank_pos, slot_count).astype(jnp.int32)
        picked = jnp.zeros((slot_count + 1,), jnp.int32).at[target].set(positions)[:slot_count]
        weight_live = jnp.zeros((slot_count + 1,), jnp.float32).at[target].set(weight)[:slot_count]
        outputs = expert_rows(tokens[picked], w_gate, w_up, w_down)
        routed = routed.at[picked].add(weight_live[:, None] * outputs.astype(jnp.float32))
        return routed, None

    routed0 = jnp.zeros((TOKENS, D), jnp.float32)
    indices = jnp.arange(EXPERTS, dtype=jnp.int32)
    routed, unused = lax.scan(one_expert, routed0, (indices, expert_gate, expert_up, expert_down))
    return (shared + routed).astype(jnp.bfloat16)
```

```python
import jax
import jax.numpy as jnp
from jax import lax
from jax.experimental import pallas as pl
from jax.experimental.pallas import tpu as pltpu
from jax.sharding import PartitionSpec as P


F32 = jnp.float32
BF16 = jnp.bfloat16
CAP = 16
EXPERTS = 64
SLOTS = EXPERTS * CAP
TOK = 128
D = 2048
NX = 4
NYZ = 16
X_GROUPS = [[x * NYZ + i for x in range(NX)] for i in range(NYZ)]
YZ_GROUPS = [[x * NYZ + i for i in range(NYZ)] for x in range(NX)]
CORE_SWAP = [(0, 1), (1, 0), (2, 3), (3, 2)]
Y_SWAP = [(0, 2), (2, 0), (1, 3), (3, 1)]
NO_SLOT = 100.0


def x_shift(d):
    return [(x * NYZ + i, (x + d) % NX * NYZ + i) for x in range(NX) for i in range(NYZ)]


def silu(v):
    return v / (1.0 + jnp.exp(-v))


def dot(a, b):
    return lax.dot_general(a, b, (((1,), (0,)), ((), ())), preferred_element_type=F32)


def dot_nt(a, b):
    return lax.dot_general(a, b, (((1,), (1,)), ((), ())), preferred_element_type=F32)


def named_counts(ids, shape, k_axis):
    expert = lax.broadcasted_iota(jnp.int32, shape, k_axis).astype(F32)
    named = jnp.zeros(shape, F32)
    for k in range(ids.shape[k_axis]):
        one = ids[:, k : k + 1] if k_axis else ids[k : k + 1, :]
        named = named + jnp.where(one == expert, 1.0, 0.0)
    return named


def order_matrix(upper):
    row = lax.broadcasted_iota(jnp.int32, (TOK, TOK), 0)
    col = lax.broadcasted_iota(jnp.int32, (TOK, TOK), 1)
    before = row < col if upper else col < row
    return jnp.where(before, 1.0, 0.0).astype(BF16)


def dispatch_kernel(pos_ref, ids_ref, tok_ref, out_ref):
    del pos_ref
    rows = out_ref.shape[0]
    first = pl.program_id(0) * rows
    named = named_counts(ids_ref[...].astype(F32), (EXPERTS, TOK), 0)
    place = dot(named.astype(BF16), order_matrix(True))
    keys = jnp.where(named > 0.0, place, NO_SLOT).astype(BF16)
    r = lax.broadcasted_iota(jnp.int32, (rows, EXPERTS), 0) + first
    e = lax.broadcasted_iota(jnp.int32, (rows, EXPERTS), 1)
    spread = jnp.where((r >> 4) == e, 1.0, 0.0).astype(BF16)
    wanted = dot(spread, keys)
    slot = ((lax.broadcasted_iota(jnp.int32, (rows, TOK), 0) + first) & 15).astype(F32)
    pick = jnp.where(wanted == slot, 1.0, 0.0).astype(BF16)
    out_ref[...] = dot(pick, tok_ref[...]).astype(BF16)


def dispatch(pos, ids_t, tokens):
    blocks = 2
    rows = SLOTS // blocks
    return pl.pallas_call(
        dispatch_kernel,
        grid_spec=pltpu.PrefetchScalarGridSpec(
            num_scalar_prefetch=1,
            grid=(blocks,),
            in_specs=[
                pl.BlockSpec(ids_t.shape, lambda i, p: (0, 0)),
                pl.BlockSpec((TOK, D // 2), lambda i, p: (0, p[0])),
            ],
            out_specs=pl.BlockSpec((rows, D // 2), lambda i, p: (i, 0)),
        ),
        out_shape=jax.ShapeDtypeStruct((SLOTS, D // 2), BF16),
        name="dispatch",
    )(pos, ids_t, tokens)


def pack_kernel(gate_ref, up_ref, down_ref, out_ref):
    fs = out_ref.shape[2] // 3
    for x in range(NX):
        cut = slice(x * fs, (x + 1) * fs)
        out_ref[x] = jnp.concatenate([gate_ref[:, cut], up_ref[:, cut], down_ref[:, cut]], axis=1)


def pack(gate, up, down_t):
    fs = gate.shape[1] // NX
    return pl.pallas_call(
        pack_kernel,
        out_shape=jax.ShapeDtypeStruct((NX, gate.shape[0], 3 * fs), BF16),
        name="pack",
    )(gate, up, down_t)


def expert_kernel(
    pos_ref, own_ref, peer_ref, wg0, wg1, wu0, wu1, wd0, wd1, wd2, wd3, keep_ref, send_ref
):
    del pos_ref
    own = own_ref[...]
    peer = peer_ref[...]
    gate = dot_nt(own, wg0[0]) + dot_nt(peer, wg1[0])
    up = dot_nt(own, wu0[0]) + dot_nt(peer, wu1[0])
    hidden = (silu(gate) * up).astype(BF16)
    keep_ref[:, :512] = dot(hidden, wd0[0]).astype(BF16)
    keep_ref[:, 512:] = dot(hidden, wd1[0]).astype(BF16)
    send_ref[:, :512] = dot(hidden, wd2[0]).astype(BF16)
    send_ref[:, 512:] = dot(hidden, wd3[0]).astype(BF16)


def expert_ffn(pos, own, peer, w_gate, w_up, w_down):
    blocks = 4
    rows = SLOTS // blocks
    mf = w_gate.shape[1]
    x_spec = pl.BlockSpec((rows, D // 2), lambda i, p: (i, 0))
    in_own = pl.BlockSpec((1, mf, D // 2), lambda i, p: (0, 0, p[0]))
    in_peer = pl.BlockSpec((1, mf, D // 2), lambda i, p: (0, 0, 1 - p[0]))
    down = [
        pl.BlockSpec((1, mf, 512), lambda i, p: (0, 0, p[0])),
        pl.BlockSpec((1, mf, 512), lambda i, p: (0, 0, 2 + p[0])),
        pl.BlockSpec((1, mf, 512), lambda i, p: (0, 0, 1 - p[0])),
        pl.BlockSpec((1, mf, 512), lambda i, p: (0, 0, 3 - p[0])),
    ]
    return pl.pallas_call(
        expert_kernel,
        grid_spec=pltpu.PrefetchScalarGridSpec(
            num_scalar_prefetch=1,
            grid=(blocks,),
            in_specs=[x_spec, x_spec, in_own, in_peer, in_own, in_peer] + down,
            out_specs=[x_spec, x_spec],
        ),
        out_shape=[jax.ShapeDtypeStruct((SLOTS, D // 2), BF16)] * 2,
        cost_estimate=pl.CostEstimate(
            flops=2 * SLOTS * D * mf * 3, bytes_accessed=13_000_000, transcendentals=SLOTS * mf
        ),
        name="experts",
    )(pos, own, peer, w_gate, w_gate, w_up, w_up, w_down, w_down, w_down, w_down)


def shared_kernel(pos_ref, tok_ref, w_ref, after_ref, keep_ref, send_ref):
    del after_ref
    core = pos_ref[0]
    fs = w_ref.shape[3] // 3
    rows = w_ref.shape[0] * w_ref.shape[2]
    total = jnp.zeros((TOK, 3 * fs), F32)
    for x in range(NX):
        w = w_ref[:, x].reshape(rows, 3 * fs)
        total = total + dot(tok_ref[0, :, x * rows : (x + 1) * rows], w)
    hidden = silu(total[:, :fs]) * total[:, fs : 2 * fs]
    hidden = jnp.concatenate([jnp.zeros((TOK, 2 * fs), F32), hidden], axis=1).astype(BF16)
    for half in range(2):
        for out_ref, at in ((keep_ref, core), (send_ref, 1 - core)):
            w = w_ref[:, pl.ds(2 * half + at, 1)].reshape(rows, 3 * fs)
            out_ref[0, :, half * 512 : (half + 1) * 512] = dot_nt(hidden, w).astype(BF16)


def shared_ffn(pos, toks, weights, after):
    fs3 = weights.shape[3]
    out_spec = pl.BlockSpec((1, TOK, D // 2), lambda i, p: (i, 0, 0))
    return pl.pallas_call(
        shared_kernel,
        grid_spec=pltpu.PrefetchScalarGridSpec(
            num_scalar_prefetch=1,
            grid=(NX,),
            in_specs=[
                pl.BlockSpec((1, TOK, D), lambda i, p: ((i + p[2]) & 3, 0, 0)),
                pl.BlockSpec(weights.shape, lambda i, p: (0, 0, 0, 0)),
                pl.BlockSpec(memory_space=pl.ANY),
            ],
            out_specs=[out_spec, out_spec],
        ),
        out_shape=[jax.ShapeDtypeStruct((NX, TOK, D // 2), BF16)] * 2,
        cost_estimate=pl.CostEstimate(
            flops=2 * NX * TOK * D * fs3 * 2, bytes_accessed=6_000_000, transcendentals=NX * TOK * fs3 // 3
        ),
        name="shared",
    )(pos, toks, weights, after)


def turned(values):
    row = lax.broadcasted_iota(jnp.int32, (TOK, TOK), 0)
    col = lax.broadcasted_iota(jnp.int32, (TOK, TOK), 1)
    eye = jnp.where(row == col, 1.0, 0.0).astype(BF16)
    total = None
    rest = values
    for _ in range(3):
        part = rest.astype(BF16)
        rest = rest - part.astype(F32)
        moved = dot_nt(eye, part)
        total = moved if total is None else total + moved
    return total


def combine_kernel(pos_ref, ids_ref, gw_ref, ret_ref, sh0, sh1, sh2, sh3, keep_ref, send_ref):
    ids = turned(ids_ref[...].astype(F32))
    gates = turned(gw_ref[...])
    named = named_counts(ids, (TOK, EXPERTS), 1)
    place = dot(order_matrix(False), named.astype(BF16))
    keys = jnp.where(named > 0.0, place, NO_SLOT).astype(BF16)
    lane = lax.broadcasted_iota(jnp.int32, (TOK, EXPERTS), 1).astype(F32)
    weight = jnp.zeros((TOK, EXPERTS), F32)
    for k in range(ids.shape[1]):
        weight = weight + jnp.where(ids[:, k : k + 1] == lane, gates[:, k : k + 1], 0.0)
    e = lax.broadcasted_iota(jnp.int32, (EXPERTS, SLOTS), 0)
    r = lax.broadcasted_iota(jnp.int32, (EXPERTS, SLOTS), 1)
    spread = jnp.where((r >> 4) == e, 1.0, 0.0).astype(BF16)
    slot = (lax.broadcasted_iota(jnp.int32, (TOK, SLOTS), 1) & 15).astype(F32)
    hit = dot(keys, spread) == slot
    ret = ret_ref[...]
    total = jnp.zeros((TOK, D // 2), F32)
    rest = weight
    for _ in range(3):
        part = rest.astype(BF16)
        rest = rest - part.astype(F32)
        row = jnp.where(hit, dot(part, spread), 0.0).astype(BF16)
        total = total + dot(row, ret)
    for shared_ref in (sh0, sh1, sh2, sh3):
        total = total + shared_ref[...].astype(F32)
    low = total[:, :512]
    high = total[:, 512:]
    first = pos_ref[1] == 0
    keep_ref[...] = jnp.where(first, low, high)
    send_ref[...] = jnp.where(first, high, low).astype(BF16)


def combine(pos, ids, gate_weights, returned, shared):
    vmem = pl.BlockSpec(memory_space=pltpu.VMEM)
    return pl.pallas_call(
        combine_kernel,
        in_specs=[pl.BlockSpec(memory_space=pltpu.SMEM)] + [vmem] * 7,
        out_specs=[vmem, vmem],
        out_shape=[
            jax.ShapeDtypeStruct((TOK, 512), F32),
            jax.ShapeDtypeStruct((TOK, 512), BF16),
        ],
        name="combine",
    )(pos, ids, gate_weights, returned, *shared)


def body(
    tokens,
    expert_ids,
    gate_weights,
    shared_gate,
    shared_up,
    shared_down,
    expert_gate,
    expert_up,
    expert_down,
):
    narrow = lax.axis_index("narrow")
    place = lax.axis_index("wide") >> 4
    pos = jnp.stack([narrow & 1, narrow >> 1, place]).astype(jnp.int32)
    ids_t = expert_ids.T
    gates_t = gate_weights.T

    packed = pack(shared_gate, shared_up, shared_down.T)
    packed = lax.all_to_all(packed, "wide", 0, 0, axis_index_groups=X_GROUPS, tiled=True)
    weights = lax.all_gather(packed[None], "wide", axis=0, axis_index_groups=YZ_GROUPS, tiled=True)
    toks = lax.all_gather(tokens[None], "wide", axis=0, axis_index_groups=X_GROUPS, tiled=True)

    outgoing = dispatch(pos, ids_t, tokens).reshape(EXPERTS, CAP, D // 2)
    received = lax.all_to_all(outgoing, "wide", 0, 0, tiled=True).reshape(SLOTS, D // 2)
    peer = lax.ppermute(received, "narrow", CORE_SWAP)
    keep, send = expert_ffn(
        pos, received, peer, expert_gate.transpose(0, 2, 1), expert_up.transpose(0, 2, 1), expert_down
    )
    other = lax.ppermute(send, "narrow", CORE_SWAP)
    summed = (keep.astype(F32) + other.astype(F32)).astype(BF16)
    returned = lax.all_to_all(summed.reshape(EXPERTS, CAP, D // 2), "wide", 0, 0, tiled=True)

    mine, theirs = shared_ffn(pos, toks, weights, summed)
    theirs = lax.ppermute(theirs, "narrow", CORE_SWAP)
    shared = []
    for d in range(NX):
        one = (mine[d].astype(F32) + theirs[d].astype(F32)).astype(BF16)
        if d > 0:
            one = lax.ppermute(one, "wide", x_shift(d))
        shared.append(one)

    kept, sent = combine(pos, ids_t, gates_t, returned.reshape(SLOTS, D // 2), shared)
    got = lax.ppermute(sent, "narrow", Y_SWAP)
    return (kept + got.astype(F32)).astype(BF16)


def solution(mesh):
    in_specs = (
        P("wide", None),
        P("wide", None),
        P("wide", None),
        P("wide", "narrow"),
        P("wide", "narrow"),
        P("narrow", "wide"),
        P("wide", None, "narrow"),
        P("wide", None, "narrow"),
        P("wide", "narrow", None),
    )
    out_specs = P("wide", "narrow")
    return jax.shard_map(body, mesh=mesh, in_specs=in_specs, out_specs=out_specs, check_vma=False)
```

```python
import jax
import jax.numpy as jnp
from jax import lax
from jax.experimental import pallas as pl
from jax.experimental.pallas import tpu as pltpu
from jax.sharding import PartitionSpec as P


F32 = jnp.float32
BF16 = jnp.bfloat16
CAP = 16
EXPERTS = 64
SLOTS = EXPERTS * CAP
TOK = 128
D = 2048
NX = 4
NYZ = 16
X_GROUPS = [[x * NYZ + i for x in range(NX)] for i in range(NYZ)]
YZ_GROUPS = [[x * NYZ + i for i in range(NYZ)] for x in range(NX)]
CORE_SWAP = [(0, 1), (1, 0), (2, 3), (3, 2)]
Y_SWAP = [(0, 2), (2, 0), (1, 3), (3, 1)]
NO_SLOT = 100.0


def x_shift(d):
    return [(x * NYZ + i, (x + d) % NX * NYZ + i) for x in range(NX) for i in range(NYZ)]


def silu(v):
    return v / (1.0 + jnp.exp(-v))


def dot(a, b):
    return lax.dot_general(a, b, (((1,), (0,)), ((), ())), preferred_element_type=F32)


def dot_nt(a, b):
    return lax.dot_general(a, b, (((1,), (1,)), ((), ())), preferred_element_type=F32)


def named_counts(ids, shape, k_axis):
    expert = lax.broadcasted_iota(jnp.int32, shape, k_axis).astype(F32)
    named = jnp.zeros(shape, F32)
    for k in range(ids.shape[k_axis]):
        one = ids[:, k : k + 1] if k_axis else ids[k : k + 1, :]
        named = named + jnp.where(one == expert, 1.0, 0.0)
    return named


def order_matrix(upper):
    row = lax.broadcasted_iota(jnp.int32, (TOK, TOK), 0)
    col = lax.broadcasted_iota(jnp.int32, (TOK, TOK), 1)
    before = row < col if upper else col < row
    return jnp.where(before, 1.0, 0.0).astype(BF16)


def dispatch_kernel(pos_ref, ids_ref, tok_ref, out_ref):
    del pos_ref
    rows = out_ref.shape[0]
    first = pl.program_id(0) * rows
    named = named_counts(ids_ref[...].astype(F32), (EXPERTS, TOK), 0)
    place = dot(named.astype(BF16), order_matrix(True))
    keys = jnp.where(named > 0.0, place, NO_SLOT).astype(BF16)
    r = lax.broadcasted_iota(jnp.int32, (rows, EXPERTS), 0) + first
    e = lax.broadcasted_iota(jnp.int32, (rows, EXPERTS), 1)
    spread = jnp.where((r >> 4) == e, 1.0, 0.0).astype(BF16)
    wanted = dot(spread, keys)
    slot = ((lax.broadcasted_iota(jnp.int32, (rows, TOK), 0) + first) & 15).astype(F32)
    pick = jnp.where(wanted == slot, 1.0, 0.0).astype(BF16)
    out_ref[...] = dot(pick, tok_ref[...]).astype(BF16)


def dispatch(pos, ids_t, tokens):
    blocks = 2
    rows = SLOTS // blocks
    return pl.pallas_call(
        dispatch_kernel,
        grid_spec=pltpu.PrefetchScalarGridSpec(
            num_scalar_prefetch=1,
            grid=(blocks,),
            in_specs=[
                pl.BlockSpec(ids_t.shape, lambda i, p: (0, 0)),
                pl.BlockSpec((TOK, D // 2), lambda i, p: (0, p[0])),
            ],
            out_specs=pl.BlockSpec((rows, D // 2), lambda i, p: (i, 0)),
        ),
        out_shape=jax.ShapeDtypeStruct((SLOTS, D // 2), BF16),
        name="dispatch",
    )(pos, ids_t, tokens)


def pack_kernel(gate_ref, up_ref, down_ref, out_ref):
    fs = out_ref.shape[2] // 3
    for x in range(NX):
        cut = slice(x * fs, (x + 1) * fs)
        out_ref[x] = jnp.concatenate([gate_ref[:, cut], up_ref[:, cut], down_ref[:, cut]], axis=1)


def pack(gate, up, down_t):
    fs = gate.shape[1] // NX
    return pl.pallas_call(
        pack_kernel,
        out_shape=jax.ShapeDtypeStruct((NX, gate.shape[0], 3 * fs), BF16),
        name="pack",
    )(gate, up, down_t)


def hidden_kernel(pos_ref, own_ref, peer_ref, wg0, wg1, wu0, wu1, out_ref):
    del pos_ref
    own = own_ref[...]
    peer = peer_ref[...]
    gate = dot_nt(own, wg0[0]) + dot_nt(peer, wg1[0])
    up = dot_nt(own, wu0[0]) + dot_nt(peer, wu1[0])
    mf = gate.shape[1]
    out_ref[:, :mf] = (silu(gate) * up).astype(BF16)
    out_ref[:, mf:] = jnp.zeros((own.shape[0], out_ref.shape[1] - mf), BF16)


def expert_hidden(pos, own, peer, w_gate, w_up):
    blocks = 4
    rows = SLOTS // blocks
    mf = w_gate.shape[1]
    padded = -(-mf // 128) * 128
    x_spec = pl.BlockSpec((rows, D // 2), lambda i, p: (i, 0))
    in_own = pl.BlockSpec((1, mf, D // 2), lambda i, p: (0, 0, p[0]))
    in_peer = pl.BlockSpec((1, mf, D // 2), lambda i, p: (0, 0, 1 - p[0]))
    return pl.pallas_call(
        hidden_kernel,
        grid_spec=pltpu.PrefetchScalarGridSpec(
            num_scalar_prefetch=1,
            grid=(blocks,),
            in_specs=[x_spec, x_spec, in_own, in_peer, in_own, in_peer],
            out_specs=pl.BlockSpec((rows, padded), lambda i, p: (i, 0)),
        ),
        out_shape=jax.ShapeDtypeStruct((SLOTS, padded), BF16),
        cost_estimate=pl.CostEstimate(
            flops=4 * SLOTS * D * mf, bytes_accessed=8_000_000, transcendentals=SLOTS * mf
        ),
        name="hidden",
    )(pos, own, peer, w_gate, w_gate, w_up, w_up)


def down_kernel(pos_ref, own_ref, peer_ref, a0, a1, b0, b1, out_ref):
    del pos_ref
    mf = a0.shape[1]
    own = own_ref[:, :mf]
    peer = peer_ref[:, :mf]
    out_ref[:, :512] = (dot(own, a0[0]) + dot(peer, b0[0])).astype(BF16)
    out_ref[:, 512:] = (dot(own, a1[0]) + dot(peer, b1[0])).astype(BF16)


def expert_down_half(pos, own, peer, w_own, w_peer):
    blocks = 4
    rows = SLOTS // blocks
    mf = w_own.shape[1]
    h_spec = pl.BlockSpec((rows, own.shape[1]), lambda i, p: (i, 0))
    low = pl.BlockSpec((1, mf, 512), lambda i, p: (0, 0, p[0]))
    high = pl.BlockSpec((1, mf, 512), lambda i, p: (0, 0, 2 + p[0]))
    return pl.pallas_call(
        down_kernel,
        grid_spec=pltpu.PrefetchScalarGridSpec(
            num_scalar_prefetch=1,
            grid=(blocks,),
            in_specs=[h_spec, h_spec, low, high, low, high],
            out_specs=pl.BlockSpec((rows, D // 2), lambda i, p: (i, 0)),
        ),
        out_shape=jax.ShapeDtypeStruct((SLOTS, D // 2), BF16),
        cost_estimate=pl.CostEstimate(
            flops=2 * SLOTS * D * mf, bytes_accessed=5_000_000, transcendentals=0
        ),
        name="down",
    )(pos, own, peer, w_own, w_own, w_peer, w_peer)


def shared_kernel(pos_ref, t0, t1, t2, t3, w_ref, after_ref, keep_ref, send_ref):
    del after_ref
    core = pos_ref[0]
    fs = w_ref.shape[3] // 3
    rows = w_ref.shape[0] * w_ref.shape[2]
    for d, tok_ref in enumerate((t0, t1, t2, t3)):
        total = jnp.zeros((TOK, 3 * fs), F32)
        for x in range(NX):
            w = w_ref[:, x].reshape(rows, 3 * fs)
            total = total + dot(tok_ref[:, x * rows : (x + 1) * rows], w)
        hidden = silu(total[:, :fs]) * total[:, fs : 2 * fs]
        hidden = jnp.concatenate([jnp.zeros((TOK, 2 * fs), F32), hidden], axis=1).astype(BF16)
        for half in range(2):
            for out_ref, at in ((keep_ref, core), (send_ref, 1 - core)):
                w = w_ref[:, pl.ds(2 * half + at, 1)].reshape(rows, 3 * fs)
                out_ref[d, :, half * 512 : (half + 1) * 512] = dot_nt(hidden, w).astype(BF16)


def shared_ffn(pos, toks, weights, after):
    fs3 = weights.shape[3]
    vmem = pl.BlockSpec(memory_space=pltpu.VMEM)
    return pl.pallas_call(
        shared_kernel,
        in_specs=[pl.BlockSpec(memory_space=pltpu.SMEM)] + [vmem] * 5 + [pl.BlockSpec(memory_space=pl.ANY)],
        out_specs=[vmem, vmem],
        out_shape=[jax.ShapeDtypeStruct((NX, TOK, D // 2), BF16)] * 2,
        cost_estimate=pl.CostEstimate(
            flops=2 * NX * TOK * D * fs3 * 2, bytes_accessed=6_000_000, transcendentals=NX * TOK * fs3 // 3
        ),
        name="shared",
    )(pos, *toks, weights, after)


def turned(values):
    row = lax.broadcasted_iota(jnp.int32, (TOK, TOK), 0)
    col = lax.broadcasted_iota(jnp.int32, (TOK, TOK), 1)
    eye = jnp.where(row == col, 1.0, 0.0).astype(BF16)
    total = None
    rest = values
    for _ in range(3):
        part = rest.astype(BF16)
        rest = rest - part.astype(F32)
        moved = dot_nt(eye, part)
        total = moved if total is None else total + moved
    return total


def combine_kernel(pos_ref, ids_ref, gw_ref, ret_ref, sh0, sh1, sh2, sh3, keep_ref, send_ref):
    ids = turned(ids_ref[...].astype(F32))
    gates = turned(gw_ref[...])
    named = named_counts(ids, (TOK, EXPERTS), 1)
    place = dot(order_matrix(False), named.astype(BF16))
    keys = jnp.where(named > 0.0, place, NO_SLOT).astype(BF16)
    lane = lax.broadcasted_iota(jnp.int32, (TOK, EXPERTS), 1).astype(F32)
    weight = jnp.zeros((TOK, EXPERTS), F32)
    for k in range(ids.shape[1]):
        weight = weight + jnp.where(ids[:, k : k + 1] == lane, gates[:, k : k + 1], 0.0)
    e = lax.broadcasted_iota(jnp.int32, (EXPERTS, SLOTS), 0)
    r = lax.broadcasted_iota(jnp.int32, (EXPERTS, SLOTS), 1)
    spread = jnp.where((r >> 4) == e, 1.0, 0.0).astype(BF16)
    slot = (lax.broadcasted_iota(jnp.int32, (TOK, SLOTS), 1) & 15).astype(F32)
    hit = dot(keys, spread) == slot
    ret = ret_ref[...]
    total = jnp.zeros((TOK, D // 2), F32)
    rest = weight
    for _ in range(3):
        part = rest.astype(BF16)
        rest = rest - part.astype(F32)
        row = jnp.where(hit, dot(part, spread), 0.0).astype(BF16)
        total = total + dot(row, ret)
    for shared_ref in (sh0, sh1, sh2, sh3):
        total = total + shared_ref[...].astype(F32)
    low = total[:, :512]
    high = total[:, 512:]
    first = pos_ref[1] == 0
    keep_ref[...] = jnp.where(first, low, high)
    send_ref[...] = jnp.where(first, high, low).astype(BF16)


def combine(pos, ids, gate_weights, returned, shared):
    vmem = pl.BlockSpec(memory_space=pltpu.VMEM)
    return pl.pallas_call(
        combine_kernel,
        in_specs=[pl.BlockSpec(memory_space=pltpu.SMEM)] + [vmem] * 7,
        out_specs=[vmem, vmem],
        out_shape=[
            jax.ShapeDtypeStruct((TOK, 512), F32),
            jax.ShapeDtypeStruct((TOK, 512), BF16),
        ],
        name="combine",
    )(pos, ids, gate_weights, returned, *shared)


def body(
    tokens,
    expert_ids,
    gate_weights,
    shared_gate,
    shared_up,
    shared_down,
    expert_gate,
    expert_up,
    expert_down,
):
    narrow = lax.axis_index("narrow")
    pos = jnp.stack([narrow & 1, narrow >> 1]).astype(jnp.int32)
    ids_t = expert_ids.T
    gates_t = gate_weights.T

    packed = pack(shared_gate, shared_up, shared_down.T)
    packed = lax.all_to_all(packed, "wide", 0, 0, axis_index_groups=X_GROUPS, tiled=True)
    weights = lax.all_gather(packed[None], "wide", axis=0, axis_index_groups=YZ_GROUPS, tiled=True)

    outgoing = dispatch(pos, ids_t, tokens).reshape(EXPERTS, CAP, D // 2)
    received = lax.all_to_all(outgoing, "wide", 0, 0, tiled=True).reshape(SLOTS, D // 2)
    toks = [tokens]
    peer_down = lax.ppermute(expert_down, "narrow", CORE_SWAP)
    for d in range(1, NX):
        toks.append(lax.ppermute(tokens, "wide", x_shift(d)))
    peer = lax.ppermute(received, "narrow", CORE_SWAP)
    hidden = expert_hidden(
        pos, received, peer, expert_gate.transpose(0, 2, 1), expert_up.transpose(0, 2, 1)
    )
    peer_hidden = lax.ppermute(hidden, "narrow", CORE_SWAP)
    summed = expert_down_half(pos, hidden, peer_hidden, expert_down, peer_down)
    returned = lax.all_to_all(summed.reshape(EXPERTS, CAP, D // 2), "wide", 0, 0, tiled=True)

    mine, theirs = shared_ffn(pos, toks, weights, summed)
    theirs = lax.ppermute(theirs, "narrow", CORE_SWAP)
    shared = []
    for d in range(NX):
        one = (mine[d].astype(F32) + theirs[d].astype(F32)).astype(BF16)
        if d > 0:
            one = lax.ppermute(one, "wide", x_shift(NX - d))
        shared.append(one)

    kept, sent = combine(pos, ids_t, gates_t, returned.reshape(SLOTS, D // 2), shared)
    got = lax.ppermute(sent, "narrow", Y_SWAP)
    return (kept + got.astype(F32)).astype(BF16)


def solution(mesh):
    in_specs = (
        P("wide", None),
        P("wide", None),
        P("wide", None),
        P("wide", "narrow"),
        P("wide", "narrow"),
        P("narrow", "wide"),
        P("wide", None, "narrow"),
        P("wide", None, "narrow"),
        P("wide", "narrow", None),
    )
    out_specs = P("wide", "narrow")
    return jax.shard_map(body, mesh=mesh, in_specs=in_specs, out_specs=out_specs, check_vma=False)
```

```python
import jax
import jax.numpy as jnp
from jax import lax
from jax.experimental import pallas as pl
from jax.experimental.pallas import tpu as pltpu
from jax.sharding import PartitionSpec as P


F32 = jnp.float32
BF16 = jnp.bfloat16
CAP = 16
EXPERTS = 64
SLOTS = EXPERTS * CAP
TOK = 128
D = 2048
NX = 4
NYZ = 16
X_GROUPS = [[x * NYZ + i for x in range(NX)] for i in range(NYZ)]
YZ_GROUPS = [[x * NYZ + i for i in range(NYZ)] for x in range(NX)]
CORE_SWAP = [(0, 1), (1, 0), (2, 3), (3, 2)]
Y_SWAP = [(0, 2), (2, 0), (1, 3), (3, 1)]
BOTH_SWAP = [(0, 3), (3, 0), (1, 2), (2, 1)]
COLS = D // 4
CHUNKS = 2
CHUNK_ROWS = SLOTS // CHUNKS
STEP_ROWS = 256
NO_SLOT = 100.0


def x_shift(d):
    return [(x * NYZ + i, (x + d) % NX * NYZ + i) for x in range(NX) for i in range(NYZ)]


def silu(v):
    return v / (1.0 + jnp.exp(-v))


def dot(a, b):
    return lax.dot_general(a, b, (((1,), (0,)), ((), ())), preferred_element_type=F32)


def dot_nt(a, b):
    return lax.dot_general(a, b, (((1,), (1,)), ((), ())), preferred_element_type=F32)


def named_counts(ids, shape, k_axis):
    expert = lax.broadcasted_iota(jnp.int32, shape, k_axis).astype(F32)
    named = jnp.zeros(shape, F32)
    for k in range(ids.shape[k_axis]):
        one = ids[:, k : k + 1] if k_axis else ids[k : k + 1, :]
        named = named + jnp.where(one == expert, 1.0, 0.0)
    return named


def order_matrix(upper):
    row = lax.broadcasted_iota(jnp.int32, (TOK, TOK), 0)
    col = lax.broadcasted_iota(jnp.int32, (TOK, TOK), 1)
    before = row < col if upper else col < row
    return jnp.where(before, 1.0, 0.0).astype(BF16)


def dispatch_kernel(pos_ref, ids_ref, tok_ref, out_ref):
    del pos_ref
    rows = out_ref.shape[0]
    first = pl.program_id(0) * rows
    named = named_counts(ids_ref[...].astype(F32), (EXPERTS, TOK), 0)
    place = dot(named.astype(BF16), order_matrix(True))
    keys = jnp.where(named > 0.0, place, NO_SLOT).astype(BF16)
    r = lax.broadcasted_iota(jnp.int32, (rows, EXPERTS), 0) + first
    e = lax.broadcasted_iota(jnp.int32, (rows, EXPERTS), 1)
    spread = jnp.where((r >> 4) == e, 1.0, 0.0).astype(BF16)
    wanted = dot(spread, keys)
    slot = ((lax.broadcasted_iota(jnp.int32, (rows, TOK), 0) + first) & 15).astype(F32)
    pick = jnp.where(wanted == slot, 1.0, 0.0).astype(BF16)
    out_ref[...] = dot(pick, tok_ref[...]).astype(BF16)


def dispatch(pos, ids_t, tokens):
    blocks = 2
    rows = SLOTS // blocks
    return pl.pallas_call(
        dispatch_kernel,
        grid_spec=pltpu.PrefetchScalarGridSpec(
            num_scalar_prefetch=1,
            grid=(blocks,),
            in_specs=[
                pl.BlockSpec(ids_t.shape, lambda i, p: (0, 0)),
                pl.BlockSpec((TOK, COLS), lambda i, p: (0, p[0])),
            ],
            out_specs=pl.BlockSpec((rows, COLS), lambda i, p: (i, 0)),
        ),
        out_shape=jax.ShapeDtypeStruct((SLOTS, COLS), BF16),
        name="dispatch",
    )(pos, ids_t, tokens)


def pack_kernel(gate_ref, up_ref, down_ref, out_ref):
    fs = out_ref.shape[2] // 3
    for x in range(NX):
        cut = slice(x * fs, (x + 1) * fs)
        out_ref[x] = jnp.concatenate([gate_ref[:, cut], up_ref[:, cut], down_ref[:, cut]], axis=1)


def pack(gate, up, down_t):
    fs = gate.shape[1] // NX
    return pl.pallas_call(
        pack_kernel,
        out_shape=jax.ShapeDtypeStruct((NX, gate.shape[0], 3 * fs), BF16),
        name="pack",
    )(gate, up, down_t)


def cut_kernel(pos_ref, a, b, c, out_a, out_b, out_c):
    del pos_ref
    out_a[...] = a[0]
    out_b[...] = b[0]
    out_c[...] = c[0]


def cut(pos, w_down):
    mf = w_down.shape[1]
    return pl.pallas_call(
        cut_kernel,
        grid_spec=pltpu.PrefetchScalarGridSpec(
            num_scalar_prefetch=1,
            grid=(1,),
            in_specs=[
                pl.BlockSpec((1, mf, COLS), lambda i, p: (0, 0, p[0] ^ 1)),
                pl.BlockSpec((1, mf, COLS), lambda i, p: (0, 0, p[0] ^ 2)),
                pl.BlockSpec((1, mf, COLS), lambda i, p: (0, 0, p[0] ^ 3)),
            ],
            out_specs=[pl.BlockSpec((mf, COLS), lambda i, p: (0, 0))] * 3,
        ),
        out_shape=[jax.ShapeDtypeStruct((mf, COLS), BF16)] * 3,
        name="cut",
    )(pos, w_down, w_down, w_down)


def hidden_kernel(pos_ref, x0, x1, x2, x3, g0, g1, g2, g3, u0, u1, u2, u3, out_ref):
    del pos_ref
    gate = jnp.zeros((x0.shape[0], g0.shape[1]), F32)
    up = gate
    for x, g, u in ((x0, g0, u0), (x1, g1, u1), (x2, g2, u2), (x3, g3, u3)):
        rows = x[...]
        gate = gate + dot_nt(rows, g[0])
        up = up + dot_nt(rows, u[0])
    mf = gate.shape[1]
    out_ref[:, :mf] = (silu(gate) * up).astype(BF16)
    out_ref[:, mf:] = jnp.zeros((gate.shape[0], out_ref.shape[1] - mf), BF16)


def expert_hidden(pos, chunk, own, core, y, both, w_gate, w_up):
    steps = CHUNK_ROWS // STEP_ROWS
    mf = w_gate.shape[1]
    padded = -(-mf // 128) * 128
    whole = pl.BlockSpec((STEP_ROWS, COLS), lambda i, p: (chunk * steps + i, 0))
    part = pl.BlockSpec((STEP_ROWS, COLS), lambda i, p: (i, 0))
    w_specs = [
        pl.BlockSpec((1, mf, COLS), lambda i, p: (0, 0, p[0])),
        pl.BlockSpec((1, mf, COLS), lambda i, p: (0, 0, p[0] ^ 1)),
        pl.BlockSpec((1, mf, COLS), lambda i, p: (0, 0, p[0] ^ 2)),
        pl.BlockSpec((1, mf, COLS), lambda i, p: (0, 0, p[0] ^ 3)),
    ]
    return pl.pallas_call(
        hidden_kernel,
        grid_spec=pltpu.PrefetchScalarGridSpec(
            num_scalar_prefetch=1,
            grid=(steps,),
            in_specs=[whole, whole, part, part] + w_specs + w_specs,
            out_specs=pl.BlockSpec((STEP_ROWS, padded), lambda i, p: (i, 0)),
        ),
        out_shape=jax.ShapeDtypeStruct((CHUNK_ROWS, padded), BF16),
        cost_estimate=pl.CostEstimate(
            flops=4 * CHUNK_ROWS * D * mf, bytes_accessed=6_000_000, transcendentals=CHUNK_ROWS * mf
        ),
        name="hidden",
    )(pos, own, core, y, both, *[w_gate] * 4, *[w_up] * 4)


def down_kernel(pos_ref, h0, h1, h2, h3, w0, w1, w2, w3, *rest):
    del pos_ref
    out_ref = rest[-1]
    mf = w1.shape[0]
    total = dot(h0[:, :mf], w0[0])
    for h, w in ((h1, w1), (h2, w2), (h3, w3)):
        total = total + dot(h[:, :mf], w[...])
    out_ref[...] = total.astype(BF16)


def expert_columns(pos, chunk, hiddens, w_own, w_others, so_far):
    steps = CHUNK_ROWS // STEP_ROWS
    mf = w_own.shape[1]
    h_spec = pl.BlockSpec((STEP_ROWS, hiddens[0].shape[1]), lambda i, p: (i, 0))
    w_spec = pl.BlockSpec((mf, COLS), lambda i, p: (0, 0))
    more = [] if so_far is None else [so_far]
    return pl.pallas_call(
        down_kernel,
        grid_spec=pltpu.PrefetchScalarGridSpec(
            num_scalar_prefetch=1,
            grid=(steps,),
            in_specs=[h_spec] * 4
            + [pl.BlockSpec((1, mf, COLS), lambda i, p: (0, 0, p[0]))]
            + [w_spec] * 3
            + [pl.BlockSpec(memory_space=pl.ANY)] * len(more),
            out_specs=pl.BlockSpec((STEP_ROWS, COLS), lambda i, p: (chunk * steps + i, 0)),
        ),
        out_shape=jax.ShapeDtypeStruct((SLOTS, COLS), BF16),
        input_output_aliases={9: 0} if more else {},
        cost_estimate=pl.CostEstimate(
            flops=8 * CHUNK_ROWS * COLS * mf, bytes_accessed=4_000_000, transcendentals=0
        ),
        name="down",
    )(pos, *hiddens, w_own, *w_others, *more)


def shared_kernel(pos_ref, t0, t1, t2, t3, w_ref, after_ref, keep_ref, send_ref):
    del after_ref
    core = pos_ref[0] & 1
    fs = w_ref.shape[3] // 3
    rows = w_ref.shape[0] * w_ref.shape[2]
    for d, tok_ref in enumerate((t0, t1, t2, t3)):
        total = jnp.zeros((TOK, 3 * fs), F32)
        for x in range(NX):
            w = w_ref[:, x].reshape(rows, 3 * fs)
            total = total + dot(tok_ref[:, x * rows : (x + 1) * rows], w)
        hidden = silu(total[:, :fs]) * total[:, fs : 2 * fs]
        hidden = jnp.concatenate([jnp.zeros((TOK, 2 * fs), F32), hidden], axis=1).astype(BF16)
        for half in range(2):
            for out_ref, at in ((keep_ref, core), (send_ref, 1 - core)):
                w = w_ref[:, pl.ds(2 * half + at, 1)].reshape(rows, 3 * fs)
                out_ref[d, :, half * 512 : (half + 1) * 512] = dot_nt(hidden, w).astype(BF16)


def shared_ffn(pos, toks, weights, after):
    fs3 = weights.shape[3]
    vmem = pl.BlockSpec(memory_space=pltpu.VMEM)
    return pl.pallas_call(
        shared_kernel,
        in_specs=[pl.BlockSpec(memory_space=pltpu.SMEM)] + [vmem] * 5 + [pl.BlockSpec(memory_space=pl.ANY)],
        out_specs=[vmem, vmem],
        out_shape=[jax.ShapeDtypeStruct((NX, TOK, D // 2), BF16)] * 2,
        cost_estimate=pl.CostEstimate(
            flops=2 * NX * TOK * D * fs3 * 2, bytes_accessed=6_000_000, transcendentals=NX * TOK * fs3 // 3
        ),
        name="shared",
    )(pos, *toks, weights, after)


def turned(values):
    row = lax.broadcasted_iota(jnp.int32, (TOK, TOK), 0)
    col = lax.broadcasted_iota(jnp.int32, (TOK, TOK), 1)
    eye = jnp.where(row == col, 1.0, 0.0).astype(BF16)
    total = None
    rest = values
    for _ in range(3):
        part = rest.astype(BF16)
        rest = rest - part.astype(F32)
        moved = dot_nt(eye, part)
        total = moved if total is None else total + moved
    return total


def fold_kernel(pos_ref, s0, s1, s2, s3, keep_ref, send_ref):
    total = s0[...].astype(F32)
    for one in (s1, s2, s3):
        total = total + one[...].astype(F32)
    low = total[:, :COLS]
    high = total[:, COLS:]
    first = pos_ref[0] < 2
    keep_ref[...] = jnp.where(first, low, high)
    send_ref[...] = jnp.where(first, high, low).astype(BF16)


def fold(pos, parts):
    vmem = pl.BlockSpec(memory_space=pltpu.VMEM)
    return pl.pallas_call(
        fold_kernel,
        in_specs=[pl.BlockSpec(memory_space=pltpu.SMEM)] + [vmem] * 4,
        out_specs=[vmem, vmem],
        out_shape=[jax.ShapeDtypeStruct((TOK, COLS), F32), jax.ShapeDtypeStruct((TOK, COLS), BF16)],
        name="fold",
    )(pos, *parts)


def combine_kernel(ids_ref, gw_ref, ret_ref, keep_ref, got_ref, out_ref):
    ids = turned(ids_ref[...].astype(F32))
    gates = turned(gw_ref[...])
    named = named_counts(ids, (TOK, EXPERTS), 1)
    place = dot(order_matrix(False), named.astype(BF16))
    keys = jnp.where(named > 0.0, place, NO_SLOT).astype(BF16)
    lane = lax.broadcasted_iota(jnp.int32, (TOK, EXPERTS), 1).astype(F32)
    weight = jnp.zeros((TOK, EXPERTS), F32)
    for k in range(ids.shape[1]):
        weight = weight + jnp.where(ids[:, k : k + 1] == lane, gates[:, k : k + 1], 0.0)
    e = lax.broadcasted_iota(jnp.int32, (EXPERTS, SLOTS), 0)
    r = lax.broadcasted_iota(jnp.int32, (EXPERTS, SLOTS), 1)
    spread = jnp.where((r >> 4) == e, 1.0, 0.0).astype(BF16)
    slot = (lax.broadcasted_iota(jnp.int32, (TOK, SLOTS), 1) & 15).astype(F32)
    hit = dot(keys, spread) == slot
    ret = ret_ref[...]
    total = keep_ref[...] + got_ref[...].astype(F32)
    rest = weight
    for _ in range(3):
        part = rest.astype(BF16)
        rest = rest - part.astype(F32)
        row = jnp.where(hit, dot(part, spread), 0.0).astype(BF16)
        total = total + dot(row, ret)
    out_ref[...] = total.astype(BF16)


def combine(ids, gate_weights, returned, keep, got):
    return pl.pallas_call(
        combine_kernel,
        out_shape=jax.ShapeDtypeStruct((TOK, COLS), BF16),
        name="combine",
    )(ids, gate_weights, returned, keep, got)


def body(
    tokens,
    expert_ids,
    gate_weights,
    shared_gate,
    shared_up,
    shared_down,
    expert_gate,
    expert_up,
    expert_down,
):
    pos = lax.axis_index("narrow").astype(jnp.int32).reshape(1)
    ids_t = expert_ids.T
    gates_t = gate_weights.T
    gate_t = expert_gate.transpose(0, 2, 1)
    up_t = expert_up.transpose(0, 2, 1)

    packed = pack(shared_gate, shared_up, shared_down.T)
    packed = lax.all_to_all(packed, "wide", 0, 0, axis_index_groups=X_GROUPS, tiled=True)
    weights = lax.all_gather(packed[None], "wide", axis=0, axis_index_groups=YZ_GROUPS, tiled=True)

    outgoing = dispatch(pos, ids_t, tokens).reshape(EXPERTS, CAP, COLS)
    own = lax.all_to_all(outgoing, "wide", 0, 0, tiled=True).reshape(SLOTS, COLS)
    toks = [tokens]
    cuts = cut(pos, expert_down)
    others = [
        lax.ppermute(w, "narrow", swap)
        for w, swap in zip(cuts, (CORE_SWAP, Y_SWAP, BOTH_SWAP))
    ]
    for d in range(1, NX):
        toks.append(lax.ppermute(tokens, "wide", x_shift(d)))

    ys = []
    for k in range(CHUNKS):
        ys.append(lax.ppermute(own[k * CHUNK_ROWS : (k + 1) * CHUNK_ROWS], "narrow", Y_SWAP))
    core = lax.ppermute(own, "narrow", CORE_SWAP)
    hiddens = []
    for k in range(CHUNKS):
        both = lax.ppermute(ys[k], "narrow", CORE_SWAP)
        hidden = expert_hidden(pos, k, own, core, ys[k], both, gate_t, up_t)
        hidden_y = lax.ppermute(hidden, "narrow", Y_SWAP)
        hidden_core = lax.ppermute(hidden, "narrow", CORE_SWAP)
        hiddens.append([hidden, hidden_core, hidden_y])
    mine, theirs = shared_ffn(pos, toks, weights, hiddens[-1][0])
    outputs = None
    for k in range(CHUNKS):
        hidden_both = lax.ppermute(hiddens[k][2], "narrow", CORE_SWAP)
        outputs = expert_columns(pos, k, hiddens[k] + [hidden_both], expert_down, others, outputs)
    returned = lax.all_to_all(outputs.reshape(EXPERTS, CAP, COLS), "wide", 0, 0, tiled=True)

    theirs = lax.ppermute(theirs, "narrow", CORE_SWAP)
    shared = []
    for d in range(NX):
        one = (mine[d].astype(F32) + theirs[d].astype(F32)).astype(BF16)
        if d > 0:
            one = lax.ppermute(one, "wide", x_shift(NX - d))
        shared.append(one)
    kept, sent = fold(pos, shared)
    got = lax.ppermute(sent, "narrow", Y_SWAP)
    return combine(ids_t, gates_t, returned.reshape(SLOTS, COLS), kept, got)


def solution(mesh):
    in_specs = (
        P("wide", None),
        P("wide", None),
        P("wide", None),
        P("wide", "narrow"),
        P("wide", "narrow"),
        P("narrow", "wide"),
        P("wide", None, "narrow"),
        P("wide", None, "narrow"),
        P("wide", "narrow", None),
    )
    out_specs = P("wide", "narrow")
    return jax.shard_map(body, mesh=mesh, in_specs=in_specs, out_specs=out_specs, check_vma=False)
```

```python
import jax
import jax.numpy as jnp
from jax import lax
from jax.experimental import pallas as pl
from jax.experimental.pallas import tpu as pltpu
from jax.sharding import PartitionSpec as P


F32 = jnp.float32
BF16 = jnp.bfloat16
CAP = 16
EXPERTS = 64
SLOTS = EXPERTS * CAP
TOK = 128
D = 2048
NX = 4
NY = 2
NZ = 8
CORE_SWAP = [(0, 1), (1, 0), (2, 3), (3, 2)]
Y_SWAP = [(0, 2), (2, 0), (1, 3), (3, 1)]
BOTH_SWAP = [(0, 3), (3, 0), (1, 2), (2, 1)]
COLS = D // 4
CHUNKS = 2
CHUNK_ROWS = SLOTS // CHUNKS
STEP_ROWS = 256
NO_SLOT = 100.0


def moved(dx, flip, dz):
    def index(x, y, z):
        return (x % NX * NY + y) * NZ + z % NZ

    return [
        (index(x, y, z), index(x + dx, y ^ flip, z + dz))
        for x in range(NX)
        for y in range(NY)
        for z in range(NZ)
    ]


def silu(v):
    return v / (1.0 + jnp.exp(-v))


def dot(a, b):
    return lax.dot_general(a, b, (((1,), (0,)), ((), ())), preferred_element_type=F32)


def dot_nt(a, b):
    return lax.dot_general(a, b, (((1,), (1,)), ((), ())), preferred_element_type=F32)


def named_counts(ids, shape, k_axis):
    expert = lax.broadcasted_iota(jnp.int32, shape, k_axis).astype(F32)
    named = jnp.zeros(shape, F32)
    for k in range(ids.shape[k_axis]):
        one = ids[:, k : k + 1] if k_axis else ids[k : k + 1, :]
        named = named + jnp.where(one == expert, 1.0, 0.0)
    return named


def order_matrix(upper):
    row = lax.broadcasted_iota(jnp.int32, (TOK, TOK), 0)
    col = lax.broadcasted_iota(jnp.int32, (TOK, TOK), 1)
    before = row < col if upper else col < row
    return jnp.where(before, 1.0, 0.0).astype(BF16)


def dispatch_kernel(pos_ref, ids_ref, tok_ref, out_ref):
    del pos_ref
    rows = out_ref.shape[0]
    first = pl.program_id(0) * rows
    named = named_counts(ids_ref[...].astype(F32), (EXPERTS, TOK), 0)
    place = dot(named.astype(BF16), order_matrix(True))
    keys = jnp.where(named > 0.0, place, NO_SLOT).astype(BF16)
    r = lax.broadcasted_iota(jnp.int32, (rows, EXPERTS), 0) + first
    e = lax.broadcasted_iota(jnp.int32, (rows, EXPERTS), 1)
    spread = jnp.where((r >> 4) == e, 1.0, 0.0).astype(BF16)
    wanted = dot(spread, keys)
    slot = ((lax.broadcasted_iota(jnp.int32, (rows, TOK), 0) + first) & 15).astype(F32)
    pick = jnp.where(wanted == slot, 1.0, 0.0).astype(BF16)
    out_ref[...] = dot(pick, tok_ref[...]).astype(BF16)


def dispatch(pos, ids_t, tokens):
    blocks = 2
    rows = SLOTS // blocks
    return pl.pallas_call(
        dispatch_kernel,
        grid_spec=pltpu.PrefetchScalarGridSpec(
            num_scalar_prefetch=1,
            grid=(blocks,),
            in_specs=[
                pl.BlockSpec(ids_t.shape, lambda i, p: (0, 0)),
                pl.BlockSpec((TOK, COLS), lambda i, p: (0, p[0])),
            ],
            out_specs=pl.BlockSpec((rows, COLS), lambda i, p: (i, 0)),
        ),
        out_shape=jax.ShapeDtypeStruct((SLOTS, COLS), BF16),
        name="dispatch",
    )(pos, ids_t, tokens)


def pack_kernel(place_ref, gate_ref, up_ref, down_ref, out_ref):
    fs = out_ref.shape[2] // 3
    for x in range(NX):
        cut = slice(x * fs, (x + 1) * fs)
        one = jnp.concatenate([gate_ref[:, cut], up_ref[:, cut], down_ref[:, cut]], axis=1)
        out_ref[pl.ds((x - place_ref[1]) & (NX - 1), 1)] = one[None]


def pack(place, gate, up, down_t):
    fs = gate.shape[1] // NX
    vmem = pl.BlockSpec(memory_space=pltpu.VMEM)
    return pl.pallas_call(
        pack_kernel,
        in_specs=[pl.BlockSpec(memory_space=pltpu.SMEM)] + [vmem] * 3,
        out_specs=vmem,
        out_shape=jax.ShapeDtypeStruct((NX, gate.shape[0], 3 * fs), BF16),
        name="pack",
    )(place, gate, up, down_t)


def cut_kernel(pos_ref, a, b, c, out_a, out_b, out_c):
    del pos_ref
    out_a[...] = a[0]
    out_b[...] = b[0]
    out_c[...] = c[0]


def cut(pos, w_down):
    mf = w_down.shape[1]
    return pl.pallas_call(
        cut_kernel,
        grid_spec=pltpu.PrefetchScalarGridSpec(
            num_scalar_prefetch=1,
            grid=(1,),
            in_specs=[
                pl.BlockSpec((1, mf, COLS), lambda i, p: (0, 0, p[0] ^ 1)),
                pl.BlockSpec((1, mf, COLS), lambda i, p: (0, 0, p[0] ^ 2)),
                pl.BlockSpec((1, mf, COLS), lambda i, p: (0, 0, p[0] ^ 3)),
            ],
            out_specs=[pl.BlockSpec((mf, COLS), lambda i, p: (0, 0))] * 3,
        ),
        out_shape=[jax.ShapeDtypeStruct((mf, COLS), BF16)] * 3,
        name="cut",
    )(pos, w_down, w_down, w_down)


def hidden_kernel(pos_ref, x0, x1, x2, x3, g0, g1, g2, g3, u0, u1, u2, u3, out_ref):
    del pos_ref
    gate = jnp.zeros((x0.shape[0], g0.shape[1]), F32)
    up = gate
    for x, g, u in ((x0, g0, u0), (x1, g1, u1), (x2, g2, u2), (x3, g3, u3)):
        rows = x[...]
        gate = gate + dot_nt(rows, g[0])
        up = up + dot_nt(rows, u[0])
    mf = gate.shape[1]
    out_ref[:, :mf] = (silu(gate) * up).astype(BF16)
    out_ref[:, mf:] = jnp.zeros((gate.shape[0], out_ref.shape[1] - mf), BF16)


def expert_hidden(pos, chunk, own, core, y, both, w_gate, w_up):
    steps = CHUNK_ROWS // STEP_ROWS
    mf = w_gate.shape[1]
    padded = -(-mf // 128) * 128
    whole = pl.BlockSpec((STEP_ROWS, COLS), lambda i, p: (chunk * steps + i, 0))
    part = pl.BlockSpec((STEP_ROWS, COLS), lambda i, p: (i, 0))
    w_specs = [
        pl.BlockSpec((1, mf, COLS), lambda i, p: (0, 0, p[0])),
        pl.BlockSpec((1, mf, COLS), lambda i, p: (0, 0, p[0] ^ 1)),
        pl.BlockSpec((1, mf, COLS), lambda i, p: (0, 0, p[0] ^ 2)),
        pl.BlockSpec((1, mf, COLS), lambda i, p: (0, 0, p[0] ^ 3)),
    ]
    return pl.pallas_call(
        hidden_kernel,
        grid_spec=pltpu.PrefetchScalarGridSpec(
            num_scalar_prefetch=1,
            grid=(steps,),
            in_specs=[whole, whole, part, part] + w_specs + w_specs,
            out_specs=pl.BlockSpec((STEP_ROWS, padded), lambda i, p: (i, 0)),
        ),
        out_shape=jax.ShapeDtypeStruct((CHUNK_ROWS, padded), BF16),
        cost_estimate=pl.CostEstimate(
            flops=4 * CHUNK_ROWS * D * mf, bytes_accessed=6_000_000, transcendentals=CHUNK_ROWS * mf
        ),
        name="hidden",
    )(pos, own, core, y, both, *[w_gate] * 4, *[w_up] * 4)


def down_kernel(pos_ref, h0, h1, h2, h3, w0, w1, w2, w3, *rest):
    del pos_ref
    out_ref = rest[-1]
    mf = w1.shape[0]
    total = dot(h0[:, :mf], w0[0])
    for h, w in ((h1, w1), (h2, w2), (h3, w3)):
        total = total + dot(h[:, :mf], w[...])
    out_ref[...] = total.astype(BF16)


def expert_columns(pos, chunk, hiddens, w_own, w_others, so_far):
    steps = CHUNK_ROWS // STEP_ROWS
    mf = w_own.shape[1]
    h_spec = pl.BlockSpec((STEP_ROWS, hiddens[0].shape[1]), lambda i, p: (i, 0))
    w_spec = pl.BlockSpec((mf, COLS), lambda i, p: (0, 0))
    more = [] if so_far is None else [so_far]
    return pl.pallas_call(
        down_kernel,
        grid_spec=pltpu.PrefetchScalarGridSpec(
            num_scalar_prefetch=1,
            grid=(steps,),
            in_specs=[h_spec] * 4
            + [pl.BlockSpec((1, mf, COLS), lambda i, p: (0, 0, p[0]))]
            + [w_spec] * 3
            + [pl.BlockSpec(memory_space=pl.ANY)] * len(more),
            out_specs=pl.BlockSpec((STEP_ROWS, COLS), lambda i, p: (chunk * steps + i, 0)),
        ),
        out_shape=jax.ShapeDtypeStruct((SLOTS, COLS), BF16),
        input_output_aliases={9: 0} if more else {},
        cost_estimate=pl.CostEstimate(
            flops=8 * CHUNK_ROWS * COLS * mf, bytes_accessed=4_000_000, transcendentals=0
        ),
        name="down",
    )(pos, *hiddens, w_own, *w_others, *more)


def shared_kernel(place_ref, t0, t1, t2, t3, *refs):
    blocks, (keep_ref, send_ref, w_ref, sems) = refs[:9], refs[10:]
    core, x, y, z = place_ref[0] & 1, place_ref[1], place_ref[2], place_ref[3]
    copies = []
    for j, (block, step) in enumerate(zip(blocks, (0, 1, 2, 3, 4, 4, 5, 6, 7))):
        to = w_ref.at[(z - step) & (NZ - 1)]
        if block.shape[0] < w_ref.shape[1]:
            first = 0 if j == 4 else block.shape[0]
            to = to.at[pl.ds(first, block.shape[0])]
        copies.append(pltpu.make_async_copy(block, to, sems.at[j]))
    for copy in copies:
        copy.start()
    for copy in copies:
        copy.wait()
    fs3 = w_ref.shape[3]
    fs = fs3 // 3
    rows = NZ * w_ref.shape[2]

    def columns(quarter, half):
        at = ((x - quarter) & (NX - 1)) * NY + (half ^ y)
        return w_ref[:, pl.ds(at, 1)].reshape(rows, fs3)

    toks = (t0, t1, t2, t3)
    totals = [jnp.zeros((TOK, fs3), F32) for _ in toks]
    for quarter in range(NX):
        for half in range(NY):
            w = columns(quarter, half)
            first = (quarter * NY + half) * rows
            for d, tok_ref in enumerate(toks):
                totals[d] = totals[d] + dot(tok_ref[:, first : first + rows], w)
    hidden = []
    for total in totals:
        one = silu(total[:, :fs]) * total[:, fs : 2 * fs]
        hidden.append(jnp.concatenate([jnp.zeros((TOK, 2 * fs), F32), one], axis=1).astype(BF16))
    for side in range(2):
        for half in range(NY):
            cut = slice((side * NY + half) * rows, (side * NY + half + 1) * rows)
            for out_ref, at in ((keep_ref, core), (send_ref, 1 - core)):
                w = columns(2 * side + at, half)
                for d in range(NX):
                    out_ref[d, :, cut] = dot_nt(hidden[d], w).astype(BF16)


def shared_ffn(place, toks, blocks, after):
    fs3 = blocks[0].shape[2]
    vmem = pl.BlockSpec(memory_space=pltpu.VMEM)
    return pl.pallas_call(
        shared_kernel,
        in_specs=[pl.BlockSpec(memory_space=pltpu.SMEM)]
        + [vmem] * 4
        + [pl.BlockSpec(memory_space=pl.ANY)] * 10,
        out_specs=[vmem, vmem],
        out_shape=[jax.ShapeDtypeStruct((NX, TOK, D // 2), BF16)] * 2,
        scratch_shapes=[
            pltpu.VMEM((NZ,) + blocks[0].shape, BF16),
            pltpu.SemaphoreType.DMA((9,)),
        ],
        cost_estimate=pl.CostEstimate(
            flops=2 * NX * TOK * D * fs3 * 2, bytes_accessed=6_000_000, transcendentals=NX * TOK * fs3 // 3
        ),
        name="shared",
    )(place, *toks, *blocks, after)


def turned(values):
    row = lax.broadcasted_iota(jnp.int32, (TOK, TOK), 0)
    col = lax.broadcasted_iota(jnp.int32, (TOK, TOK), 1)
    eye = jnp.where(row == col, 1.0, 0.0).astype(BF16)
    total = None
    rest = values
    for _ in range(3):
        part = rest.astype(BF16)
        rest = rest - part.astype(F32)
        moved = dot_nt(eye, part)
        total = moved if total is None else total + moved
    return total


def fold_kernel(pos_ref, s0, s1, s2, s3, keep_ref, send_ref):
    total = s0[...].astype(F32)
    for one in (s1, s2, s3):
        total = total + one[...].astype(F32)
    low = total[:, :COLS]
    high = total[:, COLS:]
    first = pos_ref[0] < 2
    keep_ref[...] = jnp.where(first, low, high)
    send_ref[...] = jnp.where(first, high, low).astype(BF16)


def fold(pos, parts):
    vmem = pl.BlockSpec(memory_space=pltpu.VMEM)
    return pl.pallas_call(
        fold_kernel,
        in_specs=[pl.BlockSpec(memory_space=pltpu.SMEM)] + [vmem] * 4,
        out_specs=[vmem, vmem],
        out_shape=[jax.ShapeDtypeStruct((TOK, COLS), F32), jax.ShapeDtypeStruct((TOK, COLS), BF16)],
        name="fold",
    )(pos, *parts)


def combine_kernel(ids_ref, gw_ref, ret_ref, keep_ref, got_ref, out_ref):
    ids = turned(ids_ref[...].astype(F32))
    gates = turned(gw_ref[...])
    named = named_counts(ids, (TOK, EXPERTS), 1)
    place = dot(order_matrix(False), named.astype(BF16))
    keys = jnp.where(named > 0.0, place, NO_SLOT).astype(BF16)
    lane = lax.broadcasted_iota(jnp.int32, (TOK, EXPERTS), 1).astype(F32)
    weight = jnp.zeros((TOK, EXPERTS), F32)
    for k in range(ids.shape[1]):
        weight = weight + jnp.where(ids[:, k : k + 1] == lane, gates[:, k : k + 1], 0.0)
    e = lax.broadcasted_iota(jnp.int32, (EXPERTS, SLOTS), 0)
    r = lax.broadcasted_iota(jnp.int32, (EXPERTS, SLOTS), 1)
    spread = jnp.where((r >> 4) == e, 1.0, 0.0).astype(BF16)
    slot = (lax.broadcasted_iota(jnp.int32, (TOK, SLOTS), 1) & 15).astype(F32)
    hit = dot(keys, spread) == slot
    ret = ret_ref[...]
    total = keep_ref[...] + got_ref[...].astype(F32)
    rest = weight
    for _ in range(3):
        part = rest.astype(BF16)
        rest = rest - part.astype(F32)
        row = jnp.where(hit, dot(part, spread), 0.0).astype(BF16)
        total = total + dot(row, ret)
    out_ref[...] = total.astype(BF16)


def combine(ids, gate_weights, returned, keep, got):
    return pl.pallas_call(
        combine_kernel,
        out_shape=jax.ShapeDtypeStruct((TOK, COLS), BF16),
        name="combine",
    )(ids, gate_weights, returned, keep, got)


def body(
    tokens,
    expert_ids,
    gate_weights,
    shared_gate,
    shared_up,
    shared_down,
    expert_gate,
    expert_up,
    expert_down,
):
    pos = lax.axis_index("narrow").astype(jnp.int32).reshape(1)
    ids_t = expert_ids.T
    gates_t = gate_weights.T
    gate_t = expert_gate.transpose(0, 2, 1)
    up_t = expert_up.transpose(0, 2, 1)

    wide = lax.axis_index("wide").astype(jnp.int32)
    place = jnp.stack([pos[0], wide >> 4, (wide >> 3) & 1, wide & 7])

    outgoing = dispatch(pos, ids_t, tokens).reshape(EXPERTS, CAP, COLS)
    own = lax.all_to_all(outgoing, "wide", 0, 0, tiled=True).reshape(SLOTS, COLS)

    pieces = pack(place, shared_gate, shared_up, shared_down.T)
    column = []
    for d in range(NX):
        for flip in range(NY):
            one = pieces[d]
            if d or flip:
                one = lax.ppermute(one, "wide", moved(d, flip, 0))
            column.append(one)
    column = jnp.stack(column)
    cuts = cut(pos, expert_down)
    toks = [tokens]
    others = [
        lax.ppermute(w, "narrow", swap)
        for w, swap in zip(cuts, (CORE_SWAP, Y_SWAP, BOTH_SWAP))
    ]
    for d in range(1, NX):
        toks.append(lax.ppermute(tokens, "wide", moved(d, 0, 0)))
    near = {k: lax.ppermute(column, "wide", moved(0, 0, k)) for k in (2, -2, 1, -1)}
    third = lax.ppermute(near[2], "wide", moved(0, 0, 1))
    fifth = lax.ppermute(near[-2], "wide", moved(0, 0, -1))
    fourth_a = lax.ppermute(near[2][:4], "wide", moved(0, 0, 2))
    fourth_b = lax.ppermute(near[-2][4:], "wide", moved(0, 0, -2))
    blocks = [column, near[1], near[2], third, fourth_a, fourth_b, fifth, near[-2], near[-1]]

    ys = []
    for k in range(CHUNKS):
        ys.append(lax.ppermute(own[k * CHUNK_ROWS : (k + 1) * CHUNK_ROWS], "narrow", Y_SWAP))
    core = lax.ppermute(own, "narrow", CORE_SWAP)
    hiddens = []
    for k in range(CHUNKS):
        both = lax.ppermute(ys[k], "narrow", CORE_SWAP)
        hidden = expert_hidden(pos, k, own, core, ys[k], both, gate_t, up_t)
        hidden_y = lax.ppermute(hidden, "narrow", Y_SWAP)
        hidden_core = lax.ppermute(hidden, "narrow", CORE_SWAP)
        hiddens.append([hidden, hidden_core, hidden_y])
    mine, theirs = shared_ffn(place, toks, blocks, hiddens[-1][0])
    outputs = None
    for k in range(CHUNKS):
        hidden_both = lax.ppermute(hiddens[k][2], "narrow", CORE_SWAP)
        outputs = expert_columns(pos, k, hiddens[k] + [hidden_both], expert_down, others, outputs)
    returned = lax.all_to_all(outputs.reshape(EXPERTS, CAP, COLS), "wide", 0, 0, tiled=True)

    theirs = lax.ppermute(theirs, "narrow", CORE_SWAP)
    shared = []
    for d in range(NX):
        one = (mine[d].astype(F32) + theirs[d].astype(F32)).astype(BF16)
        if d > 0:
            one = lax.ppermute(one, "wide", moved(-d, 0, 0))
        shared.append(one)
    kept, sent = fold(pos, shared)
    got = lax.ppermute(sent, "narrow", Y_SWAP)
    return combine(ids_t, gates_t, returned.reshape(SLOTS, COLS), kept, got)


def solution(mesh):
    in_specs = (
        P("wide", None),
        P("wide", None),
        P("wide", None),
        P("wide", "narrow"),
        P("wide", "narrow"),
        P("narrow", "wide"),
        P("wide", None, "narrow"),
        P("wide", None, "narrow"),
        P("wide", "narrow", None),
    )
    out_specs = P("wide", "narrow")
    return jax.shard_map(body, mesh=mesh, in_specs=in_specs, out_specs=out_specs, check_vma=False)
```

```python
import jax
import jax.numpy as jnp
from jax import lax
from jax.experimental import pallas as pl
from jax.experimental.pallas import tpu as pltpu
from jax.sharding import PartitionSpec as P


F32 = jnp.float32
BF16 = jnp.bfloat16
CAP = 16
EXPERTS = 64
SLOTS = EXPERTS * CAP
TOK = 128
D = 2048
NX = 4
NY = 2
NZ = 8
CORE_SWAP = [(0, 1), (1, 0), (2, 3), (3, 2)]
Y_SWAP = [(0, 2), (2, 0), (1, 3), (3, 1)]
BOTH_SWAP = [(0, 3), (3, 0), (1, 2), (2, 1)]
COLS = D // 4
CHUNKS = 2
CHUNK_ROWS = SLOTS // CHUNKS
STEP_ROWS = 256
NO_SLOT = 100.0


def moved(dx, flip, dz):
    def index(x, y, z):
        return (x % NX * NY + y) * NZ + z % NZ

    return [
        (index(x, y, z), index(x + dx, y ^ flip, z + dz))
        for x in range(NX)
        for y in range(NY)
        for z in range(NZ)
    ]


PLANES = [[xy * NZ + z for xy in range(NX * NY)] for z in range(NZ)]


def silu(v):
    return v / (1.0 + jnp.exp(-v))


def dot(a, b):
    return lax.dot_general(a, b, (((1,), (0,)), ((), ())), preferred_element_type=F32)


def dot_nt(a, b):
    return lax.dot_general(a, b, (((1,), (1,)), ((), ())), preferred_element_type=F32)


def named_counts(ids, shape, k_axis):
    expert = lax.broadcasted_iota(jnp.int32, shape, k_axis).astype(F32)
    named = jnp.zeros(shape, F32)
    for k in range(ids.shape[k_axis]):
        one = ids[:, k : k + 1] if k_axis else ids[k : k + 1, :]
        named = named + jnp.where(one == expert, 1.0, 0.0)
    return named


def order_matrix(upper):
    row = lax.broadcasted_iota(jnp.int32, (TOK, TOK), 0)
    col = lax.broadcasted_iota(jnp.int32, (TOK, TOK), 1)
    before = row < col if upper else col < row
    return jnp.where(before, 1.0, 0.0).astype(BF16)


def dispatch_kernel(pos_ref, ids_ref, tok_ref, out_ref):
    del pos_ref
    rows = out_ref.shape[0]
    first = pl.program_id(0) * rows
    named = named_counts(ids_ref[...].astype(F32), (EXPERTS, TOK), 0)
    place = dot(named.astype(BF16), order_matrix(True))
    keys = jnp.where(named > 0.0, place, NO_SLOT).astype(BF16)
    r = lax.broadcasted_iota(jnp.int32, (rows, EXPERTS), 0) + first
    e = lax.broadcasted_iota(jnp.int32, (rows, EXPERTS), 1)
    spread = jnp.where((r >> 4) == e, 1.0, 0.0).astype(BF16)
    wanted = dot(spread, keys)
    slot = ((lax.broadcasted_iota(jnp.int32, (rows, TOK), 0) + first) & 15).astype(F32)
    pick = jnp.where(wanted == slot, 1.0, 0.0).astype(BF16)
    out_ref[...] = dot(pick, tok_ref[...]).astype(BF16)


def dispatch(pos, ids_t, tokens):
    blocks = 2
    rows = SLOTS // blocks
    return pl.pallas_call(
        dispatch_kernel,
        grid_spec=pltpu.PrefetchScalarGridSpec(
            num_scalar_prefetch=1,
            grid=(blocks,),
            in_specs=[
                pl.BlockSpec(ids_t.shape, lambda i, p: (0, 0)),
                pl.BlockSpec((TOK, COLS), lambda i, p: (0, p[0])),
            ],
            out_specs=pl.BlockSpec((rows, COLS), lambda i, p: (i, 0)),
        ),
        out_shape=jax.ShapeDtypeStruct((SLOTS, COLS), BF16),
        name="dispatch",
    )(pos, ids_t, tokens)


def pack_kernel(gate_ref, up_ref, down_ref, out_ref):
    fs = out_ref.shape[2] // 3
    for x in range(NX):
        cut = slice(x * fs, (x + 1) * fs)
        one = jnp.concatenate([gate_ref[:, cut], up_ref[:, cut], down_ref[:, cut]], axis=1)
        for y in range(NY):
            out_ref[x * NY + y] = one


def pack(gate, up, down_t):
    fs = gate.shape[1] // NX
    return pl.pallas_call(
        pack_kernel,
        out_shape=jax.ShapeDtypeStruct((NX * NY, gate.shape[0], 3 * fs), BF16),
        name="pack",
    )(gate, up, down_t)


def cut_kernel(pos_ref, a, b, c, out_a, out_b, out_c):
    del pos_ref
    out_a[...] = a[0]
    out_b[...] = b[0]
    out_c[...] = c[0]


def cut(pos, w_down):
    mf = w_down.shape[1]
    return pl.pallas_call(
        cut_kernel,
        grid_spec=pltpu.PrefetchScalarGridSpec(
            num_scalar_prefetch=1,
            grid=(1,),
            in_specs=[
                pl.BlockSpec((1, mf, COLS), lambda i, p: (0, 0, p[0] ^ 2)),
                pl.BlockSpec((1, mf, COLS), lambda i, p: (0, 0, p[0] ^ 3)),
                pl.BlockSpec((1, mf, COLS), lambda i, p: (0, 0, p[0] ^ 1)),
            ],
            out_specs=[pl.BlockSpec((mf, COLS), lambda i, p: (0, 0))] * 3,
        ),
        out_shape=[jax.ShapeDtypeStruct((mf, COLS), BF16)] * 3,
        name="cut",
    )(pos, w_down, w_down, w_down)


def hidden_kernel(pos_ref, x0, x1, x2, x3, g0, g1, g2, g3, u0, u1, u2, u3, out_ref):
    del pos_ref
    gate = jnp.zeros((x0.shape[0], g0.shape[1]), F32)
    up = gate
    for x, g, u in ((x0, g0, u0), (x1, g1, u1), (x2, g2, u2), (x3, g3, u3)):
        rows = x[...]
        gate = gate + dot_nt(rows, g[0])
        up = up + dot_nt(rows, u[0])
    mf = gate.shape[1]
    out_ref[:, :mf] = (silu(gate) * up).astype(BF16)
    out_ref[:, mf:] = jnp.zeros((gate.shape[0], out_ref.shape[1] - mf), BF16)


def expert_hidden(pos, chunk, own, core, y, both, w_gate, w_up):
    steps = CHUNK_ROWS // STEP_ROWS
    mf = w_gate.shape[1]
    padded = -(-mf // 128) * 128
    whole = pl.BlockSpec((STEP_ROWS, COLS), lambda i, p: (chunk * steps + i, 0))
    part = pl.BlockSpec((STEP_ROWS, COLS), lambda i, p: (i, 0))
    w_specs = [
        pl.BlockSpec((1, mf, COLS), lambda i, p: (0, 0, p[0])),
        pl.BlockSpec((1, mf, COLS), lambda i, p: (0, 0, p[0] ^ 1)),
        pl.BlockSpec((1, mf, COLS), lambda i, p: (0, 0, p[0] ^ 2)),
        pl.BlockSpec((1, mf, COLS), lambda i, p: (0, 0, p[0] ^ 3)),
    ]
    return pl.pallas_call(
        hidden_kernel,
        grid_spec=pltpu.PrefetchScalarGridSpec(
            num_scalar_prefetch=1,
            grid=(steps,),
            in_specs=[whole, whole, part, part] + w_specs + w_specs,
            out_specs=pl.BlockSpec((STEP_ROWS, padded), lambda i, p: (i, 0)),
        ),
        out_shape=jax.ShapeDtypeStruct((CHUNK_ROWS, padded), BF16),
        cost_estimate=pl.CostEstimate(
            flops=4 * CHUNK_ROWS * D * mf, bytes_accessed=6_000_000, transcendentals=CHUNK_ROWS * mf
        ),
        name="hidden",
    )(pos, own, core, y, both, *[w_gate] * 4, *[w_up] * 4)


def down_kernel(pos_ref, h0, h1, h2, h3, w0, w1, w2, w3, *rest):
    del pos_ref
    out_ref = rest[-1]
    mf = w1.shape[0]
    total = dot(h0[:, :mf], w0[0])
    for h, w in ((h1, w1), (h2, w2), (h3, w3)):
        total = total + dot(h[:, :mf], w[...])
    out_ref[...] = total.astype(BF16)


def expert_columns(pos, chunk, hiddens, w_own, w_others, so_far):
    steps = CHUNK_ROWS // STEP_ROWS
    mf = w_own.shape[1]
    h_spec = pl.BlockSpec((STEP_ROWS, hiddens[0].shape[1]), lambda i, p: (i, 0))
    w_spec = pl.BlockSpec((mf, COLS), lambda i, p: (0, 0))
    more = [] if so_far is None else [so_far]
    return pl.pallas_call(
        down_kernel,
        grid_spec=pltpu.PrefetchScalarGridSpec(
            num_scalar_prefetch=1,
            grid=(steps,),
            in_specs=[h_spec] * 4
            + [pl.BlockSpec((1, mf, COLS), lambda i, p: (0, 0, p[0]))]
            + [w_spec] * 3
            + [pl.BlockSpec(memory_space=pl.ANY)] * len(more),
            out_specs=pl.BlockSpec((STEP_ROWS, COLS), lambda i, p: (chunk * steps + i, 0)),
        ),
        out_shape=jax.ShapeDtypeStruct((SLOTS, COLS), BF16),
        input_output_aliases={9: 0} if more else {},
        cost_estimate=pl.CostEstimate(
            flops=8 * CHUNK_ROWS * COLS * mf, bytes_accessed=4_000_000, transcendentals=0
        ),
        name="down",
    )(pos, *hiddens, w_own, *w_others, *more)


def shared_kernel(place_ref, t0, t1, t2, t3, *refs):
    blocks, (keep_ref, send_ref, w_ref, sems) = refs[:NZ], refs[NZ + 1 :]
    core, z = place_ref[0] & 1, place_ref[1]
    copies = []
    for step, block in enumerate(blocks):
        to = w_ref.at[(z - step) & (NZ - 1)]
        copies.append(pltpu.make_async_copy(block, to, sems.at[step]))
    for copy in copies:
        copy.start()
    for copy in copies:
        copy.wait()
    fs3 = w_ref.shape[3]
    fs = fs3 // 3
    rows = NZ * w_ref.shape[2]

    def columns(quarter, half):
        return w_ref[:, pl.ds(quarter * NY + half, 1)].reshape(rows, fs3)

    toks = (t0, t1, t2, t3)
    totals = [jnp.zeros((TOK, fs3), F32) for _ in toks]
    for quarter in range(NX):
        for half in range(NY):
            w = columns(quarter, half)
            first = (quarter * NY + half) * rows
            for d, tok_ref in enumerate(toks):
                totals[d] = totals[d] + dot(tok_ref[:, first : first + rows], w)
    hidden = []
    for total in totals:
        one = silu(total[:, :fs]) * total[:, fs : 2 * fs]
        hidden.append(jnp.concatenate([jnp.zeros((TOK, 2 * fs), F32), one], axis=1).astype(BF16))
    for side in range(2):
        for half in range(NY):
            cut = slice((side * NY + half) * rows, (side * NY + half + 1) * rows)
            for out_ref, at in ((keep_ref, core), (send_ref, 1 - core)):
                w = columns(2 * side + at, half)
                for d in range(NX):
                    out_ref[d, :, cut] = dot_nt(hidden[d], w).astype(BF16)


def shared_ffn(place, toks, blocks, after):
    fs3 = blocks[0].shape[2]
    vmem = pl.BlockSpec(memory_space=pltpu.VMEM)
    return pl.pallas_call(
        shared_kernel,
        in_specs=[pl.BlockSpec(memory_space=pltpu.SMEM)]
        + [vmem] * 4
        + [pl.BlockSpec(memory_space=pl.ANY)] * (NZ + 1),
        out_specs=[vmem, vmem],
        out_shape=[jax.ShapeDtypeStruct((NX, TOK, D // 2), BF16)] * 2,
        scratch_shapes=[
            pltpu.VMEM((NZ,) + blocks[0].shape, BF16),
            pltpu.SemaphoreType.DMA((NZ,)),
        ],
        cost_estimate=pl.CostEstimate(
            flops=2 * NX * TOK * D * fs3 * 2, bytes_accessed=6_000_000, transcendentals=NX * TOK * fs3 // 3
        ),
        name="shared",
    )(place, *toks, *blocks, after)


def turned(values):
    row = lax.broadcasted_iota(jnp.int32, (TOK, TOK), 0)
    col = lax.broadcasted_iota(jnp.int32, (TOK, TOK), 1)
    eye = jnp.where(row == col, 1.0, 0.0).astype(BF16)
    total = None
    rest = values
    for _ in range(3):
        part = rest.astype(BF16)
        rest = rest - part.astype(F32)
        moved = dot_nt(eye, part)
        total = moved if total is None else total + moved
    return total


def fold_kernel(pos_ref, s0, s1, s2, s3, keep_ref, send_ref):
    total = s0[...].astype(F32)
    for one in (s1, s2, s3):
        total = total + one[...].astype(F32)
    low = total[:, :COLS]
    high = total[:, COLS:]
    first = pos_ref[0] < 2
    keep_ref[...] = jnp.where(first, low, high)
    send_ref[...] = jnp.where(first, high, low).astype(BF16)


def fold(pos, parts):
    vmem = pl.BlockSpec(memory_space=pltpu.VMEM)
    return pl.pallas_call(
        fold_kernel,
        in_specs=[pl.BlockSpec(memory_space=pltpu.SMEM)] + [vmem] * 4,
        out_specs=[vmem, vmem],
        out_shape=[jax.ShapeDtypeStruct((TOK, COLS), F32), jax.ShapeDtypeStruct((TOK, COLS), BF16)],
        name="fold",
    )(pos, *parts)


def combine_kernel(ids_ref, gw_ref, ret_ref, keep_ref, got_ref, out_ref):
    ids = turned(ids_ref[...].astype(F32))
    gates = turned(gw_ref[...])
    named = named_counts(ids, (TOK, EXPERTS), 1)
    place = dot(order_matrix(False), named.astype(BF16))
    keys = jnp.where(named > 0.0, place, NO_SLOT).astype(BF16)
    lane = lax.broadcasted_iota(jnp.int32, (TOK, EXPERTS), 1).astype(F32)
    weight = jnp.zeros((TOK, EXPERTS), F32)
    for k in range(ids.shape[1]):
        weight = weight + jnp.where(ids[:, k : k + 1] == lane, gates[:, k : k + 1], 0.0)
    e = lax.broadcasted_iota(jnp.int32, (EXPERTS, SLOTS), 0)
    r = lax.broadcasted_iota(jnp.int32, (EXPERTS, SLOTS), 1)
    spread = jnp.where((r >> 4) == e, 1.0, 0.0).astype(BF16)
    slot = (lax.broadcasted_iota(jnp.int32, (TOK, SLOTS), 1) & 15).astype(F32)
    hit = dot(keys, spread) == slot
    ret = ret_ref[...]
    total = keep_ref[...] + got_ref[...].astype(F32)
    rest = weight
    for _ in range(3):
        part = rest.astype(BF16)
        rest = rest - part.astype(F32)
        row = jnp.where(hit, dot(part, spread), 0.0).astype(BF16)
        total = total + dot(row, ret)
    out_ref[...] = total.astype(BF16)


def combine(ids, gate_weights, returned, keep, got):
    return pl.pallas_call(
        combine_kernel,
        out_shape=jax.ShapeDtypeStruct((TOK, COLS), BF16),
        name="combine",
    )(ids, gate_weights, returned, keep, got)


def body(
    tokens,
    expert_ids,
    gate_weights,
    shared_gate,
    shared_up,
    shared_down,
    expert_gate,
    expert_up,
    expert_down,
):
    pos = lax.axis_index("narrow").astype(jnp.int32).reshape(1)
    ids_t = expert_ids.T
    gates_t = gate_weights.T
    gate_t = expert_gate.transpose(0, 2, 1)
    up_t = expert_up.transpose(0, 2, 1)

    place = jnp.stack([pos[0], lax.axis_index("wide").astype(jnp.int32) & (NZ - 1)])

    pieces = pack(shared_gate, shared_up, shared_down.T)
    column = lax.all_to_all(pieces, "wide", 0, 0, axis_index_groups=PLANES, tiled=True)

    outgoing = dispatch(pos, ids_t, tokens).reshape(EXPERTS, CAP, COLS)
    own = lax.all_to_all(outgoing, "wide", 0, 0, tiled=True).reshape(SLOTS, COLS)

    cuts = cut(pos, expert_down)
    others = [
        lax.ppermute(w, "narrow", swap)
        for w, swap in zip(cuts, (Y_SWAP, BOTH_SWAP, CORE_SWAP))
    ]
    near = {k: lax.ppermute(column, "wide", moved(0, 0, k)) for k in (2, -2, 1, -1)}
    toks = [tokens]
    for d in range(1, NX):
        toks.append(lax.ppermute(tokens, "wide", moved(d, 0, 0)))
    third = lax.ppermute(near[2], "wide", moved(0, 0, 1))
    fourth = lax.ppermute(near[2], "wide", moved(0, 0, 2))
    fifth = lax.ppermute(near[-2], "wide", moved(0, 0, -1))
    blocks = [column, near[1], near[2], third, fourth, fifth, near[-2], near[-1]]

    ys = []
    for k in range(CHUNKS):
        ys.append(lax.ppermute(own[k * CHUNK_ROWS : (k + 1) * CHUNK_ROWS], "narrow", Y_SWAP))
    core = lax.ppermute(own, "narrow", CORE_SWAP)
    hiddens = []
    for k in range(CHUNKS):
        both = lax.ppermute(ys[k], "narrow", CORE_SWAP)
        hidden = expert_hidden(pos, k, own, core, ys[k], both, gate_t, up_t)
        hidden_y = lax.ppermute(hidden, "narrow", Y_SWAP)
        hidden_core = lax.ppermute(hidden, "narrow", CORE_SWAP)
        hiddens.append([hidden, hidden_y, hidden_core])
    mine, theirs = shared_ffn(place, toks, blocks, hiddens[-1][0])
    theirs = lax.ppermute(theirs, "narrow", CORE_SWAP)
    shared = []
    for d in range(NX):
        one = (mine[d].astype(F32) + theirs[d].astype(F32)).astype(BF16)
        if d > 0:
            one = lax.ppermute(one, "wide", moved(-d, 0, 0))
        shared.append(one)
    outputs = None
    for k in range(CHUNKS):
        hidden_both = lax.ppermute(hiddens[k][1], "narrow", CORE_SWAP)
        hiddens[k].insert(2, hidden_both)
        outputs = expert_columns(pos, k, hiddens[k], expert_down, others, outputs)
    returned = lax.all_to_all(outputs.reshape(EXPERTS, CAP, COLS), "wide", 0, 0, tiled=True)

    kept, sent = fold(pos, shared)
    got = lax.ppermute(sent, "narrow", Y_SWAP)
    return combine(ids_t, gates_t, returned.reshape(SLOTS, COLS), kept, got)


def solution(mesh):
    in_specs = (
        P("wide", None),
        P("wide", None),
        P("wide", None),
        P("wide", "narrow"),
        P("wide", "narrow"),
        P("narrow", "wide"),
        P("wide", None, "narrow"),
        P("wide", None, "narrow"),
        P("wide", "narrow", None),
    )
    out_specs = P("wide", "narrow")
    return jax.shard_map(body, mesh=mesh, in_specs=in_specs, out_specs=out_specs, check_vma=False)
```

```python
import jax
import jax.numpy as jnp
from jax import lax
from jax.experimental import pallas as pl
from jax.experimental.pallas import tpu as pltpu
from jax.sharding import PartitionSpec as P


F32 = jnp.float32
BF16 = jnp.bfloat16
CAP = 16
EXPERTS = 64
SLOTS = EXPERTS * CAP
TOK = 128
D = 2048
FS = 2816
NX = 4
NY = 2
NZ = 8
CORE_SWAP = [(0, 1), (1, 0), (2, 3), (3, 2)]
Y_SWAP = [(0, 2), (2, 0), (1, 3), (3, 1)]
BOTH_SWAP = [(0, 3), (3, 0), (1, 2), (2, 1)]
COLS = D // 4
CHUNKS = 2
CHUNK_ROWS = SLOTS // CHUNKS
STEP_ROWS = 256
NO_SLOT = 100.0


def moved(dx, flip, dz):
    def index(x, y, z):
        return (x % NX * NY + y) * NZ + z % NZ

    return [
        (index(x, y, z), index(x + dx, y ^ flip, z + dz))
        for x in range(NX)
        for y in range(NY)
        for z in range(NZ)
    ]


def turned_about(k):
    def index(x, y, z, n):
        return ((x * NY + y) * NZ + z) * 4 + n

    return [
        (index(x, y, z, n), index((n + k) % 4, y, z, x))
        for x in range(NX)
        for y in range(NY)
        for z in range(NZ)
        for n in range(4)
    ]


def silu(v):
    return v / (1.0 + jnp.exp(-v))


def dot(a, b):
    return lax.dot_general(a, b, (((1,), (0,)), ((), ())), preferred_element_type=F32)


def dot_nt(a, b):
    return lax.dot_general(a, b, (((1,), (1,)), ((), ())), preferred_element_type=F32)


def named_counts(ids, shape, k_axis):
    expert = lax.broadcasted_iota(jnp.int32, shape, k_axis).astype(F32)
    named = jnp.zeros(shape, F32)
    for k in range(ids.shape[k_axis]):
        one = ids[:, k : k + 1] if k_axis else ids[k : k + 1, :]
        named = named + jnp.where(one == expert, 1.0, 0.0)
    return named


def order_matrix(upper):
    row = lax.broadcasted_iota(jnp.int32, (TOK, TOK), 0)
    col = lax.broadcasted_iota(jnp.int32, (TOK, TOK), 1)
    before = row < col if upper else col < row
    return jnp.where(before, 1.0, 0.0).astype(BF16)


def dispatch_kernel(pos_ref, ids_ref, tok_ref, out_ref):
    del pos_ref
    rows = out_ref.shape[0]
    first = pl.program_id(0) * rows
    named = named_counts(ids_ref[...].astype(F32), (EXPERTS, TOK), 0)
    place = dot(named.astype(BF16), order_matrix(True))
    keys = jnp.where(named > 0.0, place, NO_SLOT).astype(BF16)
    r = lax.broadcasted_iota(jnp.int32, (rows, EXPERTS), 0) + first
    e = lax.broadcasted_iota(jnp.int32, (rows, EXPERTS), 1)
    spread = jnp.where((r >> 4) == e, 1.0, 0.0).astype(BF16)
    wanted = dot(spread, keys)
    slot = ((lax.broadcasted_iota(jnp.int32, (rows, TOK), 0) + first) & 15).astype(F32)
    pick = jnp.where(wanted == slot, 1.0, 0.0).astype(BF16)
    out_ref[...] = dot(pick, tok_ref[...]).astype(BF16)


def dispatch(pos, ids_t, tokens):
    blocks = 2
    rows = SLOTS // blocks
    return pl.pallas_call(
        dispatch_kernel,
        grid_spec=pltpu.PrefetchScalarGridSpec(
            num_scalar_prefetch=1,
            grid=(blocks,),
            in_specs=[
                pl.BlockSpec(ids_t.shape, lambda i, p: (0, 0)),
                pl.BlockSpec((TOK, COLS), lambda i, p: (0, p[0])),
            ],
            out_specs=pl.BlockSpec((rows, COLS), lambda i, p: (i, 0)),
        ),
        out_shape=jax.ShapeDtypeStruct((SLOTS, COLS), BF16),
        name="dispatch",
    )(pos, ids_t, tokens)


def padded_to(value, lanes):
    return jnp.concatenate([value, jnp.zeros((value.shape[0], lanes - value.shape[1]), F32)], axis=1)


def chosen(parts, at):
    total = parts[-1]
    for i in range(len(parts) - 1):
        total = jnp.where(at == i, parts[i], total)
    return total


def pack_kernel(place_ref, gate_ref, up_ref, down_ref, *outs):
    n, x = place_ref[0], place_ref[1]
    fs = gate_ref.shape[1] // NX
    gate, up, down = gate_ref[...].astype(F32), up_ref[...].astype(F32), down_ref[...].astype(F32)
    inward, outward = [], []
    for i in range(NX):
        cut = slice(i * fs, (i + 1) * fs)
        both = jnp.concatenate([gate[:, cut], up[:, cut]], axis=1)
        inward.append(padded_to(both, outs[0].shape[1]))
        outward.append(padded_to(down[:, cut], outs[NX].shape[1]))
    for d in range(NX):
        outs[d][...] = chosen(inward, (x + d) & 3).astype(BF16)
        outs[NX + d][...] = chosen(outward, (n + d) & 3).astype(BF16)


def pack(place, gate, up, down_t):
    fs = gate.shape[1] // NX
    rows = gate.shape[0]
    vmem = pl.BlockSpec(memory_space=pltpu.VMEM)
    inward = jax.ShapeDtypeStruct((rows, -(-2 * fs // 128) * 128), BF16)
    outward = jax.ShapeDtypeStruct((rows, -(-fs // 128) * 128), BF16)
    return pl.pallas_call(
        pack_kernel,
        in_specs=[pl.BlockSpec(memory_space=pltpu.SMEM)] + [vmem] * 3,
        out_specs=[vmem] * 8,
        out_shape=[inward] * 4 + [outward] * 4,
        name="pack",
    )(place, gate, up, down_t)


def stack_kernel(place_ref, *refs):
    pieces, out_ref = refs[:8], refs[8]
    x = place_ref[1]
    lanes = pieces[0].shape[1]
    for d in range(NX):
        at = (x - d) & 3
        out_ref[pl.ds(at, 1), :, :lanes] = pieces[d][...][None]
        out_ref[pl.ds(at, 1), :, lanes:] = pieces[NX + d][...][None]


def stack(place, pieces):
    vmem = pl.BlockSpec(memory_space=pltpu.VMEM)
    lanes = pieces[0].shape[1] + pieces[NX].shape[1]
    return pl.pallas_call(
        stack_kernel,
        in_specs=[pl.BlockSpec(memory_space=pltpu.SMEM)] + [vmem] * 8,
        out_specs=vmem,
        out_shape=jax.ShapeDtypeStruct((NX, pieces[0].shape[0], lanes), BF16),
        name="stack",
    )(place, *pieces)


def cut_kernel(pos_ref, a, b, c, out_a, out_b, out_c):
    del pos_ref
    out_a[...] = a[0]
    out_b[...] = b[0]
    out_c[...] = c[0]


def cut(pos, w_down):
    mf = w_down.shape[1]
    return pl.pallas_call(
        cut_kernel,
        grid_spec=pltpu.PrefetchScalarGridSpec(
            num_scalar_prefetch=1,
            grid=(1,),
            in_specs=[
                pl.BlockSpec((1, mf, COLS), lambda i, p: (0, 0, p[0] ^ 2)),
                pl.BlockSpec((1, mf, COLS), lambda i, p: (0, 0, p[0] ^ 3)),
                pl.BlockSpec((1, mf, COLS), lambda i, p: (0, 0, p[0] ^ 1)),
            ],
            out_specs=[pl.BlockSpec((mf, COLS), lambda i, p: (0, 0))] * 3,
        ),
        out_shape=[jax.ShapeDtypeStruct((mf, COLS), BF16)] * 3,
        name="cut",
    )(pos, w_down, w_down, w_down)


def hidden_kernel(pos_ref, x0, x1, x2, x3, g0, g1, g2, g3, u0, u1, u2, u3, out_ref):
    del pos_ref
    gate = jnp.zeros((x0.shape[0], g0.shape[1]), F32)
    up = gate
    for x, g, u in ((x0, g0, u0), (x1, g1, u1), (x2, g2, u2), (x3, g3, u3)):
        rows = x[...]
        gate = gate + dot_nt(rows, g[0])
        up = up + dot_nt(rows, u[0])
    mf = gate.shape[1]
    out_ref[:, :mf] = (silu(gate) * up).astype(BF16)
    out_ref[:, mf:] = jnp.zeros((gate.shape[0], out_ref.shape[1] - mf), BF16)


def expert_hidden(pos, chunk, own, core, y, both, w_gate, w_up):
    steps = CHUNK_ROWS // STEP_ROWS
    mf = w_gate.shape[1]
    padded = -(-mf // 128) * 128
    whole = pl.BlockSpec((STEP_ROWS, COLS), lambda i, p: (chunk * steps + i, 0))
    part = pl.BlockSpec((STEP_ROWS, COLS), lambda i, p: (i, 0))
    w_specs = [
        pl.BlockSpec((1, mf, COLS), lambda i, p: (0, 0, p[0])),
        pl.BlockSpec((1, mf, COLS), lambda i, p: (0, 0, p[0] ^ 1)),
        pl.BlockSpec((1, mf, COLS), lambda i, p: (0, 0, p[0] ^ 2)),
        pl.BlockSpec((1, mf, COLS), lambda i, p: (0, 0, p[0] ^ 3)),
    ]
    return pl.pallas_call(
        hidden_kernel,
        grid_spec=pltpu.PrefetchScalarGridSpec(
            num_scalar_prefetch=1,
            grid=(steps,),
            in_specs=[whole, whole, part, part] + w_specs + w_specs,
            out_specs=pl.BlockSpec((STEP_ROWS, padded), lambda i, p: (i, 0)),
        ),
        out_shape=jax.ShapeDtypeStruct((CHUNK_ROWS, padded), BF16),
        cost_estimate=pl.CostEstimate(
            flops=4 * CHUNK_ROWS * D * mf, bytes_accessed=6_000_000, transcendentals=CHUNK_ROWS * mf
        ),
        name="hidden",
    )(pos, own, core, y, both, *[w_gate] * 4, *[w_up] * 4)


def down_kernel(pos_ref, h0, h1, h2, h3, w0, w1, w2, w3, *rest):
    del pos_ref
    out_ref = rest[-1]
    mf = w1.shape[0]
    total = dot(h0[:, :mf], w0[0])
    for h, w in ((h1, w1), (h2, w2), (h3, w3)):
        total = total + dot(h[:, :mf], w[...])
    out_ref[...] = total.astype(BF16)


def expert_columns(pos, chunk, hiddens, w_own, w_others, so_far):
    steps = CHUNK_ROWS // STEP_ROWS
    mf = w_own.shape[1]
    h_spec = pl.BlockSpec((STEP_ROWS, hiddens[0].shape[1]), lambda i, p: (i, 0))
    w_spec = pl.BlockSpec((mf, COLS), lambda i, p: (0, 0))
    more = [] if so_far is None else [so_far]
    return pl.pallas_call(
        down_kernel,
        grid_spec=pltpu.PrefetchScalarGridSpec(
            num_scalar_prefetch=1,
            grid=(steps,),
            in_specs=[h_spec] * 4
            + [pl.BlockSpec((1, mf, COLS), lambda i, p: (0, 0, p[0]))]
            + [w_spec] * 3
            + [pl.BlockSpec(memory_space=pl.ANY)] * len(more),
            out_specs=pl.BlockSpec((STEP_ROWS, COLS), lambda i, p: (chunk * steps + i, 0)),
        ),
        out_shape=jax.ShapeDtypeStruct((SLOTS, COLS), BF16),
        input_output_aliases={9: 0} if more else {},
        cost_estimate=pl.CostEstimate(
            flops=8 * CHUNK_ROWS * COLS * mf, bytes_accessed=4_000_000, transcendentals=0
        ),
        name="down",
    )(pos, *hiddens, w_own, *w_others, *more)


def fetch(blocks, w_ref, sems, z, first):
    copies = []
    for step, block in enumerate(blocks):
        part = block.at[:, :, :, pl.ds(first, w_ref.shape[4])]
        copies.append(pltpu.make_async_copy(part, w_ref.at[(z - step) & (NZ - 1)], sems.at[step]))
    for copy in copies:
        copy.start()
    for copy in copies:
        copy.wait()


def shared_hidden_kernel(place_ref, t0, t1, t2, t3, *refs):
    blocks, (out_ref, w_ref, sems) = refs[:NZ], refs[NZ + 1 :]
    y, z = place_ref[2], place_ref[3]
    fetch(blocks, w_ref, sems, z, 0)
    rows = NZ * w_ref.shape[3]
    lanes = w_ref.shape[4]
    fs = FS // (4 * NX)
    total = jnp.zeros((NX * TOK, lanes), F32)
    for quarter in range(NX):
        for half in range(NY):
            w = w_ref[:, pl.ds(half ^ y, 1), quarter].reshape(rows, lanes)
            first = (quarter * NY + half) * rows
            tok = jnp.concatenate([t[:, first : first + rows] for t in (t0, t1, t2, t3)], axis=0)
            total = total + dot(tok, w)
    hidden = silu(total[:, :fs]) * total[:, fs : 2 * fs]
    out_ref[...] = padded_to(hidden, out_ref.shape[1]).astype(BF16)


def shared_hidden(place, toks, blocks, after, lanes, units):
    vmem = pl.BlockSpec(memory_space=pltpu.VMEM)
    return pl.pallas_call(
        shared_hidden_kernel,
        in_specs=[pl.BlockSpec(memory_space=pltpu.SMEM)]
        + [vmem] * 4
        + [pl.BlockSpec(memory_space=pl.ANY)] * (NZ + 1),
        out_specs=vmem,
        out_shape=jax.ShapeDtypeStruct((NX * TOK, units), BF16),
        scratch_shapes=[
            pltpu.VMEM((NZ,) + blocks[0].shape[:3] + (lanes,), BF16),
            pltpu.SemaphoreType.DMA((NZ,)),
        ],
        cost_estimate=pl.CostEstimate(
            flops=2 * NX * TOK * D * lanes, bytes_accessed=5_000_000, transcendentals=NX * TOK * units
        ),
        name="shared_hidden",
    )(place, *toks, *blocks, after)


def shared_down_kernel(place_ref, h0, h1, h2, h3, *refs):
    blocks, outs, (w_ref, sems) = refs[:NZ], refs[NZ + 1 : NZ + 5], refs[NZ + 5 :]
    n, y, z = place_ref[0], place_ref[2], place_ref[3]
    units = w_ref.shape[4]
    fetch(blocks, w_ref, sems, z, blocks[0].shape[3] - units)
    rows = NZ * w_ref.shape[3]
    for half in range(NY):
        total = jnp.zeros((NX * TOK, rows), F32)
        for j, h in enumerate((h0, h1, h2, h3)):
            w = w_ref[:, pl.ds(half ^ y, 1), pl.ds(n ^ j, 1)].reshape(rows, units)
            total = total + dot_nt(h[...], w)
        for d in range(NX):
            outs[d][:, half * rows : (half + 1) * rows] = total[d * TOK : (d + 1) * TOK].astype(BF16)


def shared_columns(place, hiddens, blocks, after):
    vmem = pl.BlockSpec(memory_space=pltpu.VMEM)
    units = hiddens[0].shape[1]
    return pl.pallas_call(
        shared_down_kernel,
        in_specs=[pl.BlockSpec(memory_space=pltpu.SMEM)]
        + [vmem] * 4
        + [pl.BlockSpec(memory_space=pl.ANY)] * (NZ + 1),
        out_specs=[vmem] * 4,
        out_shape=[jax.ShapeDtypeStruct((TOK, COLS), BF16)] * 4,
        scratch_shapes=[
            pltpu.VMEM((NZ,) + blocks[0].shape[:3] + (units,), BF16),
            pltpu.SemaphoreType.DMA((NZ,)),
        ],
        cost_estimate=pl.CostEstimate(
            flops=2 * NX * TOK * D * units, bytes_accessed=4_000_000, transcendentals=0
        ),
        name="shared_down",
    )(place, *hiddens, *blocks, after)


def turned(values):
    row = lax.broadcasted_iota(jnp.int32, (TOK, TOK), 0)
    col = lax.broadcasted_iota(jnp.int32, (TOK, TOK), 1)
    eye = jnp.where(row == col, 1.0, 0.0).astype(BF16)
    total = None
    rest = values
    for _ in range(3):
        part = rest.astype(BF16)
        rest = rest - part.astype(F32)
        moved = dot_nt(eye, part)
        total = moved if total is None else total + moved
    return total


def combine_kernel(ids_ref, gw_ref, ret_ref, s0, s1, s2, s3, out_ref):
    ids = turned(ids_ref[...].astype(F32))
    gates = turned(gw_ref[...])
    named = named_counts(ids, (TOK, EXPERTS), 1)
    place = dot(order_matrix(False), named.astype(BF16))
    keys = jnp.where(named > 0.0, place, NO_SLOT).astype(BF16)
    lane = lax.broadcasted_iota(jnp.int32, (TOK, EXPERTS), 1).astype(F32)
    weight = jnp.zeros((TOK, EXPERTS), F32)
    for k in range(ids.shape[1]):
        weight = weight + jnp.where(ids[:, k : k + 1] == lane, gates[:, k : k + 1], 0.0)
    e = lax.broadcasted_iota(jnp.int32, (EXPERTS, SLOTS), 0)
    r = lax.broadcasted_iota(jnp.int32, (EXPERTS, SLOTS), 1)
    spread = jnp.where((r >> 4) == e, 1.0, 0.0).astype(BF16)
    slot = (lax.broadcasted_iota(jnp.int32, (TOK, SLOTS), 1) & 15).astype(F32)
    hit = dot(keys, spread) == slot
    ret = ret_ref[...]
    total = s0[...].astype(F32)
    for part in (s1, s2, s3):
        total = total + part[...].astype(F32)
    rest = weight
    for _ in range(3):
        part = rest.astype(BF16)
        rest = rest - part.astype(F32)
        row = jnp.where(hit, dot(part, spread), 0.0).astype(BF16)
        total = total + dot(row, ret)
    out_ref[...] = total.astype(BF16)


def combine(ids, gate_weights, returned, shared):
    return pl.pallas_call(
        combine_kernel,
        out_shape=jax.ShapeDtypeStruct((TOK, COLS), BF16),
        name="combine",
    )(ids, gate_weights, returned, *shared)


def body(
    tokens,
    expert_ids,
    gate_weights,
    shared_gate,
    shared_up,
    shared_down,
    expert_gate,
    expert_up,
    expert_down,
):
    pos = lax.axis_index("narrow").astype(jnp.int32).reshape(1)
    ids_t = expert_ids.T
    gates_t = gate_weights.T
    gate_t = expert_gate.transpose(0, 2, 1)
    up_t = expert_up.transpose(0, 2, 1)

    wide = lax.axis_index("wide").astype(jnp.int32)
    place = jnp.stack([pos[0], wide >> 4, (wide >> 3) & 1, wide & 7])

    outgoing = dispatch(pos, ids_t, tokens).reshape(EXPERTS, CAP, COLS)
    own = lax.all_to_all(outgoing, "wide", 0, 0, tiled=True).reshape(SLOTS, COLS)

    pieces = list(pack(place, shared_gate, shared_up, shared_down.T))
    for d in range(1, NX):
        pieces[d] = lax.ppermute(pieces[d], "wide", moved(d, 0, 0))
    for d in range(NX):
        pieces[NX + d] = lax.ppermute(pieces[NX + d], ("wide", "narrow"), turned_about(d))
    cuts = cut(pos, expert_down)
    others = [
        lax.ppermute(w, "narrow", swap)
        for w, swap in zip(cuts, (Y_SWAP, BOTH_SWAP, CORE_SWAP))
    ]
    column = stack(place, pieces)
    flipped = lax.ppermute(column, "wide", moved(0, 1, 0))
    column = jnp.stack([column, flipped])
    near = {k: lax.ppermute(column, "wide", moved(0, 0, k)) for k in (2, -2, 1, -1, 4)}
    toks = [tokens]
    for d in range(1, NX):
        toks.append(lax.ppermute(tokens, "wide", moved(d, 0, 0)))
    third = lax.ppermute(near[2], "wide", moved(0, 0, 1))
    fifth = lax.ppermute(near[-2], "wide", moved(0, 0, -1))
    blocks = [column, near[1], near[2], third, near[4], fifth, near[-2], near[-1]]

    ys = []
    for k in range(CHUNKS):
        ys.append(lax.ppermute(own[k * CHUNK_ROWS : (k + 1) * CHUNK_ROWS], "narrow", Y_SWAP))
    core = lax.ppermute(own, "narrow", CORE_SWAP)
    hiddens = []
    for k in range(CHUNKS):
        both = lax.ppermute(ys[k], "narrow", CORE_SWAP)
        hidden = expert_hidden(pos, k, own, core, ys[k], both, gate_t, up_t)
        hidden_y = lax.ppermute(hidden, "narrow", Y_SWAP)
        hidden_core = lax.ppermute(hidden, "narrow", CORE_SWAP)
        hiddens.append([hidden, hidden_y, hidden_core])
    lanes, units = pieces[0].shape[1], pieces[NX].shape[1]
    common = shared_hidden(place, toks, blocks, hiddens[-1][0], lanes, units)
    common_y = lax.ppermute(common, "narrow", Y_SWAP)
    common_core = lax.ppermute(common, "narrow", CORE_SWAP)
    common_both = lax.ppermute(common_y, "narrow", CORE_SWAP)
    outputs = None
    for k in range(CHUNKS):
        hidden_both = lax.ppermute(hiddens[k][1], "narrow", CORE_SWAP)
        hiddens[k].insert(2, hidden_both)
        outputs = expert_columns(pos, k, hiddens[k], expert_down, others, outputs)
    returned = lax.all_to_all(outputs.reshape(EXPERTS, CAP, COLS), "wide", 0, 0, tiled=True)

    shared = list(shared_columns(place, [common, common_core, common_y, common_both], blocks, outputs))
    for d in range(1, NX):
        shared[d] = lax.ppermute(shared[d], "wide", moved(-d, 0, 0))
    return combine(ids_t, gates_t, returned.reshape(SLOTS, COLS), shared)


def solution(mesh):
    in_specs = (
        P("wide", None),
        P("wide", None),
        P("wide", None),
        P("wide", "narrow"),
        P("wide", "narrow"),
        P("narrow", "wide"),
        P("wide", None, "narrow"),
        P("wide", None, "narrow"),
        P("wide", "narrow", None),
    )
    out_specs = P("wide", "narrow")
    return jax.shard_map(body, mesh=mesh, in_specs=in_specs, out_specs=out_specs, check_vma=False)
```

```python
import jax
import jax.numpy as jnp
from jax import lax
from jax.experimental import pallas as pl
from jax.experimental.pallas import tpu as pltpu
from jax.sharding import PartitionSpec as P


F32 = jnp.float32
BF16 = jnp.bfloat16
CAP = 16
EXPERTS = 64
SLOTS = EXPERTS * CAP
TOK = 128
D = 2048
FS = 2816
NX = 4
NY = 2
NZ = 8
CORE_SWAP = [(0, 1), (1, 0), (2, 3), (3, 2)]
Y_SWAP = [(0, 2), (2, 0), (1, 3), (3, 1)]
BOTH_SWAP = [(0, 3), (3, 0), (1, 2), (2, 1)]
COLS = D // 4
CHUNKS = 2
CHUNK_ROWS = SLOTS // CHUNKS
STEP_ROWS = 256
NO_SLOT = 100.0


def moved(dx, flip, dz):
    def index(x, y, z):
        return (x % NX * NY + y) * NZ + z % NZ

    return [
        (index(x, y, z), index(x + dx, y ^ flip, z + dz))
        for x in range(NX)
        for y in range(NY)
        for z in range(NZ)
    ]


def turned_about(k):
    def index(x, y, z, n):
        return ((x * NY + y) * NZ + z) * 4 + n

    return [
        (index(x, y, z, n), index((n + k) % 4, y, z, x))
        for x in range(NX)
        for y in range(NY)
        for z in range(NZ)
        for n in range(4)
    ]


def silu(v):
    return v / (1.0 + jnp.exp(-v))


def dot(a, b):
    return lax.dot_general(a, b, (((1,), (0,)), ((), ())), preferred_element_type=F32)


def dot_nt(a, b):
    return lax.dot_general(a, b, (((1,), (1,)), ((), ())), preferred_element_type=F32)


def named_counts(ids, shape, k_axis):
    expert = lax.broadcasted_iota(jnp.int32, shape, k_axis).astype(F32)
    named = jnp.zeros(shape, F32)
    for k in range(ids.shape[k_axis]):
        one = ids[:, k : k + 1] if k_axis else ids[k : k + 1, :]
        named = named + jnp.where(one == expert, 1.0, 0.0)
    return named


def order_matrix(upper):
    row = lax.broadcasted_iota(jnp.int32, (TOK, TOK), 0)
    col = lax.broadcasted_iota(jnp.int32, (TOK, TOK), 1)
    before = row < col if upper else col < row
    return jnp.where(before, 1.0, 0.0).astype(BF16)


def dispatch_kernel(pos_ref, ids_ref, tok_ref, out_ref):
    del pos_ref
    rows = out_ref.shape[0]
    first = pl.program_id(0) * rows
    named = named_counts(ids_ref[...].astype(F32), (EXPERTS, TOK), 0)
    place = dot(named.astype(BF16), order_matrix(True))
    keys = jnp.where(named > 0.0, place, NO_SLOT).astype(BF16)
    r = lax.broadcasted_iota(jnp.int32, (rows, EXPERTS), 0) + first
    e = lax.broadcasted_iota(jnp.int32, (rows, EXPERTS), 1)
    spread = jnp.where((r >> 4) == e, 1.0, 0.0).astype(BF16)
    wanted = dot(spread, keys)
    slot = ((lax.broadcasted_iota(jnp.int32, (rows, TOK), 0) + first) & 15).astype(F32)
    pick = jnp.where(wanted == slot, 1.0, 0.0).astype(BF16)
    out_ref[...] = dot(pick, tok_ref[...]).astype(BF16)


def dispatch(pos, ids_t, tokens):
    blocks = 2
    rows = SLOTS // blocks
    return pl.pallas_call(
        dispatch_kernel,
        grid_spec=pltpu.PrefetchScalarGridSpec(
            num_scalar_prefetch=1,
            grid=(blocks,),
            in_specs=[
                pl.BlockSpec(ids_t.shape, lambda i, p: (0, 0)),
                pl.BlockSpec((TOK, COLS), lambda i, p: (0, p[0])),
            ],
            out_specs=pl.BlockSpec((rows, COLS), lambda i, p: (i, 0)),
        ),
        out_shape=jax.ShapeDtypeStruct((SLOTS, COLS), BF16),
        name="dispatch",
    )(pos, ids_t, tokens)


def padded_to(value, lanes):
    return jnp.concatenate([value, jnp.zeros((value.shape[0], lanes - value.shape[1]), F32)], axis=1)


def chosen(parts, at):
    total = parts[-1]
    for i in range(len(parts) - 1):
        total = jnp.where(at == i, parts[i], total)
    return total


def pack_kernel(place_ref, gate_ref, up_ref, down_ref, *outs):
    n, x = place_ref[0], place_ref[1]
    fs = gate_ref.shape[1] // NX
    gate, up, down = gate_ref[...].astype(F32), up_ref[...].astype(F32), down_ref[...].astype(F32)
    inward, outward = [], []
    for i in range(NX):
        cut = slice(i * fs, (i + 1) * fs)
        both = jnp.concatenate([gate[:, cut], up[:, cut]], axis=1)
        inward.append(padded_to(both, outs[0].shape[1]))
        outward.append(padded_to(down[:, cut], outs[NX].shape[1]))
    for d in range(NX):
        outs[d][...] = chosen(inward, (x + d) & 3).astype(BF16)
        outs[NX + d][...] = chosen(outward, (n + d) & 3).astype(BF16)


def pack(place, gate, up, down_t):
    fs = gate.shape[1] // NX
    rows = gate.shape[0]
    vmem = pl.BlockSpec(memory_space=pltpu.VMEM)
    inward = jax.ShapeDtypeStruct((rows, -(-2 * fs // 128) * 128), BF16)
    outward = jax.ShapeDtypeStruct((rows, -(-fs // 128) * 128), BF16)
    return pl.pallas_call(
        pack_kernel,
        in_specs=[pl.BlockSpec(memory_space=pltpu.SMEM)] + [vmem] * 3,
        out_specs=[vmem] * 8,
        out_shape=[inward] * 4 + [outward] * 4,
        name="pack",
    )(place, gate, up, down_t)


def stack_kernel(place_ref, *refs):
    pieces, out_ref = refs[:8], refs[8]
    x = place_ref[1]
    lanes = pieces[0].shape[1]
    for d in range(NX):
        at = (x - d) & 3
        out_ref[pl.ds(at, 1), :, :lanes] = pieces[d][...][None]
        out_ref[pl.ds(at, 1), :, lanes:] = pieces[NX + d][...][None]


def stack(place, pieces):
    vmem = pl.BlockSpec(memory_space=pltpu.VMEM)
    lanes = pieces[0].shape[1] + pieces[NX].shape[1]
    return pl.pallas_call(
        stack_kernel,
        in_specs=[pl.BlockSpec(memory_space=pltpu.SMEM)] + [vmem] * 8,
        out_specs=vmem,
        out_shape=jax.ShapeDtypeStruct((NX, pieces[0].shape[0], lanes), BF16),
        name="stack",
    )(place, *pieces)


def cut_kernel(pos_ref, a, b, c, out_a, out_b, out_c):
    del pos_ref
    out_a[...] = a[0]
    out_b[...] = b[0]
    out_c[...] = c[0]


def cut(pos, w_down):
    mf = w_down.shape[1]
    return pl.pallas_call(
        cut_kernel,
        grid_spec=pltpu.PrefetchScalarGridSpec(
            num_scalar_prefetch=1,
            grid=(1,),
            in_specs=[
                pl.BlockSpec((1, mf, COLS), lambda i, p: (0, 0, p[0] ^ 2)),
                pl.BlockSpec((1, mf, COLS), lambda i, p: (0, 0, p[0] ^ 3)),
                pl.BlockSpec((1, mf, COLS), lambda i, p: (0, 0, p[0] ^ 1)),
            ],
            out_specs=[pl.BlockSpec((mf, COLS), lambda i, p: (0, 0))] * 3,
        ),
        out_shape=[jax.ShapeDtypeStruct((mf, COLS), BF16)] * 3,
        name="cut",
    )(pos, w_down, w_down, w_down)


def hidden_kernel(pos_ref, x0, x1, x2, x3, g0, g1, g2, g3, u0, u1, u2, u3, out_ref):
    del pos_ref
    gate = jnp.zeros((x0.shape[0], g0.shape[1]), F32)
    up = gate
    for x, g, u in ((x0, g0, u0), (x1, g1, u1), (x2, g2, u2), (x3, g3, u3)):
        rows = x[...]
        gate = gate + dot_nt(rows, g[0])
        up = up + dot_nt(rows, u[0])
    mf = gate.shape[1]
    out_ref[:, :mf] = (silu(gate) * up).astype(BF16)
    out_ref[:, mf:] = jnp.zeros((gate.shape[0], out_ref.shape[1] - mf), BF16)


def expert_hidden(pos, chunk, own, core, y, both, w_gate, w_up):
    steps = CHUNK_ROWS // STEP_ROWS
    mf = w_gate.shape[1]
    padded = -(-mf // 128) * 128
    whole = pl.BlockSpec((STEP_ROWS, COLS), lambda i, p: (chunk * steps + i, 0))
    part = pl.BlockSpec((STEP_ROWS, COLS), lambda i, p: (i, 0))
    w_specs = [
        pl.BlockSpec((1, mf, COLS), lambda i, p: (0, 0, p[0])),
        pl.BlockSpec((1, mf, COLS), lambda i, p: (0, 0, p[0] ^ 1)),
        pl.BlockSpec((1, mf, COLS), lambda i, p: (0, 0, p[0] ^ 2)),
        pl.BlockSpec((1, mf, COLS), lambda i, p: (0, 0, p[0] ^ 3)),
    ]
    return pl.pallas_call(
        hidden_kernel,
        grid_spec=pltpu.PrefetchScalarGridSpec(
            num_scalar_prefetch=1,
            grid=(steps,),
            in_specs=[whole, whole, part, part] + w_specs + w_specs,
            out_specs=pl.BlockSpec((STEP_ROWS, padded), lambda i, p: (i, 0)),
        ),
        out_shape=jax.ShapeDtypeStruct((CHUNK_ROWS, padded), BF16),
        cost_estimate=pl.CostEstimate(
            flops=4 * CHUNK_ROWS * D * mf, bytes_accessed=6_000_000, transcendentals=CHUNK_ROWS * mf
        ),
        name="hidden",
    )(pos, own, core, y, both, *[w_gate] * 4, *[w_up] * 4)


def down_kernel(pos_ref, h0, h1, h2, h3, w0, w1, w2, w3, *rest):
    del pos_ref
    out_ref = rest[-1]
    mf = w1.shape[0]
    total = dot(h0[:, :mf], w0[0])
    for h, w in ((h1, w1), (h2, w2), (h3, w3)):
        total = total + dot(h[:, :mf], w[...])
    out_ref[...] = total.astype(BF16)


def expert_columns(pos, chunk, hiddens, w_own, w_others, so_far):
    steps = CHUNK_ROWS // STEP_ROWS
    mf = w_own.shape[1]
    h_spec = pl.BlockSpec((STEP_ROWS, hiddens[0].shape[1]), lambda i, p: (i, 0))
    w_spec = pl.BlockSpec((mf, COLS), lambda i, p: (0, 0))
    more = [] if so_far is None else [so_far]
    return pl.pallas_call(
        down_kernel,
        grid_spec=pltpu.PrefetchScalarGridSpec(
            num_scalar_prefetch=1,
            grid=(steps,),
            in_specs=[h_spec] * 4
            + [pl.BlockSpec((1, mf, COLS), lambda i, p: (0, 0, p[0]))]
            + [w_spec] * 3
            + [pl.BlockSpec(memory_space=pl.ANY)] * len(more),
            out_specs=pl.BlockSpec((STEP_ROWS, COLS), lambda i, p: (chunk * steps + i, 0)),
        ),
        out_shape=jax.ShapeDtypeStruct((SLOTS, COLS), BF16),
        input_output_aliases={9: 0} if more else {},
        cost_estimate=pl.CostEstimate(
            flops=8 * CHUNK_ROWS * COLS * mf, bytes_accessed=4_000_000, transcendentals=0
        ),
        name="down",
    )(pos, *hiddens, w_own, *w_others, *more)


def fetch(blocks, w_ref, sems, z, first):
    copies = []
    for step, block in enumerate(blocks):
        part = block.at[:, :, :, pl.ds(first, w_ref.shape[4])]
        copies.append(pltpu.make_async_copy(part, w_ref.at[(z - step) & (NZ - 1)], sems.at[step]))
    for copy in copies:
        copy.start()
    for copy in copies:
        copy.wait()


def shared_hidden_kernel(place_ref, t0, t1, t2, t3, *refs):
    blocks, (out_ref, w_ref, sems) = refs[:NZ], refs[NZ + 1 :]
    y, z = place_ref[2], place_ref[3]
    fetch(blocks, w_ref, sems, z, 0)
    rows = NZ * w_ref.shape[3]
    lanes = w_ref.shape[4]
    fs = FS // (4 * NX)
    total = jnp.zeros((NX * TOK, lanes), F32)
    for quarter in range(NX):
        for half in range(NY):
            w = w_ref[:, pl.ds(half ^ y, 1), quarter].reshape(rows, lanes)
            first = (quarter * NY + half) * rows
            tok = jnp.concatenate([t[:, first : first + rows] for t in (t0, t1, t2, t3)], axis=0)
            total = total + dot(tok, w)
    hidden = silu(total[:, :fs]) * total[:, fs : 2 * fs]
    out_ref[...] = padded_to(hidden, out_ref.shape[1]).astype(BF16)


def shared_hidden(place, toks, blocks, after, lanes, units):
    vmem = pl.BlockSpec(memory_space=pltpu.VMEM)
    return pl.pallas_call(
        shared_hidden_kernel,
        in_specs=[pl.BlockSpec(memory_space=pltpu.SMEM)]
        + [vmem] * 4
        + [pl.BlockSpec(memory_space=pl.ANY)] * (NZ + 1),
        out_specs=vmem,
        out_shape=jax.ShapeDtypeStruct((NX * TOK, units), BF16),
        scratch_shapes=[
            pltpu.VMEM((NZ,) + blocks[0].shape[:3] + (lanes,), BF16),
            pltpu.SemaphoreType.DMA((NZ,)),
        ],
        cost_estimate=pl.CostEstimate(
            flops=2 * NX * TOK * D * lanes, bytes_accessed=5_000_000, transcendentals=NX * TOK * units
        ),
        name="shared_hidden",
    )(place, *toks, *blocks, after)


def shared_down_kernel(place_ref, h0, h1, h2, h3, *refs):
    blocks, outs, (w_ref, sems) = refs[:NZ], refs[NZ + 1 : NZ + 5], refs[NZ + 5 :]
    n, y, z = place_ref[0], place_ref[2], place_ref[3]
    units = w_ref.shape[4]
    fetch(blocks, w_ref, sems, z, blocks[0].shape[3] - units)
    rows = NZ * w_ref.shape[3]
    for half in range(NY):
        total = jnp.zeros((NX * TOK, rows), F32)
        for j, h in enumerate((h0, h1, h2, h3)):
            w = w_ref[:, pl.ds(half ^ y, 1), pl.ds(n ^ j, 1)].reshape(rows, units)
            total = total + dot_nt(h[...], w)
        for d in range(NX):
            outs[d][:, half * rows : (half + 1) * rows] = total[d * TOK : (d + 1) * TOK].astype(BF16)


def shared_columns(place, hiddens, blocks, after):
    vmem = pl.BlockSpec(memory_space=pltpu.VMEM)
    units = hiddens[0].shape[1]
    return pl.pallas_call(
        shared_down_kernel,
        in_specs=[pl.BlockSpec(memory_space=pltpu.SMEM)]
        + [vmem] * 4
        + [pl.BlockSpec(memory_space=pl.ANY)] * (NZ + 1),
        out_specs=[vmem] * 4,
        out_shape=[jax.ShapeDtypeStruct((TOK, COLS), BF16)] * 4,
        scratch_shapes=[
            pltpu.VMEM((NZ,) + blocks[0].shape[:3] + (units,), BF16),
            pltpu.SemaphoreType.DMA((NZ,)),
        ],
        cost_estimate=pl.CostEstimate(
            flops=2 * NX * TOK * D * units, bytes_accessed=4_000_000, transcendentals=0
        ),
        name="shared_down",
    )(place, *hiddens, *blocks, after)


def turned(values):
    row = lax.broadcasted_iota(jnp.int32, (TOK, TOK), 0)
    col = lax.broadcasted_iota(jnp.int32, (TOK, TOK), 1)
    eye = jnp.where(row == col, 1.0, 0.0).astype(BF16)
    total = None
    rest = values
    for _ in range(3):
        part = rest.astype(BF16)
        rest = rest - part.astype(F32)
        moved = dot_nt(eye, part)
        total = moved if total is None else total + moved
    return total


def combine_kernel(ids_ref, gw_ref, ret_ref, s0, s1, s2, s3, out_ref):
    ids = turned(ids_ref[...].astype(F32))
    gates = turned(gw_ref[...])
    named = named_counts(ids, (TOK, EXPERTS), 1)
    place = dot(order_matrix(False), named.astype(BF16))
    keys = jnp.where(named > 0.0, place, NO_SLOT).astype(BF16)
    lane = lax.broadcasted_iota(jnp.int32, (TOK, EXPERTS), 1).astype(F32)
    weight = jnp.zeros((TOK, EXPERTS), F32)
    for k in range(ids.shape[1]):
        weight = weight + jnp.where(ids[:, k : k + 1] == lane, gates[:, k : k + 1], 0.0)
    e = lax.broadcasted_iota(jnp.int32, (EXPERTS, SLOTS), 0)
    r = lax.broadcasted_iota(jnp.int32, (EXPERTS, SLOTS), 1)
    spread = jnp.where((r >> 4) == e, 1.0, 0.0).astype(BF16)
    slot = (lax.broadcasted_iota(jnp.int32, (TOK, SLOTS), 1) & 15).astype(F32)
    hit = dot(keys, spread) == slot
    ret = ret_ref[...]
    total = s0[...].astype(F32)
    for part in (s1, s2, s3):
        total = total + part[...].astype(F32)
    rest = weight
    for _ in range(3):
        part = rest.astype(BF16)
        rest = rest - part.astype(F32)
        row = jnp.where(hit, dot(part, spread), 0.0).astype(BF16)
        total = total + dot(row, ret)
    out_ref[...] = total.astype(BF16)


def combine(ids, gate_weights, returned, shared):
    return pl.pallas_call(
        combine_kernel,
        out_shape=jax.ShapeDtypeStruct((TOK, COLS), BF16),
        name="combine",
    )(ids, gate_weights, returned, *shared)


def body(
    tokens,
    expert_ids,
    gate_weights,
    shared_gate,
    shared_up,
    shared_down,
    expert_gate,
    expert_up,
    expert_down,
):
    pos = lax.axis_index("narrow").astype(jnp.int32).reshape(1)
    ids_t = expert_ids.T
    gates_t = gate_weights.T
    gate_t = expert_gate.transpose(0, 2, 1)
    up_t = expert_up.transpose(0, 2, 1)

    wide = lax.axis_index("wide").astype(jnp.int32)
    place = jnp.stack([pos[0], wide >> 4, (wide >> 3) & 1, wide & 7])

    outgoing = dispatch(pos, ids_t, tokens).reshape(EXPERTS, CAP, COLS)
    own = lax.all_to_all(outgoing, "wide", 0, 0, tiled=True).reshape(SLOTS, COLS)

    pieces = list(pack(place, shared_gate, shared_up, shared_down.T))
    for d in range(1, NX):
        pieces[d] = lax.ppermute(pieces[d], "wide", moved(d, 0, 0))
    for d in range(NX):
        pieces[NX + d] = lax.ppermute(pieces[NX + d], ("wide", "narrow"), turned_about(d))
    cuts = cut(pos, expert_down)
    others = [
        lax.ppermute(w, "narrow", swap)
        for w, swap in zip(cuts, (Y_SWAP, BOTH_SWAP, CORE_SWAP))
    ]
    column = stack(place, pieces)
    flipped = lax.ppermute(column, "wide", moved(0, 1, 0))
    column = jnp.stack([column, flipped])
    blocks = [column]
    for k in range(1, NZ):
        blocks.append(lax.ppermute(column, "wide", moved(0, 0, k)))
    toks = [tokens]
    for d in range(1, NX):
        toks.append(lax.ppermute(tokens, "wide", moved(d, 0, 0)))
    ys = []
    for k in range(CHUNKS):
        ys.append(lax.ppermute(own[k * CHUNK_ROWS : (k + 1) * CHUNK_ROWS], "narrow", Y_SWAP))
    core = lax.ppermute(own, "narrow", CORE_SWAP)
    hiddens = []
    for k in range(CHUNKS):
        both = lax.ppermute(ys[k], "narrow", CORE_SWAP)
        hidden = expert_hidden(pos, k, own, core, ys[k], both, gate_t, up_t)
        hidden_y = lax.ppermute(hidden, "narrow", Y_SWAP)
        hidden_core = lax.ppermute(hidden, "narrow", CORE_SWAP)
        hiddens.append([hidden, hidden_y, hidden_core])
    lanes, units = pieces[0].shape[1], pieces[NX].shape[1]
    common = shared_hidden(place, toks, blocks, hiddens[-1][0], lanes, units)
    common_y = lax.ppermute(common, "narrow", Y_SWAP)
    common_core = lax.ppermute(common, "narrow", CORE_SWAP)
    common_both = lax.ppermute(common_y, "narrow", CORE_SWAP)
    outputs = None
    for k in range(CHUNKS):
        hidden_both = lax.ppermute(hiddens[k][1], "narrow", CORE_SWAP)
        hiddens[k].insert(2, hidden_both)
        outputs = expert_columns(pos, k, hiddens[k], expert_down, others, outputs)
    returned = lax.all_to_all(outputs.reshape(EXPERTS, CAP, COLS), "wide", 0, 0, tiled=True)

    shared = list(shared_columns(place, [common, common_core, common_y, common_both], blocks, outputs))
    for d in range(1, NX):
        shared[d] = lax.ppermute(shared[d], "wide", moved(-d, 0, 0))
    return combine(ids_t, gates_t, returned.reshape(SLOTS, COLS), shared)


def solution(mesh):
    in_specs = (
        P("wide", None),
        P("wide", None),
        P("wide", None),
        P("wide", "narrow"),
        P("wide", "narrow"),
        P("narrow", "wide"),
        P("wide", None, "narrow"),
        P("wide", None, "narrow"),
        P("wide", "narrow", None),
    )
    out_specs = P("wide", "narrow")
    return jax.shard_map(body, mesh=mesh, in_specs=in_specs, out_specs=out_specs, check_vma=False)
```

```python
import jax
import jax.numpy as jnp
from jax import lax
from jax.experimental import pallas as pl
from jax.experimental.pallas import tpu as pltpu
from jax.sharding import PartitionSpec as P


F32 = jnp.float32
BF16 = jnp.bfloat16
CAP = 16
EXPERTS = 64
SLOTS = EXPERTS * CAP
TOK = 128
D = 2048
FS = 2816
NX = 4
NY = 2
NZ = 8
PAIRS = NZ // 2
CORE_SWAP = [(0, 1), (1, 0), (2, 3), (3, 2)]
Y_SWAP = [(0, 2), (2, 0), (1, 3), (3, 1)]
BOTH_SWAP = [(0, 3), (3, 0), (1, 2), (2, 1)]
COLS = D // 4
CHUNKS = 2
CHUNK_ROWS = SLOTS // CHUNKS
STEP_ROWS = 256
NO_SLOT = 100.0


def moved(dx, flip, dz, pair=0):
    def index(x, y, z):
        return (x % NX * NY + y) * NZ + z % NZ

    return [
        (index(x, y, z), index(x + dx, y ^ flip, (z ^ pair) + dz))
        for x in range(NX)
        for y in range(NY)
        for z in range(NZ)
    ]


def turned_about(k):
    def index(x, y, z, n):
        return ((x * NY + y) * NZ + z) * 4 + n

    return [
        (index(x, y, z, n), index((n + k) % 4, y, z, x))
        for x in range(NX)
        for y in range(NY)
        for z in range(NZ)
        for n in range(4)
    ]


def silu(v):
    return v / (1.0 + jnp.exp(-v))


def dot(a, b):
    return lax.dot_general(a, b, (((1,), (0,)), ((), ())), preferred_element_type=F32)


def dot_nt(a, b):
    return lax.dot_general(a, b, (((1,), (1,)), ((), ())), preferred_element_type=F32)


def named_counts(ids, shape, k_axis):
    expert = lax.broadcasted_iota(jnp.int32, shape, k_axis).astype(F32)
    named = jnp.zeros(shape, F32)
    for k in range(ids.shape[k_axis]):
        one = ids[:, k : k + 1] if k_axis else ids[k : k + 1, :]
        named = named + jnp.where(one == expert, 1.0, 0.0)
    return named


def order_matrix(upper):
    row = lax.broadcasted_iota(jnp.int32, (TOK, TOK), 0)
    col = lax.broadcasted_iota(jnp.int32, (TOK, TOK), 1)
    before = row < col if upper else col < row
    return jnp.where(before, 1.0, 0.0).astype(BF16)


def dispatch_kernel(pos_ref, ids_ref, tok_ref, out_ref):
    del pos_ref
    rows = out_ref.shape[0]
    first = pl.program_id(0) * rows
    named = named_counts(ids_ref[...].astype(F32), (EXPERTS, TOK), 0)
    place = dot(named.astype(BF16), order_matrix(True))
    keys = jnp.where(named > 0.0, place, NO_SLOT).astype(BF16)
    r = lax.broadcasted_iota(jnp.int32, (rows, EXPERTS), 0) + first
    e = lax.broadcasted_iota(jnp.int32, (rows, EXPERTS), 1)
    spread = jnp.where((r >> 4) == e, 1.0, 0.0).astype(BF16)
    wanted = dot(spread, keys)
    slot = ((lax.broadcasted_iota(jnp.int32, (rows, TOK), 0) + first) & 15).astype(F32)
    pick = jnp.where(wanted == slot, 1.0, 0.0).astype(BF16)
    out_ref[...] = dot(pick, tok_ref[...]).astype(BF16)


def dispatch(pos, ids_t, tokens):
    blocks = 2
    rows = SLOTS // blocks
    return pl.pallas_call(
        dispatch_kernel,
        grid_spec=pltpu.PrefetchScalarGridSpec(
            num_scalar_prefetch=1,
            grid=(blocks,),
            in_specs=[
                pl.BlockSpec(ids_t.shape, lambda i, p: (0, 0)),
                pl.BlockSpec((TOK, COLS), lambda i, p: (0, p[0])),
            ],
            out_specs=pl.BlockSpec((rows, COLS), lambda i, p: (i, 0)),
        ),
        out_shape=jax.ShapeDtypeStruct((SLOTS, COLS), BF16),
        name="dispatch",
    )(pos, ids_t, tokens)


def padded_to(value, lanes):
    return jnp.concatenate([value, jnp.zeros((value.shape[0], lanes - value.shape[1]), F32)], axis=1)


def pack_kernel(gate_ref, up_ref, down_ref, out_ref):
    fs = gate_ref.shape[1] // NX
    inward, outward = lanes_of(fs)
    for i in range(NX):
        cut = slice(i * fs, (i + 1) * fs)
        both = jnp.concatenate([gate_ref[:, cut], up_ref[:, cut]], axis=1).astype(F32)
        out_ref[i, :, :inward] = padded_to(both, inward).astype(BF16)
        out_ref[i, :, inward:] = padded_to(down_ref[:, cut].astype(F32), outward).astype(BF16)


def lanes_of(fs):
    return -(-2 * fs // 128) * 128, -(-fs // 128) * 128


def pack(gate, up, down_t):
    return pl.pallas_call(
        pack_kernel,
        out_shape=jax.ShapeDtypeStruct((NX, gate.shape[0], sum(lanes_of(gate.shape[1] // NX))), BF16),
        name="pack",
    )(gate, up, down_t)


def deal_kernel(place_ref, *refs):
    raws, outs = refs[:4], refs[4:]
    n, x, y, z = place_ref[0], place_ref[1], place_ref[2], place_ref[3]
    rows = raws[0].shape[1]
    inward = outs[0].shape[1]
    for i, raw in enumerate(raws):
        at = ((y ^ (i & 1)) * 2 + ((z & 1) ^ (i >> 1))) * rows
        to = pl.ds(pl.multiple_of(at, rows), rows)
        for d in range(NX):
            outs[d][to, :] = raw[pl.ds((x + d) & 3, 1), :, :inward].reshape(rows, inward)
            outs[NX + d][to, :] = raw[pl.ds((n + d) & 3, 1), :, inward:].reshape(
                rows, raw.shape[2] - inward
            )


def deal(place, raws, fs):
    inward, outward = lanes_of(fs)
    rows = 4 * raws[0].shape[1]
    vmem = pl.BlockSpec(memory_space=pltpu.VMEM)
    return pl.pallas_call(
        deal_kernel,
        in_specs=[pl.BlockSpec(memory_space=pltpu.SMEM)] + [vmem] * 4,
        out_specs=[vmem] * 8,
        out_shape=[jax.ShapeDtypeStruct((rows, inward), BF16)] * 4
        + [jax.ShapeDtypeStruct((rows, outward), BF16)] * 4,
        name="deal",
    )(place, *raws)


def stack_kernel(place_ref, *refs):
    pieces, outs = refs[:8], refs[8:]
    x = place_ref[1]
    for d in range(NX):
        at = pl.ds((x - d) & 3, 1)
        outs[0][at] = pieces[d][...][None]
        outs[1][at] = pieces[NX + d][...][None]


def stack(place, pieces):
    vmem = pl.BlockSpec(memory_space=pltpu.VMEM)
    return pl.pallas_call(
        stack_kernel,
        in_specs=[pl.BlockSpec(memory_space=pltpu.SMEM)] + [vmem] * 8,
        out_specs=[vmem] * 2,
        out_shape=[jax.ShapeDtypeStruct((NX,) + pieces[i].shape, BF16) for i in (0, NX)],
        name="stack",
    )(place, *pieces)


def cut_kernel(pos_ref, a, b, c, out_a, out_b, out_c):
    del pos_ref
    out_a[...] = a[0]
    out_b[...] = b[0]
    out_c[...] = c[0]


def cut(pos, w_down):
    mf = w_down.shape[1]
    return pl.pallas_call(
        cut_kernel,
        grid_spec=pltpu.PrefetchScalarGridSpec(
            num_scalar_prefetch=1,
            grid=(1,),
            in_specs=[
                pl.BlockSpec((1, mf, COLS), lambda i, p: (0, 0, p[0] ^ 2)),
                pl.BlockSpec((1, mf, COLS), lambda i, p: (0, 0, p[0] ^ 3)),
                pl.BlockSpec((1, mf, COLS), lambda i, p: (0, 0, p[0] ^ 1)),
            ],
            out_specs=[pl.BlockSpec((mf, COLS), lambda i, p: (0, 0))] * 3,
        ),
        out_shape=[jax.ShapeDtypeStruct((mf, COLS), BF16)] * 3,
        name="cut",
    )(pos, w_down, w_down, w_down)


def hidden_kernel(pos_ref, x0, x1, x2, x3, g0, g1, g2, g3, u0, u1, u2, u3, out_ref):
    del pos_ref
    gate = jnp.zeros((x0.shape[0], g0.shape[1]), F32)
    up = gate
    for x, g, u in ((x0, g0, u0), (x1, g1, u1), (x2, g2, u2), (x3, g3, u3)):
        rows = x[...]
        gate = gate + dot_nt(rows, g[0])
        up = up + dot_nt(rows, u[0])
    mf = gate.shape[1]
    out_ref[:, :mf] = (silu(gate) * up).astype(BF16)
    out_ref[:, mf:] = jnp.zeros((gate.shape[0], out_ref.shape[1] - mf), BF16)


def expert_hidden(pos, chunk, own, core, y, both, w_gate, w_up):
    steps = CHUNK_ROWS // STEP_ROWS
    mf = w_gate.shape[1]
    padded = -(-mf // 128) * 128
    whole = pl.BlockSpec((STEP_ROWS, COLS), lambda i, p: (chunk * steps + i, 0))
    part = pl.BlockSpec((STEP_ROWS, COLS), lambda i, p: (i, 0))
    w_specs = [
        pl.BlockSpec((1, mf, COLS), lambda i, p: (0, 0, p[0])),
        pl.BlockSpec((1, mf, COLS), lambda i, p: (0, 0, p[0] ^ 1)),
        pl.BlockSpec((1, mf, COLS), lambda i, p: (0, 0, p[0] ^ 2)),
        pl.BlockSpec((1, mf, COLS), lambda i, p: (0, 0, p[0] ^ 3)),
    ]
    return pl.pallas_call(
        hidden_kernel,
        grid_spec=pltpu.PrefetchScalarGridSpec(
            num_scalar_prefetch=1,
            grid=(steps,),
            in_specs=[whole, whole, part, part] + w_specs + w_specs,
            out_specs=pl.BlockSpec((STEP_ROWS, padded), lambda i, p: (i, 0)),
        ),
        out_shape=jax.ShapeDtypeStruct((CHUNK_ROWS, padded), BF16),
        cost_estimate=pl.CostEstimate(
            flops=4 * CHUNK_ROWS * D * mf, bytes_accessed=6_000_000, transcendentals=CHUNK_ROWS * mf
        ),
        name="hidden",
    )(pos, own, core, y, both, *[w_gate] * 4, *[w_up] * 4)


def down_kernel(pos_ref, h0, h1, h2, h3, w0, w1, w2, w3, *rest):
    del pos_ref
    out_ref = rest[-1]
    mf = w1.shape[0]
    total = dot(h0[:, :mf], w0[0])
    for h, w in ((h1, w1), (h2, w2), (h3, w3)):
        total = total + dot(h[:, :mf], w[...])
    out_ref[...] = total.astype(BF16)


def expert_columns(pos, chunk, hiddens, w_own, w_others, so_far):
    steps = CHUNK_ROWS // STEP_ROWS
    mf = w_own.shape[1]
    h_spec = pl.BlockSpec((STEP_ROWS, hiddens[0].shape[1]), lambda i, p: (i, 0))
    w_spec = pl.BlockSpec((mf, COLS), lambda i, p: (0, 0))
    more = [] if so_far is None else [so_far]
    return pl.pallas_call(
        down_kernel,
        grid_spec=pltpu.PrefetchScalarGridSpec(
            num_scalar_prefetch=1,
            grid=(steps,),
            in_specs=[h_spec] * 4
            + [pl.BlockSpec((1, mf, COLS), lambda i, p: (0, 0, p[0]))]
            + [w_spec] * 3
            + [pl.BlockSpec(memory_space=pl.ANY)] * len(more),
            out_specs=pl.BlockSpec((STEP_ROWS, COLS), lambda i, p: (chunk * steps + i, 0)),
        ),
        out_shape=jax.ShapeDtypeStruct((SLOTS, COLS), BF16),
        input_output_aliases={9: 0} if more else {},
        cost_estimate=pl.CostEstimate(
            flops=8 * CHUNK_ROWS * COLS * mf, bytes_accessed=4_000_000, transcendentals=0
        ),
        name="down",
    )(pos, *hiddens, w_own, *w_others, *more)


def fetch(blocks, w_ref, sems, z):
    copies = []
    for step, block in enumerate(blocks):
        to = w_ref.at[((z >> 1) - step) & (PAIRS - 1)]
        copies.append(pltpu.make_async_copy(block, to, sems.at[step]))
    for copy in copies:
        copy.start()
    for copy in copies:
        copy.wait()


def shared_hidden_kernel(place_ref, t0, t1, t2, t3, *refs):
    blocks, (out_ref, w_ref, sems) = refs[:PAIRS], refs[PAIRS + 1 :]
    z = place_ref[3]
    fetch(blocks, w_ref, sems, z)
    rows = PAIRS * w_ref.shape[3]
    lanes = w_ref.shape[4]
    fs = FS // (4 * NX)
    total = jnp.zeros((NX * TOK, lanes), F32)
    for quarter in range(NX):
        for half in range(NY):
            w = w_ref[:, quarter, half].reshape(rows, lanes)
            first = (quarter * NY + half) * rows
            tok = jnp.concatenate([t[:, first : first + rows] for t in (t0, t1, t2, t3)], axis=0)
            total = total + dot(tok, w)
    hidden = silu(total[:, :fs]) * total[:, fs : 2 * fs]
    out_ref[...] = padded_to(hidden, out_ref.shape[1]).astype(BF16)


def shared_hidden(place, toks, blocks, after, units):
    lanes = blocks[0].shape[3]
    vmem = pl.BlockSpec(memory_space=pltpu.VMEM)
    return pl.pallas_call(
        shared_hidden_kernel,
        in_specs=[pl.BlockSpec(memory_space=pltpu.SMEM)]
        + [vmem] * 4
        + [pl.BlockSpec(memory_space=pl.ANY)] * (PAIRS + 1),
        out_specs=vmem,
        out_shape=jax.ShapeDtypeStruct((NX * TOK, units), BF16),
        scratch_shapes=[
            pltpu.VMEM((PAIRS,) + blocks[0].shape, BF16),
            pltpu.SemaphoreType.DMA((PAIRS,)),
        ],
        cost_estimate=pl.CostEstimate(
            flops=2 * NX * TOK * D * lanes, bytes_accessed=5_000_000, transcendentals=NX * TOK * units
        ),
        name="shared_hidden",
    )(place, *toks, *blocks, after)


def shared_down_kernel(place_ref, h0, h1, h2, h3, *refs):
    blocks, outs, (w_ref, sems) = refs[:PAIRS], refs[PAIRS + 1 : PAIRS + 5], refs[PAIRS + 5 :]
    n, z = place_ref[0], place_ref[3]
    units = w_ref.shape[4]
    fetch(blocks, w_ref, sems, z)
    rows = PAIRS * w_ref.shape[3]
    for half in range(NY):
        total = jnp.zeros((NX * TOK, rows), F32)
        for j, h in enumerate((h0, h1, h2, h3)):
            w = w_ref[:, pl.ds(n ^ j, 1), half].reshape(rows, units)
            total = total + dot_nt(h[...], w)
        for d in range(NX):
            outs[d][:, half * rows : (half + 1) * rows] = total[d * TOK : (d + 1) * TOK].astype(BF16)


def shared_columns(place, hiddens, blocks, after):
    vmem = pl.BlockSpec(memory_space=pltpu.VMEM)
    units = hiddens[0].shape[1]
    return pl.pallas_call(
        shared_down_kernel,
        in_specs=[pl.BlockSpec(memory_space=pltpu.SMEM)]
        + [vmem] * 4
        + [pl.BlockSpec(memory_space=pl.ANY)] * (PAIRS + 1),
        out_specs=[vmem] * 4,
        out_shape=[jax.ShapeDtypeStruct((TOK, COLS), BF16)] * 4,
        scratch_shapes=[
            pltpu.VMEM((PAIRS,) + blocks[0].shape, BF16),
            pltpu.SemaphoreType.DMA((PAIRS,)),
        ],
        cost_estimate=pl.CostEstimate(
            flops=2 * NX * TOK * D * units, bytes_accessed=4_000_000, transcendentals=0
        ),
        name="shared_down",
    )(place, *hiddens, *blocks, after)


def turned(values):
    row = lax.broadcasted_iota(jnp.int32, (TOK, TOK), 0)
    col = lax.broadcasted_iota(jnp.int32, (TOK, TOK), 1)
    eye = jnp.where(row == col, 1.0, 0.0).astype(BF16)
    total = None
    rest = values
    for _ in range(3):
        part = rest.astype(BF16)
        rest = rest - part.astype(F32)
        moved = dot_nt(eye, part)
        total = moved if total is None else total + moved
    return total


def combine_kernel(ids_ref, gw_ref, ret_ref, s0, s1, s2, s3, out_ref):
    ids = turned(ids_ref[...].astype(F32))
    gates = turned(gw_ref[...])
    named = named_counts(ids, (TOK, EXPERTS), 1)
    place = dot(order_matrix(False), named.astype(BF16))
    keys = jnp.where(named > 0.0, place, NO_SLOT).astype(BF16)
    lane = lax.broadcasted_iota(jnp.int32, (TOK, EXPERTS), 1).astype(F32)
    weight = jnp.zeros((TOK, EXPERTS), F32)
    for k in range(ids.shape[1]):
        weight = weight + jnp.where(ids[:, k : k + 1] == lane, gates[:, k : k + 1], 0.0)
    e = lax.broadcasted_iota(jnp.int32, (EXPERTS, SLOTS), 0)
    r = lax.broadcasted_iota(jnp.int32, (EXPERTS, SLOTS), 1)
    spread = jnp.where((r >> 4) == e, 1.0, 0.0).astype(BF16)
    slot = (lax.broadcasted_iota(jnp.int32, (TOK, SLOTS), 1) & 15).astype(F32)
    hit = dot(keys, spread) == slot
    ret = ret_ref[...]
    total = s0[...].astype(F32)
    for part in (s1, s2, s3):
        total = total + part[...].astype(F32)
    rest = weight
    for _ in range(3):
        part = rest.astype(BF16)
        rest = rest - part.astype(F32)
        row = jnp.where(hit, dot(part, spread), 0.0).astype(BF16)
        total = total + dot(row, ret)
    out_ref[...] = total.astype(BF16)


def combine(ids, gate_weights, returned, shared):
    return pl.pallas_call(
        combine_kernel,
        out_shape=jax.ShapeDtypeStruct((TOK, COLS), BF16),
        name="combine",
    )(ids, gate_weights, returned, *shared)


def body(
    tokens,
    expert_ids,
    gate_weights,
    shared_gate,
    shared_up,
    shared_down,
    expert_gate,
    expert_up,
    expert_down,
):
    pos = lax.axis_index("narrow").astype(jnp.int32).reshape(1)
    ids_t = expert_ids.T
    gates_t = gate_weights.T
    gate_t = expert_gate.transpose(0, 2, 1)
    up_t = expert_up.transpose(0, 2, 1)

    wide = lax.axis_index("wide").astype(jnp.int32)
    place = jnp.stack([pos[0], wide >> 4, (wide >> 3) & 1, wide & 7])

    raw = pack(shared_gate, shared_up, shared_down.T)
    raws = [raw] + [lax.ppermute(raw, "wide", moved(0, i & 1, 0, i >> 1)) for i in (1, 2, 3)]

    outgoing = dispatch(pos, ids_t, tokens).reshape(EXPERTS, CAP, COLS)
    own = lax.all_to_all(outgoing, "wide", 0, 0, tiled=True).reshape(SLOTS, COLS)

    pieces = list(deal(place, raws, shared_gate.shape[1] // NX))
    for d in range(NX):
        pieces[NX + d] = lax.ppermute(pieces[NX + d], ("wide", "narrow"), turned_about(d))
    for d in range(1, NX):
        pieces[d] = lax.ppermute(pieces[d], "wide", moved(d, 0, 0))
    cuts = cut(pos, expert_down)
    others = [
        lax.ppermute(w, "narrow", swap)
        for w, swap in zip(cuts, (Y_SWAP, BOTH_SWAP, CORE_SWAP))
    ]
    columns = stack(place, pieces)
    inward, outward = [
        [c.reshape(NX, NY, c.shape[1] // NY, c.shape[2])] for c in columns
    ]
    for blocks in (inward, outward):
        for k in range(1, PAIRS):
            blocks.append(lax.ppermute(blocks[0], "wide", moved(0, 0, 2 * k)))
    toks = [tokens]
    for d in range(1, NX):
        toks.append(lax.ppermute(tokens, "wide", moved(d, 0, 0)))

    ys = []
    for k in range(CHUNKS):
        ys.append(lax.ppermute(own[k * CHUNK_ROWS : (k + 1) * CHUNK_ROWS], "narrow", Y_SWAP))
    core = lax.ppermute(own, "narrow", CORE_SWAP)
    hiddens = []
    for k in range(CHUNKS):
        both = lax.ppermute(ys[k], "narrow", CORE_SWAP)
        hidden = expert_hidden(pos, k, own, core, ys[k], both, gate_t, up_t)
        hidden_y = lax.ppermute(hidden, "narrow", Y_SWAP)
        hidden_core = lax.ppermute(hidden, "narrow", CORE_SWAP)
        hiddens.append([hidden, hidden_y, hidden_core])
    common = shared_hidden(place, toks, inward, hiddens[-1][0], pieces[NX].shape[1])
    common_y = lax.ppermute(common, "narrow", Y_SWAP)
    common_core = lax.ppermute(common, "narrow", CORE_SWAP)
    common_both = lax.ppermute(common_y, "narrow", CORE_SWAP)
    outputs = None
    for k in range(CHUNKS):
        hidden_both = lax.ppermute(hiddens[k][1], "narrow", CORE_SWAP)
        hiddens[k].insert(2, hidden_both)
        outputs = expert_columns(pos, k, hiddens[k], expert_down, others, outputs)
    returned = lax.all_to_all(outputs.reshape(EXPERTS, CAP, COLS), "wide", 0, 0, tiled=True)

    shared = list(shared_columns(place, [common, common_core, common_y, common_both], outward, outputs))
    for d in range(1, NX):
        shared[d] = lax.ppermute(shared[d], "wide", moved(-d, 0, 0))
    return combine(ids_t, gates_t, returned.reshape(SLOTS, COLS), shared)


def solution(mesh):
    in_specs = (
        P("wide", None),
        P("wide", None),
        P("wide", None),
        P("wide", "narrow"),
        P("wide", "narrow"),
        P("narrow", "wide"),
        P("wide", None, "narrow"),
        P("wide", None, "narrow"),
        P("wide", "narrow", None),
    )
    out_specs = P("wide", "narrow")
    return jax.shard_map(body, mesh=mesh, in_specs=in_specs, out_specs=out_specs, check_vma=False)
```

```python
import jax
import jax.numpy as jnp
from jax import lax
from jax.experimental import pallas as pl
from jax.experimental.pallas import tpu as pltpu
from jax.sharding import PartitionSpec as P


F32 = jnp.float32
BF16 = jnp.bfloat16
CAP = 16
EXPERTS = 64
SLOTS = EXPERTS * CAP
TOK = 128
D = 2048
FS = 2816
NX = 4
NY = 2
NZ = 8
PAIRS = NZ // 2
CORE_SWAP = [(0, 1), (1, 0), (2, 3), (3, 2)]
Y_SWAP = [(0, 2), (2, 0), (1, 3), (3, 1)]
BOTH_SWAP = [(0, 3), (3, 0), (1, 2), (2, 1)]
COLS = D // 4
CHUNKS = 2
CHUNK_ROWS = SLOTS // CHUNKS
STEP_ROWS = 256
NO_SLOT = 100.0


def moved(dx, flip, dz, pair=0):
    def index(x, y, z):
        return (x % NX * NY + y) * NZ + z % NZ

    return [
        (index(x, y, z), index(x + dx, y ^ flip, (z ^ pair) + dz))
        for x in range(NX)
        for y in range(NY)
        for z in range(NZ)
    ]


def turned_about(k):
    def index(x, y, z, n):
        return ((x * NY + y) * NZ + z) * 4 + n

    return [
        (index(x, y, z, n), index((n + k) % 4, y, z, x))
        for x in range(NX)
        for y in range(NY)
        for z in range(NZ)
        for n in range(4)
    ]


def silu(v):
    return v / (1.0 + jnp.exp(-v))


def dot(a, b):
    return lax.dot_general(a, b, (((1,), (0,)), ((), ())), preferred_element_type=F32)


def dot_nt(a, b):
    return lax.dot_general(a, b, (((1,), (1,)), ((), ())), preferred_element_type=F32)


def named_counts(ids, shape, k_axis):
    expert = lax.broadcasted_iota(jnp.int32, shape, k_axis).astype(F32)
    named = jnp.zeros(shape, F32)
    for k in range(ids.shape[k_axis]):
        one = ids[:, k : k + 1] if k_axis else ids[k : k + 1, :]
        named = named + jnp.where(one == expert, 1.0, 0.0)
    return named


def order_matrix(upper):
    row = lax.broadcasted_iota(jnp.int32, (TOK, TOK), 0)
    col = lax.broadcasted_iota(jnp.int32, (TOK, TOK), 1)
    before = row < col if upper else col < row
    return jnp.where(before, 1.0, 0.0).astype(BF16)


def dispatch_kernel(pos_ref, ids_ref, tok_ref, out_ref):
    del pos_ref
    rows = out_ref.shape[0]
    first = pl.program_id(0) * rows
    named = named_counts(ids_ref[...].astype(F32), (EXPERTS, TOK), 0)
    place = dot(named.astype(BF16), order_matrix(True))
    keys = jnp.where(named > 0.0, place, NO_SLOT).astype(BF16)
    r = lax.broadcasted_iota(jnp.int32, (rows, EXPERTS), 0) + first
    e = lax.broadcasted_iota(jnp.int32, (rows, EXPERTS), 1)
    spread = jnp.where((r >> 4) == e, 1.0, 0.0).astype(BF16)
    wanted = dot(spread, keys)
    slot = ((lax.broadcasted_iota(jnp.int32, (rows, TOK), 0) + first) & 15).astype(F32)
    pick = jnp.where(wanted == slot, 1.0, 0.0).astype(BF16)
    out_ref[...] = dot(pick, tok_ref[...]).astype(BF16)


def dispatch(pos, ids_t, tokens):
    blocks = 2
    rows = SLOTS // blocks
    return pl.pallas_call(
        dispatch_kernel,
        grid_spec=pltpu.PrefetchScalarGridSpec(
            num_scalar_prefetch=1,
            grid=(blocks,),
            in_specs=[
                pl.BlockSpec(ids_t.shape, lambda i, p: (0, 0)),
                pl.BlockSpec((TOK, COLS), lambda i, p: (0, p[0])),
            ],
            out_specs=pl.BlockSpec((rows, COLS), lambda i, p: (i, 0)),
        ),
        out_shape=jax.ShapeDtypeStruct((SLOTS, COLS), BF16),
        name="dispatch",
    )(pos, ids_t, tokens)


def padded_to(value, lanes):
    return jnp.concatenate([value, jnp.zeros((value.shape[0], lanes - value.shape[1]), F32)], axis=1)


def pack_kernel(gate_ref, up_ref, down_ref, out_ref):
    fs = gate_ref.shape[1] // NX
    inward, outward = lanes_of(fs)
    for i in range(NX):
        cut = slice(i * fs, (i + 1) * fs)
        both = jnp.concatenate([gate_ref[:, cut], up_ref[:, cut]], axis=1).astype(F32)
        out_ref[i, :, :inward] = padded_to(both, inward).astype(BF16)
        out_ref[i, :, inward:] = padded_to(down_ref[:, cut].astype(F32), outward).astype(BF16)


def lanes_of(fs):
    return -(-2 * fs // 128) * 128, -(-fs // 128) * 128


def pack(gate, up, down_t):
    return pl.pallas_call(
        pack_kernel,
        out_shape=jax.ShapeDtypeStruct((NX, gate.shape[0], sum(lanes_of(gate.shape[1] // NX))), BF16),
        name="pack",
    )(gate, up, down_t)


def deal_kernel(place_ref, *refs):
    raws, outs = refs[:4], refs[4:]
    n, x, y, z = place_ref[0], place_ref[1], place_ref[2], place_ref[3]
    rows = raws[0].shape[1]
    inward = outs[0].shape[1]
    for i, raw in enumerate(raws):
        at = ((y ^ (i & 1)) * 2 + ((z & 1) ^ (i >> 1))) * rows
        to = pl.ds(pl.multiple_of(at, rows), rows)
        for d in range(NX):
            outs[d][to, :] = raw[pl.ds((x + d) & 3, 1), :, :inward].reshape(rows, inward)
            outs[NX + d][to, :] = raw[pl.ds((n + d) & 3, 1), :, inward:].reshape(
                rows, raw.shape[2] - inward
            )


def deal(place, raws, fs):
    inward, outward = lanes_of(fs)
    rows = 4 * raws[0].shape[1]
    vmem = pl.BlockSpec(memory_space=pltpu.VMEM)
    return pl.pallas_call(
        deal_kernel,
        in_specs=[pl.BlockSpec(memory_space=pltpu.SMEM)] + [vmem] * 4,
        out_specs=[vmem] * 8,
        out_shape=[jax.ShapeDtypeStruct((rows, inward), BF16)] * 4
        + [jax.ShapeDtypeStruct((rows, outward), BF16)] * 4,
        name="deal",
    )(place, *raws)


def stack_kernel(place_ref, *refs):
    pieces, out_ref = refs[:8], refs[8]
    x = place_ref[1]
    lanes = pieces[0].shape[1]
    for d in range(NX):
        at = (x - d) & 3
        out_ref[pl.ds(at, 1), :, :lanes] = pieces[d][...][None]
        out_ref[pl.ds(at, 1), :, lanes:] = pieces[NX + d][...][None]


def stack(place, pieces):
    vmem = pl.BlockSpec(memory_space=pltpu.VMEM)
    lanes = pieces[0].shape[1] + pieces[NX].shape[1]
    return pl.pallas_call(
        stack_kernel,
        in_specs=[pl.BlockSpec(memory_space=pltpu.SMEM)] + [vmem] * 8,
        out_specs=vmem,
        out_shape=jax.ShapeDtypeStruct((NX, pieces[0].shape[0], lanes), BF16),
        name="stack",
    )(place, *pieces)


def cut_kernel(pos_ref, a, b, c, out_a, out_b, out_c):
    del pos_ref
    out_a[...] = a[0]
    out_b[...] = b[0]
    out_c[...] = c[0]


def cut(pos, w_down):
    mf = w_down.shape[1]
    return pl.pallas_call(
        cut_kernel,
        grid_spec=pltpu.PrefetchScalarGridSpec(
            num_scalar_prefetch=1,
            grid=(1,),
            in_specs=[
                pl.BlockSpec((1, mf, COLS), lambda i, p: (0, 0, p[0] ^ 2)),
                pl.BlockSpec((1, mf, COLS), lambda i, p: (0, 0, p[0] ^ 3)),
                pl.BlockSpec((1, mf, COLS), lambda i, p: (0, 0, p[0] ^ 1)),
            ],
            out_specs=[pl.BlockSpec((mf, COLS), lambda i, p: (0, 0))] * 3,
        ),
        out_shape=[jax.ShapeDtypeStruct((mf, COLS), BF16)] * 3,
        name="cut",
    )(pos, w_down, w_down, w_down)


def hidden_kernel(pos_ref, x0, x1, x2, x3, g0, g1, g2, g3, u0, u1, u2, u3, out_ref):
    del pos_ref
    gate = jnp.zeros((x0.shape[0], g0.shape[1]), F32)
    up = gate
    for x, g, u in ((x0, g0, u0), (x1, g1, u1), (x2, g2, u2), (x3, g3, u3)):
        rows = x[...]
        gate = gate + dot_nt(rows, g[0])
        up = up + dot_nt(rows, u[0])
    mf = gate.shape[1]
    out_ref[:, :mf] = (silu(gate) * up).astype(BF16)
    out_ref[:, mf:] = jnp.zeros((gate.shape[0], out_ref.shape[1] - mf), BF16)


def expert_hidden(pos, chunk, own, core, y, both, w_gate, w_up):
    steps = CHUNK_ROWS // STEP_ROWS
    mf = w_gate.shape[1]
    padded = -(-mf // 128) * 128
    whole = pl.BlockSpec((STEP_ROWS, COLS), lambda i, p: (chunk * steps + i, 0))
    part = pl.BlockSpec((STEP_ROWS, COLS), lambda i, p: (i, 0))
    w_specs = [
        pl.BlockSpec((1, mf, COLS), lambda i, p: (0, 0, p[0])),
        pl.BlockSpec((1, mf, COLS), lambda i, p: (0, 0, p[0] ^ 1)),
        pl.BlockSpec((1, mf, COLS), lambda i, p: (0, 0, p[0] ^ 2)),
        pl.BlockSpec((1, mf, COLS), lambda i, p: (0, 0, p[0] ^ 3)),
    ]
    return pl.pallas_call(
        hidden_kernel,
        grid_spec=pltpu.PrefetchScalarGridSpec(
            num_scalar_prefetch=1,
            grid=(steps,),
            in_specs=[whole, whole, part, part] + w_specs + w_specs,
            out_specs=pl.BlockSpec((STEP_ROWS, padded), lambda i, p: (i, 0)),
        ),
        out_shape=jax.ShapeDtypeStruct((CHUNK_ROWS, padded), BF16),
        cost_estimate=pl.CostEstimate(
            flops=4 * CHUNK_ROWS * D * mf, bytes_accessed=6_000_000, transcendentals=CHUNK_ROWS * mf
        ),
        name="hidden",
    )(pos, own, core, y, both, *[w_gate] * 4, *[w_up] * 4)


def down_kernel(pos_ref, h0, h1, h2, h3, w0, w1, w2, w3, *rest):
    del pos_ref
    out_ref = rest[-1]
    mf = w1.shape[0]
    total = dot(h0[:, :mf], w0[0])
    for h, w in ((h1, w1), (h2, w2), (h3, w3)):
        total = total + dot(h[:, :mf], w[...])
    out_ref[...] = total.astype(BF16)


def expert_columns(pos, chunk, hiddens, w_own, w_others, so_far):
    steps = CHUNK_ROWS // STEP_ROWS
    mf = w_own.shape[1]
    h_spec = pl.BlockSpec((STEP_ROWS, hiddens[0].shape[1]), lambda i, p: (i, 0))
    w_spec = pl.BlockSpec((mf, COLS), lambda i, p: (0, 0))
    more = [] if so_far is None else [so_far]
    return pl.pallas_call(
        down_kernel,
        grid_spec=pltpu.PrefetchScalarGridSpec(
            num_scalar_prefetch=1,
            grid=(steps,),
            in_specs=[h_spec] * 4
            + [pl.BlockSpec((1, mf, COLS), lambda i, p: (0, 0, p[0]))]
            + [w_spec] * 3
            + [pl.BlockSpec(memory_space=pl.ANY)] * len(more),
            out_specs=pl.BlockSpec((STEP_ROWS, COLS), lambda i, p: (chunk * steps + i, 0)),
        ),
        out_shape=jax.ShapeDtypeStruct((SLOTS, COLS), BF16),
        input_output_aliases={9: 0} if more else {},
        cost_estimate=pl.CostEstimate(
            flops=8 * CHUNK_ROWS * COLS * mf, bytes_accessed=4_000_000, transcendentals=0
        ),
        name="down",
    )(pos, *hiddens, w_own, *w_others, *more)


def fetch(blocks, w_ref, sems, z, first):
    copies = []
    for step, block in enumerate(blocks):
        part = block.at[:, :, :, pl.ds(first, w_ref.shape[4])]
        copies.append(pltpu.make_async_copy(part, w_ref.at[((z >> 1) - step) & (PAIRS - 1)], sems.at[step]))
    for copy in copies:
        copy.start()
    for copy in copies:
        copy.wait()


def shared_hidden_kernel(place_ref, t0, t1, t2, t3, *refs):
    blocks, (out_ref, w_ref, sems) = refs[:PAIRS], refs[PAIRS + 1 :]
    z = place_ref[3]
    fetch(blocks, w_ref, sems, z, 0)
    rows = PAIRS * w_ref.shape[3]
    lanes = w_ref.shape[4]
    fs = FS // (4 * NX)
    total = jnp.zeros((NX * TOK, lanes), F32)
    for quarter in range(NX):
        for half in range(NY):
            w = w_ref[:, quarter, half].reshape(rows, lanes)
            first = (quarter * NY + half) * rows
            tok = jnp.concatenate([t[:, first : first + rows] for t in (t0, t1, t2, t3)], axis=0)
            total = total + dot(tok, w)
    hidden = silu(total[:, :fs]) * total[:, fs : 2 * fs]
    out_ref[...] = padded_to(hidden, out_ref.shape[1]).astype(BF16)


def shared_hidden(place, toks, blocks, after, lanes, units):
    vmem = pl.BlockSpec(memory_space=pltpu.VMEM)
    return pl.pallas_call(
        shared_hidden_kernel,
        in_specs=[pl.BlockSpec(memory_space=pltpu.SMEM)]
        + [vmem] * 4
        + [pl.BlockSpec(memory_space=pl.ANY)] * (PAIRS + 1),
        out_specs=vmem,
        out_shape=jax.ShapeDtypeStruct((NX * TOK, units), BF16),
        scratch_shapes=[
            pltpu.VMEM((PAIRS,) + blocks[0].shape[:3] + (lanes,), BF16),
            pltpu.SemaphoreType.DMA((PAIRS,)),
        ],
        cost_estimate=pl.CostEstimate(
            flops=2 * NX * TOK * D * lanes, bytes_accessed=5_000_000, transcendentals=NX * TOK * units
        ),
        name="shared_hidden",
    )(place, *toks, *blocks, after)


def shared_down_kernel(place_ref, h0, h1, h2, h3, *refs):
    blocks, outs, (w_ref, sems) = refs[:PAIRS], refs[PAIRS + 1 : PAIRS + 5], refs[PAIRS + 5 :]
    n, z = place_ref[0], place_ref[3]
    units = w_ref.shape[4]
    fetch(blocks, w_ref, sems, z, blocks[0].shape[3] - units)
    rows = PAIRS * w_ref.shape[3]
    for half in range(NY):
        total = jnp.zeros((NX * TOK, rows), F32)
        for j, h in enumerate((h0, h1, h2, h3)):
            w = w_ref[:, pl.ds(n ^ j, 1), half].reshape(rows, units)
            total = total + dot_nt(h[...], w)
        for d in range(NX):
            outs[d][:, half * rows : (half + 1) * rows] = total[d * TOK : (d + 1) * TOK].astype(BF16)


def shared_columns(place, hiddens, blocks, after):
    vmem = pl.BlockSpec(memory_space=pltpu.VMEM)
    units = hiddens[0].shape[1]
    return pl.pallas_call(
        shared_down_kernel,
        in_specs=[pl.BlockSpec(memory_space=pltpu.SMEM)]
        + [vmem] * 4
        + [pl.BlockSpec(memory_space=pl.ANY)] * (PAIRS + 1),
        out_specs=[vmem] * 4,
        out_shape=[jax.ShapeDtypeStruct((TOK, COLS), BF16)] * 4,
        scratch_shapes=[
            pltpu.VMEM((PAIRS,) + blocks[0].shape[:3] + (units,), BF16),
            pltpu.SemaphoreType.DMA((PAIRS,)),
        ],
        cost_estimate=pl.CostEstimate(
            flops=2 * NX * TOK * D * units, bytes_accessed=4_000_000, transcendentals=0
        ),
        name="shared_down",
    )(place, *hiddens, *blocks, after)


def turned(values):
    row = lax.broadcasted_iota(jnp.int32, (TOK, TOK), 0)
    col = lax.broadcasted_iota(jnp.int32, (TOK, TOK), 1)
    eye = jnp.where(row == col, 1.0, 0.0).astype(BF16)
    total = None
    rest = values
    for _ in range(3):
        part = rest.astype(BF16)
        rest = rest - part.astype(F32)
        moved = dot_nt(eye, part)
        total = moved if total is None else total + moved
    return total


def combine_kernel(ids_ref, gw_ref, ret_ref, s0, s1, s2, s3, out_ref):
    ids = turned(ids_ref[...].astype(F32))
    gates = turned(gw_ref[...])
    named = named_counts(ids, (TOK, EXPERTS), 1)
    place = dot(order_matrix(False), named.astype(BF16))
    keys = jnp.where(named > 0.0, place, NO_SLOT).astype(BF16)
    lane = lax.broadcasted_iota(jnp.int32, (TOK, EXPERTS), 1).astype(F32)
    weight = jnp.zeros((TOK, EXPERTS), F32)
    for k in range(ids.shape[1]):
        weight = weight + jnp.where(ids[:, k : k + 1] == lane, gates[:, k : k + 1], 0.0)
    e = lax.broadcasted_iota(jnp.int32, (EXPERTS, SLOTS), 0)
    r = lax.broadcasted_iota(jnp.int32, (EXPERTS, SLOTS), 1)
    spread = jnp.where((r >> 4) == e, 1.0, 0.0).astype(BF16)
    slot = (lax.broadcasted_iota(jnp.int32, (TOK, SLOTS), 1) & 15).astype(F32)
    hit = dot(keys, spread) == slot
    ret = ret_ref[...]
    total = s0[...].astype(F32)
    for part in (s1, s2, s3):
        total = total + part[...].astype(F32)
    rest = weight
    for _ in range(3):
        part = rest.astype(BF16)
        rest = rest - part.astype(F32)
        row = jnp.where(hit, dot(part, spread), 0.0).astype(BF16)
        total = total + dot(row, ret)
    out_ref[...] = total.astype(BF16)


def combine(ids, gate_weights, returned, shared):
    return pl.pallas_call(
        combine_kernel,
        out_shape=jax.ShapeDtypeStruct((TOK, COLS), BF16),
        name="combine",
    )(ids, gate_weights, returned, *shared)


def body(
    tokens,
    expert_ids,
    gate_weights,
    shared_gate,
    shared_up,
    shared_down,
    expert_gate,
    expert_up,
    expert_down,
):
    pos = lax.axis_index("narrow").astype(jnp.int32).reshape(1)
    ids_t = expert_ids.T
    gates_t = gate_weights.T
    gate_t = expert_gate.transpose(0, 2, 1)
    up_t = expert_up.transpose(0, 2, 1)

    wide = lax.axis_index("wide").astype(jnp.int32)
    place = jnp.stack([pos[0], wide >> 4, (wide >> 3) & 1, wide & 7])

    raw = pack(shared_gate, shared_up, shared_down.T)
    raws = [raw] + [lax.ppermute(raw, "wide", moved(0, i & 1, 0, i >> 1)) for i in (1, 2, 3)]

    outgoing = dispatch(pos, ids_t, tokens).reshape(EXPERTS, CAP, COLS)
    own = lax.all_to_all(outgoing, "wide", 0, 0, tiled=True).reshape(SLOTS, COLS)

    pieces = list(deal(place, raws, shared_gate.shape[1] // NX))
    for d in range(NX):
        pieces[NX + d] = lax.ppermute(pieces[NX + d], ("wide", "narrow"), turned_about(d))
    for d in range(1, NX):
        pieces[d] = lax.ppermute(pieces[d], "wide", moved(d, 0, 0))
    cuts = cut(pos, expert_down)
    others = [
        lax.ppermute(w, "narrow", swap)
        for w, swap in zip(cuts, (Y_SWAP, BOTH_SWAP, CORE_SWAP))
    ]
    column = stack(place, pieces)
    column = column.reshape(NX, NY, column.shape[1] // NY, column.shape[2])
    blocks = [column]
    for k in range(1, PAIRS):
        blocks.append(lax.ppermute(column, "wide", moved(0, 0, 2 * k)))
    toks = [tokens]
    for d in range(1, NX):
        toks.append(lax.ppermute(tokens, "wide", moved(d, 0, 0)))

    ys = []
    for k in range(CHUNKS):
        ys.append(lax.ppermute(own[k * CHUNK_ROWS : (k + 1) * CHUNK_ROWS], "narrow", Y_SWAP))
    core = lax.ppermute(own, "narrow", CORE_SWAP)
    hiddens = []
    for k in range(CHUNKS):
        both = lax.ppermute(ys[k], "narrow", CORE_SWAP)
        hidden = expert_hidden(pos, k, own, core, ys[k], both, gate_t, up_t)
        hidden_y = lax.ppermute(hidden, "narrow", Y_SWAP)
        hidden_core = lax.ppermute(hidden, "narrow", CORE_SWAP)
        hiddens.append([hidden, hidden_y, hidden_core])
    lanes, units = pieces[0].shape[1], pieces[NX].shape[1]
    common = shared_hidden(place, toks, blocks, hiddens[-1][0], lanes, units)
    common_y = lax.ppermute(common, "narrow", Y_SWAP)
    common_core = lax.ppermute(common, "narrow", CORE_SWAP)
    common_both = lax.ppermute(common_y, "narrow", CORE_SWAP)
    outputs = None
    for k in range(CHUNKS):
        hidden_both = lax.ppermute(hiddens[k][1], "narrow", CORE_SWAP)
        hiddens[k].insert(2, hidden_both)
        outputs = expert_columns(pos, k, hiddens[k], expert_down, others, outputs)
    returned = lax.all_to_all(outputs.reshape(EXPERTS, CAP, COLS), "wide", 0, 0, tiled=True)

    shared = list(shared_columns(place, [common, common_core, common_y, common_both], blocks, outputs))
    for d in range(1, NX):
        shared[d] = lax.ppermute(shared[d], "wide", moved(-d, 0, 0))
    return combine(ids_t, gates_t, returned.reshape(SLOTS, COLS), shared)


def solution(mesh):
    in_specs = (
        P("wide", None),
        P("wide", None),
        P("wide", None),
        P("wide", "narrow"),
        P("wide", "narrow"),
        P("narrow", "wide"),
        P("wide", None, "narrow"),
        P("wide", None, "narrow"),
        P("wide", "narrow", None),
    )
    out_specs = P("wide", "narrow")
    return jax.shard_map(body, mesh=mesh, in_specs=in_specs, out_specs=out_specs, check_vma=False)
```

```python
import jax
import jax.numpy as jnp
from jax import lax
from jax.experimental import pallas as pl
from jax.experimental.pallas import tpu as pltpu
from jax.sharding import PartitionSpec as P


F32 = jnp.float32
BF16 = jnp.bfloat16
CAP = 16
EXPERTS = 64
SLOTS = EXPERTS * CAP
TOK = 128
D = 2048
FS = 2816
NX = 4
NY = 2
NZ = 8
PAIRS = NZ // 2
CORE_SWAP = [(0, 1), (1, 0), (2, 3), (3, 2)]
Y_SWAP = [(0, 2), (2, 0), (1, 3), (3, 1)]
BOTH_SWAP = [(0, 3), (3, 0), (1, 2), (2, 1)]
COLS = D // 4
CHUNKS = 2
CHUNK_ROWS = SLOTS // CHUNKS
STEP_ROWS = 256
NO_SLOT = 100.0


def moved(dx, flip, dz, pair=0):
    def index(x, y, z):
        return (x % NX * NY + y) * NZ + z % NZ

    return [
        (index(x, y, z), index(x + dx, y ^ flip, (z ^ pair) + dz))
        for x in range(NX)
        for y in range(NY)
        for z in range(NZ)
    ]


def turned_about(k):
    def index(x, y, z, n):
        return ((x * NY + y) * NZ + z) * 4 + n

    return [
        (index(x, y, z, n), index((n + k) % 4, y, z, x))
        for x in range(NX)
        for y in range(NY)
        for z in range(NZ)
        for n in range(4)
    ]


def silu(v):
    return v / (1.0 + jnp.exp(-v))


def dot(a, b):
    return lax.dot_general(a, b, (((1,), (0,)), ((), ())), preferred_element_type=F32)


def dot_nt(a, b):
    return lax.dot_general(a, b, (((1,), (1,)), ((), ())), preferred_element_type=F32)


def named_counts(ids, shape, k_axis):
    expert = lax.broadcasted_iota(jnp.int32, shape, k_axis).astype(F32)
    named = jnp.zeros(shape, F32)
    for k in range(ids.shape[k_axis]):
        one = ids[:, k : k + 1] if k_axis else ids[k : k + 1, :]
        named = named + jnp.where(one == expert, 1.0, 0.0)
    return named


def order_matrix(upper):
    row = lax.broadcasted_iota(jnp.int32, (TOK, TOK), 0)
    col = lax.broadcasted_iota(jnp.int32, (TOK, TOK), 1)
    before = row < col if upper else col < row
    return jnp.where(before, 1.0, 0.0).astype(BF16)


def dispatch_kernel(pos_ref, ids_ref, tok_ref, out_ref):
    del pos_ref
    rows = out_ref.shape[0]
    first = pl.program_id(0) * rows
    named = named_counts(ids_ref[...].astype(F32), (EXPERTS, TOK), 0)
    place = dot(named.astype(BF16), order_matrix(True))
    keys = jnp.where(named > 0.0, place, NO_SLOT).astype(BF16)
    r = lax.broadcasted_iota(jnp.int32, (rows, EXPERTS), 0) + first
    e = lax.broadcasted_iota(jnp.int32, (rows, EXPERTS), 1)
    spread = jnp.where((r >> 4) == e, 1.0, 0.0).astype(BF16)
    wanted = dot(spread, keys)
    slot = ((lax.broadcasted_iota(jnp.int32, (rows, TOK), 0) + first) & 15).astype(F32)
    pick = jnp.where(wanted == slot, 1.0, 0.0).astype(BF16)
    out_ref[...] = dot(pick, tok_ref[...]).astype(BF16)


def dispatch(pos, ids_t, tokens):
    blocks = 2
    rows = SLOTS // blocks
    return pl.pallas_call(
        dispatch_kernel,
        grid_spec=pltpu.PrefetchScalarGridSpec(
            num_scalar_prefetch=1,
            grid=(blocks,),
            in_specs=[
                pl.BlockSpec(ids_t.shape, lambda i, p: (0, 0)),
                pl.BlockSpec((TOK, COLS), lambda i, p: (0, p[0])),
            ],
            out_specs=pl.BlockSpec((rows, COLS), lambda i, p: (i, 0)),
        ),
        out_shape=jax.ShapeDtypeStruct((SLOTS, COLS), BF16),
        name="dispatch",
    )(pos, ids_t, tokens)


def padded_to(value, lanes):
    return jnp.concatenate([value, jnp.zeros((value.shape[0], lanes - value.shape[1]), F32)], axis=1)


def pack_kernel(gate_ref, up_ref, down_ref, out_ref):
    fs = gate_ref.shape[1] // NX
    inward, outward = lanes_of(fs)
    for i in range(NX):
        cut = slice(i * fs, (i + 1) * fs)
        both = jnp.concatenate([gate_ref[:, cut], up_ref[:, cut]], axis=1).astype(F32)
        out_ref[i, :, :inward] = padded_to(both, inward).astype(BF16)
        out_ref[i, :, inward:] = padded_to(down_ref[:, cut].astype(F32), outward).astype(BF16)


def lanes_of(fs):
    return -(-2 * fs // 128) * 128, -(-fs // 128) * 128


def pack(gate, up, down_t):
    return pl.pallas_call(
        pack_kernel,
        out_shape=jax.ShapeDtypeStruct((NX, gate.shape[0], sum(lanes_of(gate.shape[1] // NX))), BF16),
        name="pack",
    )(gate, up, down_t)


def deal_kernel(place_ref, *refs):
    raws, outs = refs[:4], refs[4:]
    n, x, y, z = place_ref[0], place_ref[1], place_ref[2], place_ref[3]
    rows = raws[0].shape[1]
    inward = outs[0].shape[1]
    for i, raw in enumerate(raws):
        at = ((y ^ (i & 1)) * 2 + ((z & 1) ^ (i >> 1))) * rows
        to = pl.ds(pl.multiple_of(at, rows), rows)
        for d in range(NX):
            outs[d][to, :] = raw[pl.ds((x + d) & 3, 1), :, :inward].reshape(rows, inward)
            outs[NX + d][to, :] = raw[pl.ds((n + d) & 3, 1), :, inward:].reshape(
                rows, raw.shape[2] - inward
            )


def deal(place, raws, fs):
    inward, outward = lanes_of(fs)
    rows = 4 * raws[0].shape[1]
    vmem = pl.BlockSpec(memory_space=pltpu.VMEM)
    return pl.pallas_call(
        deal_kernel,
        in_specs=[pl.BlockSpec(memory_space=pltpu.SMEM)] + [vmem] * 4,
        out_specs=[vmem] * 8,
        out_shape=[jax.ShapeDtypeStruct((rows, inward), BF16)] * 4
        + [jax.ShapeDtypeStruct((rows, outward), BF16)] * 4,
        name="deal",
    )(place, *raws)


def stack_kernel(place_ref, *refs):
    pieces, out_ref = refs[:8], refs[8]
    x = place_ref[1]
    lanes = pieces[0].shape[1]
    for d in range(NX):
        at = (x - d) & 3
        out_ref[pl.ds(at, 1), :, :lanes] = pieces[d][...][None]
        out_ref[pl.ds(at, 1), :, lanes:] = pieces[NX + d][...][None]


def stack(place, pieces):
    vmem = pl.BlockSpec(memory_space=pltpu.VMEM)
    lanes = pieces[0].shape[1] + pieces[NX].shape[1]
    return pl.pallas_call(
        stack_kernel,
        in_specs=[pl.BlockSpec(memory_space=pltpu.SMEM)] + [vmem] * 8,
        out_specs=vmem,
        out_shape=jax.ShapeDtypeStruct((NX, pieces[0].shape[0], lanes), BF16),
        name="stack",
    )(place, *pieces)


def cut_kernel(pos_ref, a, b, c, out_a, out_b, out_c):
    del pos_ref
    out_a[...] = a[0]
    out_b[...] = b[0]
    out_c[...] = c[0]


def cut(pos, w_down):
    mf = w_down.shape[1]
    return pl.pallas_call(
        cut_kernel,
        grid_spec=pltpu.PrefetchScalarGridSpec(
            num_scalar_prefetch=1,
            grid=(1,),
            in_specs=[
                pl.BlockSpec((1, mf, COLS), lambda i, p: (0, 0, p[0] ^ 2)),
                pl.BlockSpec((1, mf, COLS), lambda i, p: (0, 0, p[0] ^ 3)),
                pl.BlockSpec((1, mf, COLS), lambda i, p: (0, 0, p[0] ^ 1)),
            ],
            out_specs=[pl.BlockSpec((mf, COLS), lambda i, p: (0, 0))] * 3,
        ),
        out_shape=[jax.ShapeDtypeStruct((mf, COLS), BF16)] * 3,
        name="cut",
    )(pos, w_down, w_down, w_down)


def hidden_kernel(pos_ref, x0, x1, x2, x3, g0, g1, g2, g3, u0, u1, u2, u3, out_ref):
    del pos_ref
    gate = jnp.zeros((x0.shape[0], g0.shape[1]), F32)
    up = gate
    for x, g, u in ((x0, g0, u0), (x1, g1, u1), (x2, g2, u2), (x3, g3, u3)):
        rows = x[...]
        gate = gate + dot_nt(rows, g[0])
        up = up + dot_nt(rows, u[0])
    mf = gate.shape[1]
    out_ref[:, :mf] = (silu(gate) * up).astype(BF16)
    out_ref[:, mf:] = jnp.zeros((gate.shape[0], out_ref.shape[1] - mf), BF16)


def expert_hidden(pos, chunk, own, core, y, both, w_gate, w_up):
    steps = CHUNK_ROWS // STEP_ROWS
    mf = w_gate.shape[1]
    padded = -(-mf // 128) * 128
    whole = pl.BlockSpec((STEP_ROWS, COLS), lambda i, p: (chunk * steps + i, 0))
    part = pl.BlockSpec((STEP_ROWS, COLS), lambda i, p: (i, 0))
    w_specs = [
        pl.BlockSpec((1, mf, COLS), lambda i, p: (0, 0, p[0])),
        pl.BlockSpec((1, mf, COLS), lambda i, p: (0, 0, p[0] ^ 1)),
        pl.BlockSpec((1, mf, COLS), lambda i, p: (0, 0, p[0] ^ 2)),
        pl.BlockSpec((1, mf, COLS), lambda i, p: (0, 0, p[0] ^ 3)),
    ]
    return pl.pallas_call(
        hidden_kernel,
        grid_spec=pltpu.PrefetchScalarGridSpec(
            num_scalar_prefetch=1,
            grid=(steps,),
            in_specs=[whole, whole, part, part] + w_specs + w_specs,
            out_specs=pl.BlockSpec((STEP_ROWS, padded), lambda i, p: (i, 0)),
        ),
        out_shape=jax.ShapeDtypeStruct((CHUNK_ROWS, padded), BF16),
        cost_estimate=pl.CostEstimate(
            flops=4 * CHUNK_ROWS * D * mf, bytes_accessed=6_000_000, transcendentals=CHUNK_ROWS * mf
        ),
        name="hidden",
    )(pos, own, core, y, both, *[w_gate] * 4, *[w_up] * 4)


def down_kernel(pos_ref, h0, h1, h2, h3, w0, w1, w2, w3, *rest):
    del pos_ref
    out_ref = rest[-1]
    mf = w1.shape[0]
    total = dot(h0[:, :mf], w0[0])
    for h, w in ((h1, w1), (h2, w2), (h3, w3)):
        total = total + dot(h[:, :mf], w[...])
    out_ref[...] = total.astype(BF16)


def expert_columns(pos, chunk, hiddens, w_own, w_others, so_far):
    steps = CHUNK_ROWS // STEP_ROWS
    mf = w_own.shape[1]
    h_spec = pl.BlockSpec((STEP_ROWS, hiddens[0].shape[1]), lambda i, p: (i, 0))
    w_spec = pl.BlockSpec((mf, COLS), lambda i, p: (0, 0))
    more = [] if so_far is None else [so_far]
    return pl.pallas_call(
        down_kernel,
        grid_spec=pltpu.PrefetchScalarGridSpec(
            num_scalar_prefetch=1,
            grid=(steps,),
            in_specs=[h_spec] * 4
            + [pl.BlockSpec((1, mf, COLS), lambda i, p: (0, 0, p[0]))]
            + [w_spec] * 3
            + [pl.BlockSpec(memory_space=pl.ANY)] * len(more),
            out_specs=pl.BlockSpec((STEP_ROWS, COLS), lambda i, p: (chunk * steps + i, 0)),
        ),
        out_shape=jax.ShapeDtypeStruct((SLOTS, COLS), BF16),
        input_output_aliases={9: 0} if more else {},
        cost_estimate=pl.CostEstimate(
            flops=8 * CHUNK_ROWS * COLS * mf, bytes_accessed=4_000_000, transcendentals=0
        ),
        name="down",
    )(pos, *hiddens, w_own, *w_others, *more)


def fetch(blocks, w_ref, sems, z, first):
    copies = []
    for step, block in enumerate(blocks):
        part = block.at[:, :, :, pl.ds(first, w_ref.shape[4])]
        copies.append(pltpu.make_async_copy(part, w_ref.at[((z >> 1) - step) & (PAIRS - 1)], sems.at[step]))
    for copy in copies:
        copy.start()
    for copy in copies:
        copy.wait()


def shared_hidden_kernel(place_ref, t0, t1, t2, t3, *refs):
    blocks, (out_ref, w_ref, sems) = refs[:PAIRS], refs[PAIRS + 1 :]
    z = place_ref[3]
    fetch(blocks, w_ref, sems, z, 0)
    rows = PAIRS * w_ref.shape[3]
    lanes = w_ref.shape[4]
    fs = FS // (4 * NX)
    total = jnp.zeros((NX * TOK, lanes), F32)
    for quarter in range(NX):
        for half in range(NY):
            w = w_ref[:, quarter, half].reshape(rows, lanes)
            first = (quarter * NY + half) * rows
            tok = jnp.concatenate([t[:, first : first + rows] for t in (t0, t1, t2, t3)], axis=0)
            total = total + dot(tok, w)
    hidden = silu(total[:, :fs]) * total[:, fs : 2 * fs]
    out_ref[...] = padded_to(hidden, out_ref.shape[1]).astype(BF16)


def shared_hidden(place, toks, blocks, after, lanes, units):
    vmem = pl.BlockSpec(memory_space=pltpu.VMEM)
    return pl.pallas_call(
        shared_hidden_kernel,
        in_specs=[pl.BlockSpec(memory_space=pltpu.SMEM)]
        + [vmem] * 4
        + [pl.BlockSpec(memory_space=pl.ANY)] * (PAIRS + 1),
        out_specs=vmem,
        out_shape=jax.ShapeDtypeStruct((NX * TOK, units), BF16),
        scratch_shapes=[
            pltpu.VMEM((PAIRS,) + blocks[0].shape[:3] + (lanes,), BF16),
            pltpu.SemaphoreType.DMA((PAIRS,)),
        ],
        cost_estimate=pl.CostEstimate(
            flops=2 * NX * TOK * D * lanes, bytes_accessed=5_000_000, transcendentals=NX * TOK * units
        ),
        name="shared_hidden",
    )(place, *toks, *blocks, after)


def shared_down_kernel(place_ref, h0, h1, h2, h3, *refs):
    blocks, outs, (w_ref, sems) = refs[:PAIRS], refs[PAIRS + 1 : PAIRS + 5], refs[PAIRS + 5 :]
    n, z = place_ref[0], place_ref[3]
    units = w_ref.shape[4]
    fetch(blocks, w_ref, sems, z, blocks[0].shape[3] - units)
    rows = PAIRS * w_ref.shape[3]
    for half in range(NY):
        total = jnp.zeros((NX * TOK, rows), F32)
        for j, h in enumerate((h0, h1, h2, h3)):
            w = w_ref[:, pl.ds(n ^ j, 1), half].reshape(rows, units)
            total = total + dot_nt(h[...], w)
        for d in range(NX):
            outs[d][:, half * rows : (half + 1) * rows] = total[d * TOK : (d + 1) * TOK].astype(BF16)


def shared_columns(place, hiddens, blocks, after):
    vmem = pl.BlockSpec(memory_space=pltpu.VMEM)
    units = hiddens[0].shape[1]
    return pl.pallas_call(
        shared_down_kernel,
        in_specs=[pl.BlockSpec(memory_space=pltpu.SMEM)]
        + [vmem] * 4
        + [pl.BlockSpec(memory_space=pl.ANY)] * (PAIRS + 1),
        out_specs=[vmem] * 4,
        out_shape=[jax.ShapeDtypeStruct((TOK, COLS), BF16)] * 4,
        scratch_shapes=[
            pltpu.VMEM((PAIRS,) + blocks[0].shape[:3] + (units,), BF16),
            pltpu.SemaphoreType.DMA((PAIRS,)),
        ],
        cost_estimate=pl.CostEstimate(
            flops=2 * NX * TOK * D * units, bytes_accessed=4_000_000, transcendentals=0
        ),
        name="shared_down",
    )(place, *hiddens, *blocks, after)


def turned(values):
    row = lax.broadcasted_iota(jnp.int32, (TOK, TOK), 0)
    col = lax.broadcasted_iota(jnp.int32, (TOK, TOK), 1)
    eye = jnp.where(row == col, 1.0, 0.0).astype(BF16)
    total = None
    rest = values
    for _ in range(3):
        part = rest.astype(BF16)
        rest = rest - part.astype(F32)
        moved = dot_nt(eye, part)
        total = moved if total is None else total + moved
    return total


def weigh_kernel(ids_ref, gw_ref, out_ref):
    ids = turned(ids_ref[...].astype(F32))
    gates = turned(gw_ref[...])
    named = named_counts(ids, (TOK, EXPERTS), 1)
    place = dot(order_matrix(False), named.astype(BF16))
    keys = jnp.where(named > 0.0, place, NO_SLOT).astype(BF16)
    lane = lax.broadcasted_iota(jnp.int32, (TOK, EXPERTS), 1).astype(F32)
    weight = jnp.zeros((TOK, EXPERTS), F32)
    for k in range(ids.shape[1]):
        weight = weight + jnp.where(ids[:, k : k + 1] == lane, gates[:, k : k + 1], 0.0)
    e = lax.broadcasted_iota(jnp.int32, (EXPERTS, SLOTS), 0)
    r = lax.broadcasted_iota(jnp.int32, (EXPERTS, SLOTS), 1)
    spread = jnp.where((r >> 4) == e, 1.0, 0.0).astype(BF16)
    slot = (lax.broadcasted_iota(jnp.int32, (TOK, SLOTS), 1) & 15).astype(F32)
    hit = dot(keys, spread) == slot
    rest = weight
    for i in range(3):
        part = rest.astype(BF16)
        rest = rest - part.astype(F32)
        out_ref[i] = jnp.where(hit, dot(part, spread), 0.0).astype(BF16)


def weigh(ids, gate_weights):
    return pl.pallas_call(
        weigh_kernel,
        out_shape=jax.ShapeDtypeStruct((3, TOK, SLOTS), BF16),
        name="weigh",
    )(ids, gate_weights)


def combine_kernel(rows_ref, ret_ref, s0, s1, s2, s3, out_ref):
    ret = ret_ref[...]
    total = s0[...].astype(F32)
    for part in (s1, s2, s3):
        total = total + part[...].astype(F32)
    for i in range(3):
        total = total + dot(rows_ref[i], ret)
    out_ref[...] = total.astype(BF16)


def combine(rows, returned, shared):
    return pl.pallas_call(
        combine_kernel,
        out_shape=jax.ShapeDtypeStruct((TOK, COLS), BF16),
        name="combine",
    )(rows, returned, *shared)


def body(
    tokens,
    expert_ids,
    gate_weights,
    shared_gate,
    shared_up,
    shared_down,
    expert_gate,
    expert_up,
    expert_down,
):
    pos = lax.axis_index("narrow").astype(jnp.int32).reshape(1)
    ids_t = expert_ids.T
    gates_t = gate_weights.T
    gate_t = expert_gate.transpose(0, 2, 1)
    up_t = expert_up.transpose(0, 2, 1)

    wide = lax.axis_index("wide").astype(jnp.int32)
    place = jnp.stack([pos[0], wide >> 4, (wide >> 3) & 1, wide & 7])

    raw = pack(shared_gate, shared_up, shared_down.T)
    raws = [raw] + [lax.ppermute(raw, "wide", moved(0, i & 1, 0, i >> 1)) for i in (1, 2, 3)]

    outgoing = dispatch(pos, ids_t, tokens).reshape(EXPERTS, CAP, COLS)
    own = lax.all_to_all(outgoing, "wide", 0, 0, tiled=True).reshape(SLOTS, COLS)

    pieces = list(deal(place, raws, shared_gate.shape[1] // NX))
    for d in range(NX):
        pieces[NX + d] = lax.ppermute(pieces[NX + d], ("wide", "narrow"), turned_about(d))
    for d in range(1, NX):
        pieces[d] = lax.ppermute(pieces[d], "wide", moved(d, 0, 0))
    cuts = cut(pos, expert_down)
    others = [
        lax.ppermute(w, "narrow", swap)
        for w, swap in zip(cuts, (Y_SWAP, BOTH_SWAP, CORE_SWAP))
    ]
    column = stack(place, pieces)
    column = column.reshape(NX, NY, column.shape[1] // NY, column.shape[2])
    blocks = [column]
    for k in range(1, PAIRS):
        blocks.append(lax.ppermute(column, "wide", moved(0, 0, 2 * k)))
    toks = [tokens]
    for d in range(1, NX):
        toks.append(lax.ppermute(tokens, "wide", moved(d, 0, 0)))

    ys = []
    for k in range(CHUNKS):
        ys.append(lax.ppermute(own[k * CHUNK_ROWS : (k + 1) * CHUNK_ROWS], "narrow", Y_SWAP))
    core = lax.ppermute(own, "narrow", CORE_SWAP)
    hiddens = []
    for k in range(CHUNKS):
        both = lax.ppermute(ys[k], "narrow", CORE_SWAP)
        hidden = expert_hidden(pos, k, own, core, ys[k], both, gate_t, up_t)
        hidden_y = lax.ppermute(hidden, "narrow", Y_SWAP)
        hidden_core = lax.ppermute(hidden, "narrow", CORE_SWAP)
        hiddens.append([hidden, hidden_y, hidden_core])
    lanes, units = pieces[0].shape[1], pieces[NX].shape[1]
    common = shared_hidden(place, toks, blocks, hiddens[-1][0], lanes, units)
    common_y = lax.ppermute(common, "narrow", Y_SWAP)
    common_core = lax.ppermute(common, "narrow", CORE_SWAP)
    common_both = lax.ppermute(common_y, "narrow", CORE_SWAP)
    outputs = None
    for k in range(CHUNKS):
        hidden_both = lax.ppermute(hiddens[k][1], "narrow", CORE_SWAP)
        hiddens[k].insert(2, hidden_both)
        outputs = expert_columns(pos, k, hiddens[k], expert_down, others, outputs)
    returned = lax.all_to_all(outputs.reshape(EXPERTS, CAP, COLS), "wide", 0, 0, tiled=True)

    shared = list(shared_columns(place, [common, common_core, common_y, common_both], blocks, outputs))
    for d in range(1, NX):
        shared[d] = lax.ppermute(shared[d], "wide", moved(-d, 0, 0))
    rows = weigh(ids_t, gates_t)
    return combine(rows, returned.reshape(SLOTS, COLS), shared)


def solution(mesh):
    in_specs = (
        P("wide", None),
        P("wide", None),
        P("wide", None),
        P("wide", "narrow"),
        P("wide", "narrow"),
        P("narrow", "wide"),
        P("wide", None, "narrow"),
        P("wide", None, "narrow"),
        P("wide", "narrow", None),
    )
    out_specs = P("wide", "narrow")
    return jax.shard_map(body, mesh=mesh, in_specs=in_specs, out_specs=out_specs, check_vma=False)
```
